32 devices in a mesh: dp: 4 (over x, y), tp: 8 (over z, core).
Axes of the slice: x: 2, y: 2, z: 4, core: 2. Of those that a mesh axis runs over, the one named last changes fastest.
Arguments:
- tok_ids: int32 [8, 2048], P('dp'), parts along dimension 0
- pad_mask: int32 [8, 2048], P('dp'), parts along dimension 0
- emb_table: bfloat16 [250880, 2048], P('tp')
- ln_emb_w: bfloat16 [2048], replicated
- ln_emb_b: bfloat16 [2048], replicated
- ln1_w: bfloat16 [2048], replicated
- ln1_b: bfloat16 [2048], replicated
- w_qkv: bfloat16 [2048, 16, 3, 128], P(None, 'tp')
- b_qkv: bfloat16 [16, 3, 128], P('tp')
- w_out: bfloat16 [2048, 2048], P('tp')
- b_out: bfloat16 [2048], replicated
- ln2_w: bfloat16 [2048], replicated
- ln2_b: bfloat16 [2048], replicated
- w_up: bfloat16 [2048, 8192], P(None, 'tp')
- b_up: bfloat16 [8192], P('tp')
- w_down: bfloat16 [8192, 2048], P('tp')
- b_down: bfloat16 [2048], replicated
Outputs:
- output: bfloat16 [8, 2048, 2048], P('dp', 'tp'), parts along dimension 0
There are 4 independent parts. The reference program is written for one: setup_inputs(seed, part) draws one part's arguments, and reference() takes and returns one part's arrays. A program takes and returns all parts, laid end to end along the dimension named above; an argument that names none is the same for every part.
All inputs are finite; a program needn't handle non-finite values.
Results may differ from the reference program's by a relative error of at most 0.014022.
Values are sent between devices in bfloat16 or wider.
A program may use at most 1 GiB of HBM per device.

```python
import math
import jax
import jax.numpy as jnp
from jax import lax

VOCAB = 250880
D = 2048
HEADS = 16
BATCH = 2
SEQ = 2048
HEAD_DIM = D // HEADS
LN_EPS = 1e-5


def alibi_slopes(n_heads):
    closest = 2 ** int(math.floor(math.log2(n_heads)))
    base_ratio = 2.0 ** (-(2.0 ** -(math.log2(closest) - 3)))
    extra_ratio = 2.0 ** (-(2.0 ** -(math.log2(2 * closest) - 3)))
    first_part = [base_ratio ** step_k for step_k in range(1, closest + 1)]
    second_part = [extra_ratio ** step_k for step_k in range(1, 2 * (n_heads - closest), 2)]
    return first_part + second_part


def layer_norm(values_in, ln_gain, ln_shift):
    values_in = values_in.astype(jnp.float32)
    mean_v = jnp.mean(values_in, axis=-1, keepdims=True)
    centered = values_in - mean_v
    var_v = jnp.mean(centered * centered, axis=-1, keepdims=True)
    scaled = centered * lax.rsqrt(var_v + LN_EPS)
    return (scaled * ln_gain.astype(jnp.float32) + ln_shift.astype(jnp.float32)).astype(jnp.bfloat16)


def bloom_gelu(values_in):
    return values_in * 0.5 * (1.0 + jnp.tanh(0.79788456 * values_in * (1.0 + 0.044715 * values_in * values_in)))


def setup_inputs(seed: int = 0, part: int = 0) -> dict:
    root_key = jax.random.key(seed)
    part_key = jax.random.fold_in(root_key, part)
    id_key, coin_key, pad_key = jax.random.split(part_key, 3)
    raw_ids = jax.random.randint(id_key, (BATCH, SEQ), 0, VOCAB)
    coin_flips = jax.random.randint(coin_key, (BATCH, SEQ), 0, 2)
    tok_ids = jnp.where(coin_flips == 1, raw_ids // 16, raw_ids).astype(jnp.int32)
    tok_ids = tok_ids.at[0, SEQ - 2].set(0).at[0, SEQ - 1].set(VOCAB - 1)
    pad_len = jax.random.randint(pad_key, (BATCH, 1), 0, SEQ // 2 + 1)
    pad_len = pad_len.at[0, 0].set(SEQ // 2)
    pad_mask = (jnp.arange(SEQ)[None, :] >= pad_len).astype(jnp.int32)
    shared = jax.random.split(root_key, 15)
    emb_table = jax.random.normal(shared[0], (VOCAB, D), jnp.float32).astype(jnp.bfloat16)
    ln_emb_w = (1.0 + 0.3 * jax.random.normal(shared[1], (D,), jnp.float32)).astype(jnp.bfloat16)
    ln_emb_b = (0.3 * jax.random.normal(shared[2], (D,), jnp.float32)).astype(jnp.bfloat16)
    ln1_w = (1.0 + 0.3 * jax.random.normal(shared[3], (D,), jnp.float32)).astype(jnp.bfloat16)
    ln1_b = (0.3 * jax.random.normal(shared[4], (D,), jnp.float32)).astype(jnp.bfloat16)
    w_qkv = (jax.random.normal(shared[5], (D, HEADS, 3, HEAD_DIM), jnp.float32) * D ** -0.5).astype(jnp.bfloat16)
    b_qkv = (0.3 * jax.random.normal(shared[6], (HEADS, 3, HEAD_DIM), jnp.float32)).astype(jnp.bfloat16)
    w_out = (jax.random.normal(shared[7], (D, D), jnp.float32) * D ** -0.5).astype(jnp.bfloat16)
    b_out = (0.3 * jax.random.normal(shared[8], (D,), jnp.float32)).astype(jnp.bfloat16)
    ln2_w = (1.0 + 0.3 * jax.random.normal(shared[9], (D,), jnp.float32)).astype(jnp.bfloat16)
    ln2_b = (0.3 * jax.random.normal(shared[10], (D,), jnp.float32)).astype(jnp.bfloat16)
    w_up = (jax.random.normal(shared[11], (D, 4 * D), jnp.float32) * D ** -0.5).astype(jnp.bfloat16)
    b_up = (0.3 * jax.random.normal(shared[12], (4 * D,), jnp.float32)).astype(jnp.bfloat16)
    w_down = (jax.random.normal(shared[13], (4 * D, D), jnp.float32) * (4 * D) ** -0.5).astype(jnp.bfloat16)
    b_down = (0.3 * jax.random.normal(shared[14], (D,), jnp.float32)).astype(jnp.bfloat16)
    return dict(tok_ids=tok_ids, pad_mask=pad_mask, emb_table=emb_table, ln_emb_w=ln_emb_w, ln_emb_b=ln_emb_b, ln1_w=ln1_w, ln1_b=ln1_b, w_qkv=w_qkv, b_qkv=b_qkv, w_out=w_out, b_out=b_out, ln2_w=ln2_w, ln2_b=ln2_b, w_up=w_up, b_up=b_up, w_down=w_down, b_down=b_down)


def reference(tok_ids, pad_mask, emb_table, ln_emb_w, ln_emb_b, ln1_w, ln1_b, w_qkv, b_qkv, w_out, b_out, ln2_w, ln2_b, w_up, b_up, w_down, b_down):
    embedded = jnp.take(emb_table, tok_ids, axis=0)
    resid_in = layer_norm(embedded, ln_emb_w, ln_emb_b).reshape(BATCH * SEQ, D)
    normed = layer_norm(resid_in, ln1_w, ln1_b)
    qkv_flat = jnp.dot(normed, w_qkv.reshape(D, 3 * D), preferred_element_type=jnp.float32) + b_qkv.reshape(3 * D).astype(jnp.float32)
    qkv_all = qkv_flat.astype(jnp.bfloat16).reshape(BATCH, SEQ, HEADS, 3, HEAD_DIM)
    slopes = jnp.array(alibi_slopes(HEADS), jnp.float32)
    positions = jnp.arange(SEQ)
    distance = (positions[None, :] - positions[:, None]).astype(jnp.float32)
    alibi_bias = slopes[:, None, None] * distance[None]
    causal = positions[None, :] <= positions[:, None]
    diagonal = positions[None, :] == positions[:, None]
    score_scale = HEAD_DIM ** -0.5

    def one_sequence(seq_pair):
        qkv_seq, mask_row = seq_pair
        queries = qkv_seq[:, :, 0].astype(jnp.float32)
        key_vals = qkv_seq[:, :, 1].astype(jnp.float32)
        values = qkv_seq[:, :, 2].astype(jnp.float32)
        scores = jnp.einsum('qhd,khd->hqk', queries, key_vals) * score_scale + alibi_bias
        allowed = (causal & (mask_row[None, :] == 1)) | diagonal
        scores = jnp.where(allowed[None], scores, -1e30)
        attn_probs = jax.nn.softmax(scores, axis=-1).astype(jnp.bfloat16)
        context = jnp.einsum('hqk,khd->qhd', attn_probs.astype(jnp.float32), values)
        return context.astype(jnp.bfloat16).reshape(SEQ, D)

    context = lax.map(one_sequence, (qkv_all, pad_mask)).reshape(BATCH * SEQ, D)
    attn_proj = jnp.dot(context, w_out, preferred_element_type=jnp.float32) + b_out.astype(jnp.float32)
    resid_mid = (resid_in.astype(jnp.float32) + attn_proj).astype(jnp.bfloat16)
    normed2 = layer_norm(resid_mid, ln2_w, ln2_b)
    hidden_up = jnp.dot(normed2, w_up, preferred_element_type=jnp.float32) + b_up.astype(jnp.float32)
    activated = bloom_gelu(hidden_up).astype(jnp.bfloat16)
    down_proj = jnp.dot(activated, w_down, preferred_element_type=jnp.float32) + b_down.astype(jnp.float32)
    result = (resid_mid.astype(jnp.float32) + down_proj).astype(jnp.bfloat16)
    return result.reshape(BATCH, SEQ, D)
```

```python
import functools
import math
import jax
import jax.numpy as jnp
from jax import lax
from jax.experimental import pallas as pl
from jax.experimental.pallas import tpu as pltpu
from jax.sharding import PartitionSpec as P

LN_EPS = 1e-5
LOG2E = 1.4426950408889634
MESH = pl.DeviceIdType.MESH


def alibi_slopes(n_heads):
    closest = 2 ** int(math.floor(math.log2(n_heads)))
    base_ratio = 2.0 ** (-(2.0 ** -(math.log2(closest) - 3)))
    extra_ratio = 2.0 ** (-(2.0 ** -(math.log2(2 * closest) - 3)))
    first_part = [base_ratio ** step_k for step_k in range(1, closest + 1)]
    second_part = [extra_ratio ** step_k for step_k in range(1, 2 * (n_heads - closest), 2)]
    return first_part + second_part


def layer_norm(values_in, ln_gain, ln_shift):
    values_in = values_in.astype(jnp.float32)
    mean_v = jnp.mean(values_in, axis=-1, keepdims=True)
    centered = values_in - mean_v
    var_v = jnp.mean(centered * centered, axis=-1, keepdims=True)
    scaled = centered * lax.rsqrt(var_v + LN_EPS)
    return (scaled * ln_gain.astype(jnp.float32) + ln_shift.astype(jnp.float32)).astype(jnp.bfloat16)


def bloom_gelu(values_in):
    return values_in * 0.5 * (1.0 + jnp.tanh(0.79788456 * values_in * (1.0 + 0.044715 * values_in * values_in)))


GROUP = 64
SUB = 32
SLOTS = 4


def lookup_kernel(tile_ref, sel_ref, table_ref, out_ref, buf, sems):
    step = pl.program_id(0)
    steps = pl.num_programs(0)

    def issue(grp):
        slot = lax.rem(grp, SLOTS)
        for i in range(GROUP):
            row = pl.multiple_of(tile_ref[grp * GROUP + i] * 8, 8)
            pltpu.make_async_copy(table_ref.at[pl.ds(row, 8), :], buf.at[slot, pl.ds(i * 8, 8), :], sems.at[slot]).start()

    @pl.when(step == 0)
    def _():
        for grp in range(SLOTS - 1):
            issue(grp)

    @pl.when(step + SLOTS - 1 < steps)
    def _():
        issue(step + SLOTS - 1)

    slot = lax.rem(step, SLOTS)
    pltpu.make_async_copy(table_ref.at[pl.ds(0, GROUP * 8), :], buf.at[slot], sems.at[slot]).wait()
    for j in range(GROUP // SUB):
        cols = lax.broadcasted_iota(jnp.int32, (SUB, SUB * 8), 1)
        onehot = (cols == sel_ref[pl.ds(j * SUB, SUB), :]).astype(jnp.float32).astype(jnp.bfloat16)
        rows = jnp.dot(onehot, buf[slot, pl.ds(j * SUB * 8, SUB * 8), :], preferred_element_type=jnp.float32)
        out_ref[pl.ds(j * SUB, SUB), :] = rows.astype(jnp.bfloat16)


def lookup(ids, table, tp_rank):
    n_tok = ids.shape[0]
    vocab_loc, d = table.shape
    loc = ids - tp_rank * vocab_loc
    held = (loc >= 0) & (loc < vocab_loc)
    spread = (jnp.arange(n_tok, dtype=jnp.int32) * 5) % (vocab_loc // 8)
    tile = jnp.where(held, loc // 8, spread)
    sel = jnp.where(held, (jnp.arange(n_tok, dtype=jnp.int32) % SUB) * 8 + loc % 8, -1)[:, None]
    return pl.pallas_call(
        lookup_kernel,
        out_shape=jax.ShapeDtypeStruct((n_tok, d), jnp.bfloat16),
        grid_spec=pltpu.PrefetchScalarGridSpec(
            num_scalar_prefetch=1,
            grid=(n_tok // GROUP,),
            in_specs=[pl.BlockSpec((GROUP, 1), lambda i, t: (i, 0)), pl.BlockSpec(memory_space=pl.ANY)],
            out_specs=pl.BlockSpec((GROUP, d), lambda i, t: (i, 0)),
            scratch_shapes=[pltpu.VMEM((SLOTS, GROUP * 8, d), jnp.bfloat16), pltpu.SemaphoreType.DMA((SLOTS,))],
        ),
        compiler_params=pltpu.CompilerParams(dimension_semantics=("arbitrary",)),
        cost_estimate=pl.CostEstimate(flops=n_tok * d * 40000, bytes_accessed=n_tok * d * 18, transcendentals=0),
        name="lookup",
    )(tile, sel, table)


CHUNK = 64
LN_ROWS = 16


def norm_rows(x, gain, shift):
    n = x.shape[-1]
    mean_v = jnp.sum(x, axis=-1, keepdims=True) * (1.0 / n)
    centered = x - mean_v
    var_v = jnp.sum(centered * centered, axis=-1, keepdims=True) * (1.0 / n)
    return (centered * lax.rsqrt(var_v + LN_EPS) * gain + shift).astype(jnp.bfloat16)


def chain_kernel(n_tp, part_ref, ln_ref, a_ref, r0_ref, own, pre, rgt, lft, abuf, r0buf,
                 own_sem, pre_send, pre_recv, r_send, r_recv, l_send, l_recv, a_loc, a_send, a_recv, r0_loc, r0_send, r0_recv):
    seq = part_ref.shape[1]
    n_chunk = seq // CHUNK
    n_z = n_tp // 2
    me = lax.axis_index("tp")
    z = me // 2
    c = lax.rem(me, 2)
    peer = me + 1 - 2 * c
    pos_per = r0_ref.shape[1]
    per_dev = pos_per // CHUNK
    last = n_z - 1

    barrier = pltpu.get_barrier_semaphore()
    pl.semaphore_signal(barrier, inc=1, device_id={"tp": peer}, device_id_type=MESH)

    @pl.when(z > 0)
    def _():
        pl.semaphore_signal(barrier, inc=1, device_id={"tp": me - 2}, device_id_type=MESH)

    @pl.when(z < last)
    def _():
        pl.semaphore_signal(barrier, inc=1, device_id={"tp": me + 2}, device_id_type=MESH)

    @pl.when((z > 0) & (z < last))
    def _():
        pl.semaphore_wait(barrier, 3)

    @pl.when((z == 0) | (z == last))
    def _():
        pl.semaphore_wait(barrier, 2)

    def rows(k):
        return pl.ds(pl.multiple_of(k * CHUNK, CHUNK), CHUNK)

    def own_copy(k):
        return pltpu.make_async_copy(part_ref.at[c, rows(k), :], own.at[rows(k), :], own_sem.at[k])

    def pre_copy(k):
        return pltpu.make_async_remote_copy(part_ref.at[1 - c, rows(k), :], pre.at[rows(k), :], pre_send.at[k], pre_recv.at[k], device_id={"tp": peer}, device_id_type=MESH)

    def right_copy(src, k):
        return pltpu.make_async_remote_copy(src.at[rows(k), :], rgt.at[rows(k), :], r_send.at[k], r_recv.at[k], device_id={"tp": me + 2}, device_id_type=MESH)

    def left_copy(k):
        return pltpu.make_async_remote_copy(pre.at[rows(k), :], lft.at[rows(k), :], l_send.at[k], l_recv.at[k], device_id={"tp": me - 2}, device_id_type=MESH)

    def a_local(k):
        return pltpu.make_async_copy(abuf.at[rows(k), :], a_ref.at[c, rows(k), :], a_loc.at[k])

    def a_peer(k):
        return pltpu.make_async_remote_copy(abuf.at[rows(k), :], a_ref.at[c, rows(k), :], a_send.at[k], a_recv.at[k], device_id={"tp": peer}, device_id_type=MESH)

    def r0_local(i):
        return pltpu.make_async_copy(r0buf.at[c, rows(i), :], r0_ref.at[c, rows(i), :], r0_loc.at[i])

    def r0_peer(i):
        return pltpu.make_async_remote_copy(r0buf.at[1 - c, rows(i), :], r0_ref.at[c, rows(i), :], r0_send.at[i], r0_recv.at[i], device_id={"tp": peer}, device_id_type=MESH)

    def start(k, carry):
        own_copy(k).start()
        pre_copy(k).start()
        return carry

    lax.fori_loop(0, n_chunk, start, 0)

    def step_body(s, carry):
        @pl.when(s < n_chunk)
        def _():
            own_copy(s).wait()
            pre_copy(s).wait_recv()
            own[rows(s), :] = own[rows(s), :] + pre[rows(s), :]

        kr = s - z

        @pl.when((kr >= 0) & (kr < n_chunk))
        def _():
            @pl.when(z == 0)
            def _():
                right_copy(own, kr).start()

            @pl.when(z > 0)
            def _():
                right_copy(rgt, kr).wait_recv()
                rgt[rows(kr), :] = rgt[rows(kr), :] + own[rows(kr), :]

                @pl.when(z < last)
                def _():
                    right_copy(rgt, kr).start()

        kl = s - (last - z)

        @pl.when((kl >= 0) & (kl < n_chunk))
        def _():
            @pl.when(z < last)
            def _():
                left_copy(kl).wait_recv()

                @pl.when(z > 0)
                def _():
                    pre[rows(kl), :] = lft[rows(kl), :] + own[rows(kl), :]

            @pl.when(z == last)
            def _():
                pre[rows(kl), :] = own[rows(kl), :]

            @pl.when(z > 0)
            def _():
                left_copy(kl).start()

        kt = s - jnp.maximum(z, last - z)

        @pl.when((kt >= 0) & (kt < n_chunk))
        def _():
            base = kt * CHUNK
            first = kt - z * 2 * per_dev
            near = (first >= 0) & (first < 2 * per_dev)
            side = jnp.where(near, first // per_dev, 0)
            inner = jnp.where(near, lax.rem(first, per_dev), 0)

            def norm(i, carry):
                sl = pl.ds(pl.multiple_of(base + i * LN_ROWS, LN_ROWS), LN_ROWS)

                @pl.when(z == 0)
                def _():
                    abuf[sl, :] = own[sl, :] + lft[sl, :]

                @pl.when((z > 0) & (z < last))
                def _():
                    abuf[sl, :] = rgt[sl, :] + lft[sl, :]

                @pl.when(z == last)
                def _():
                    abuf[sl, :] = rgt[sl, :]

                r0 = norm_rows(abuf[sl, :].astype(jnp.float32), ln_ref[0:1, :], ln_ref[1:2, :])
                abuf[sl, :] = norm_rows(r0.astype(jnp.float32), ln_ref[2:3, :], ln_ref[3:4, :])

                @pl.when(near)
                def _():
                    r0buf[side, pl.ds(pl.multiple_of(inner * CHUNK + i * LN_ROWS, LN_ROWS), LN_ROWS), :] = r0

                return carry

            lax.fori_loop(0, CHUNK // LN_ROWS, norm, 0)
            a_local(kt).start()
            a_peer(kt).start()

            @pl.when(near & (side == c))
            def _():
                r0_local(inner).start()

            @pl.when(near & (side != c))
            def _():
                r0_peer(inner).start()

        return carry

    lax.fori_loop(0, n_chunk + last, step_body, 0)

    def drain(k, carry):
        pre_copy(k).wait_send()
        a_local(k).wait()
        a_peer(k).wait()

        @pl.when(z < last)
        def _():
            right_copy(rgt, k).wait_send()

        @pl.when(z > 0)
        def _():
            left_copy(k).wait_send()

        return carry

    lax.fori_loop(0, n_chunk, drain, 0)

    def drain_r0(i, carry):
        r0_local(i).wait()
        r0_peer(i).wait()
        return carry

    lax.fori_loop(0, per_dev, drain_r0, 0)


def chain(part, ln_pack, n_tp):
    n_seq, seq, d = part.shape
    n_chunk = seq // CHUNK
    per_dev = seq // n_tp // CHUNK
    dma = pltpu.SemaphoreType.DMA
    big = pltpu.VMEM((seq, d), jnp.bfloat16)
    return pl.pallas_call(
        functools.partial(chain_kernel, n_tp),
        out_shape=(jax.ShapeDtypeStruct((n_seq, seq, d), jnp.bfloat16), jax.ShapeDtypeStruct((n_seq, seq // n_tp, d), jnp.bfloat16)),
        in_specs=[pl.BlockSpec(memory_space=pl.ANY), pl.BlockSpec(memory_space=pltpu.VMEM)],
        out_specs=(pl.BlockSpec(memory_space=pl.ANY), pl.BlockSpec(memory_space=pl.ANY)),
        scratch_shapes=[big, big, big, big, big, pltpu.VMEM((2, seq // n_tp, d), jnp.bfloat16)]
        + [dma((n_chunk,))] * 10 + [dma((per_dev,))] * 3,
        compiler_params=pltpu.CompilerParams(collective_id=0, has_side_effects=True, vmem_limit_bytes=60000 * 1024),
        cost_estimate=pl.CostEstimate(flops=10 ** 12, bytes_accessed=8 * part.size, transcendentals=0),
        name="chain",
    )(part, ln_pack)


def attend_kernel(n_tp, head_dim, qkv_ref, pad_ref, slope_ref, bup_ref, ctx_ref, ball_ref, cbuf, send_sem, recv_sem, loc_sem, b_send, b_recv, b_loc):
    n_seq, heads = qkv_ref.shape[1], qkv_ref.shape[2]
    seq = qkv_ref.shape[3]
    blk = seq // n_tp
    feat = heads * head_dim
    me = lax.axis_index("tp")

    barrier = pltpu.get_barrier_semaphore()
    for r in range(1, n_tp):
        pl.semaphore_signal(barrier, inc=1, device_id={"tp": lax.rem(me + r, n_tp)}, device_id_type=MESH)
    pl.semaphore_wait(barrier, n_tp - 1)

    def cols(t):
        return pl.ds(pl.multiple_of(t * feat, feat), feat)

    def bias_copy(r):
        return pltpu.make_async_remote_copy(bup_ref, ball_ref.at[me], b_send.at[r], b_recv.at[r], device_id={"tp": lax.rem(me + r, n_tp)}, device_id_type=MESH)

    for r in range(1, n_tp):
        bias_copy(r).start()
    own_bias = pltpu.make_async_copy(bup_ref, ball_ref.at[me], b_loc.at[0])
    own_bias.start()

    def ctx_copy(b, r):
        return pltpu.make_async_remote_copy(cbuf.at[b, r], ctx_ref.at[b, :, cols(me)], send_sem.at[b, r], recv_sem.at[b, r], device_id={"tp": lax.rem(me + r, n_tp)}, device_id_type=MESH)

    def ctx_local(b):
        return pltpu.make_async_copy(cbuf.at[b, 0], ctx_ref.at[b, :, cols(me)], loc_sem.at[b])

    def one(i, carry):
        b = lax.rem(i, n_seq)
        r = n_tp - 1 - i // n_seq
        dest = lax.rem(me + r, n_tp)
        for j in range(n_tp):
            @pl.when(dest == j)
            def _(j=j):
                span = (j + 1) * blk
                lo = j * blk
                key_pos = lax.broadcasted_iota(jnp.int32, (1, span), 1)
                key_ok = pad_ref[b, :, 0:span] == 1
                row_in = lax.broadcasted_iota(jnp.int32, (blk, blk), 0)
                col_in = lax.broadcasted_iota(jnp.int32, (blk, blk), 1)
                diag_ok = ((col_in < row_in) & (pad_ref[b, :, lo:span] == 1)) | (col_in == row_in)
                for h in range(heads):
                    slope = slope_ref[0, h] * LOG2E
                    rel = slope * (key_pos - lo).astype(jnp.float32)
                    far = jnp.where(key_ok, rel, -1e30)
                    q = qkv_ref[0, b, h, lo:span, :]
                    scale = head_dim ** -0.5 * LOG2E
                    diag = lax.dot_general(q, qkv_ref[1, b, h, lo:span, :], (((1,), (1,)), ((), ())), preferred_element_type=jnp.float32)
                    diag = jnp.where(diag_ok, diag * scale + rel[:, lo:span], -1e30)
                    top = jnp.max(diag, axis=-1, keepdims=True)
                    if j:
                        past = lax.dot_general(q, qkv_ref[1, b, h, 0:lo, :], (((1,), (1,)), ((), ())), preferred_element_type=jnp.float32)
                        past = past * scale + far[:, 0:lo]
                        top = jnp.maximum(top, jnp.max(past, axis=-1, keepdims=True))
                        past = jnp.exp2(past - top)
                    diag = jnp.exp2(diag - top)
                    total = jnp.sum(diag, axis=-1, keepdims=True)
                    if j:
                        total = total + jnp.sum(past, axis=-1, keepdims=True)
                    inv = 1.0 / total
                    out = jnp.dot((diag * inv).astype(jnp.bfloat16), qkv_ref[2, b, h, lo:span, :], preferred_element_type=jnp.float32)
                    if j:
                        out = out + jnp.dot((past * inv).astype(jnp.bfloat16), qkv_ref[2, b, h, 0:lo, :], preferred_element_type=jnp.float32)
                    cbuf[b, r, :, h * head_dim:(h + 1) * head_dim] = out.astype(jnp.bfloat16)

        @pl.when(r > 0)
        def _():
            ctx_copy(b, r).start()

        @pl.when(r == 0)
        def _():
            ctx_local(b).start()

        return carry

    lax.fori_loop(0, n_seq * n_tp, one, 0)

    for b in range(n_seq):
        ctx_local(b).wait()
        for r in range(1, n_tp):
            ctx_copy(b, r).wait()
    own_bias.wait()
    for r in range(1, n_tp):
        bias_copy(r).wait()


def attend(qkv, pad_mask, slopes, b_up, n_tp):
    _, n_seq, heads, seq, head_dim = qkv.shape
    blk = seq // n_tp
    feat = heads * head_dim
    dma = pltpu.SemaphoreType.DMA
    vmem = pl.BlockSpec(memory_space=pltpu.VMEM)
    return pl.pallas_call(
        functools.partial(attend_kernel, n_tp, head_dim),
        out_shape=(jax.ShapeDtypeStruct((n_seq, blk, n_tp * feat), jnp.bfloat16), jax.ShapeDtypeStruct((n_tp,) + b_up.shape, jnp.bfloat16)),
        in_specs=[vmem, vmem, pl.BlockSpec(memory_space=pltpu.SMEM), vmem],
        out_specs=(pl.BlockSpec(memory_space=pl.ANY), pl.BlockSpec(memory_space=pl.ANY)),
        scratch_shapes=[pltpu.VMEM((n_seq, n_tp, blk, feat), jnp.bfloat16), dma((n_seq, n_tp)), dma((n_seq, n_tp)), dma((n_seq,)), dma((n_tp,)), dma((n_tp,)), dma((1,))],
        compiler_params=pltpu.CompilerParams(collective_id=1, has_side_effects=True, vmem_limit_bytes=56000 * 1024),
        cost_estimate=pl.CostEstimate(flops=30 * 10 ** 9, bytes_accessed=2 * qkv.size, transcendentals=seq * seq * 2),
        name="attend",
    )(qkv, pad_mask[:, None, :], slopes[None, :], b_up)


def solution(mesh):
    n_tp = mesh.shape['tp']
    n_dp = mesh.shape['dp']

    def local_step(tok_ids, pad_mask, emb_shard, ln_emb_w, ln_emb_b, ln1_w, ln1_b, w_qkv, b_qkv, w_out, b_out, ln2_w, ln2_b, w_up, b_up, w_down, b_down):
        f32 = jnp.float32
        tp_rank = lax.axis_index('tp')
        dp_rank = lax.axis_index('dp')
        n_seq, seq = tok_ids.shape
        d = emb_shard.shape[1]
        heads_loc = w_qkv.shape[1]

        def part(w, axis):
            size = w.shape[axis] // n_dp
            return lax.dynamic_slice_in_dim(w, dp_rank * size, size, axis)

        half = n_tp // 2
        swap = [(t, (t + half) % n_tp) for t in range(n_tp)]
        quads = [list(range(half)), list(range(half, n_tp))]
        wo = lax.all_gather(part(w_out, 0), ('tp', 'dp'), axis=0, tiled=True)
        up_part = lax.ppermute(part(w_up, 1), 'tp', swap)
        down_part = lax.ppermute(part(w_down, 0), 'tp', swap)

        part_emb = lookup(tok_ids.reshape(-1), emb_shard, tp_rank).reshape(n_seq, seq, d)
        part_emb, up_part, down_part = lax.optimization_barrier((part_emb, up_part, down_part))
        wu = lax.all_gather(up_part, 'dp', axis=0, tiled=False)
        wd = lax.all_gather(down_part, 'dp', axis=0, tiled=True)
        ln_pack = jnp.stack([ln_emb_w, ln_emb_b, ln1_w, ln1_b]).astype(f32)
        normed_all, resid_in = chain(part_emb, ln_pack, n_tp)
        normed_all, wu, wd = lax.optimization_barrier((normed_all, wu, wd))
        qkv = (jnp.einsum('bsd,dhce->cbhse', normed_all, w_qkv, preferred_element_type=f32) + b_qkv.astype(f32).transpose(1, 0, 2)[:, None, :, None, :]).astype(jnp.bfloat16)
        all_slopes = jnp.array(alibi_slopes(heads_loc * n_tp), f32)
        head_slopes = lax.dynamic_slice_in_dim(all_slopes, tp_rank * heads_loc, heads_loc)
        context, b_all = attend(qkv, pad_mask, head_slopes, b_up.reshape(8, -1), n_tp)
        attn = jnp.einsum('bsk,kc->bsc', context, wo, preferred_element_type=f32)
        resid_mid = (resid_in.astype(f32) + (attn + b_out.astype(f32))).astype(jnp.bfloat16)
        normed2 = layer_norm(resid_mid, ln2_w, ln2_b)
        far_bias = lax.dynamic_index_in_dim(b_all, (tp_rank + half) % n_tp, 0, keepdims=False).reshape(n_dp, -1)
        quad_in = lax.all_gather(normed2, 'tp', axis=1, tiled=True, axis_index_groups=quads)
        near_up = jnp.einsum('bsk,kf->bsf', quad_in, w_up, preferred_element_type=f32) + b_up.astype(f32)
        far_up = jnp.einsum('bsk,nkc->bsnc', quad_in, wu, preferred_element_type=f32) + far_bias.astype(f32)
        near_act = bloom_gelu(near_up).astype(jnp.bfloat16)
        far_act = bloom_gelu(far_up).astype(jnp.bfloat16).reshape(near_act.shape)
        down = jnp.einsum('bsf,fd->bsd', near_act, w_down, preferred_element_type=f32) + jnp.einsum('bsf,fd->bsd', far_act, wd, preferred_element_type=f32)
        down_sum = lax.psum_scatter(down.astype(jnp.bfloat16), 'tp', scatter_dimension=1, tiled=True, axis_index_groups=quads)
        return (resid_mid.astype(f32) + (down_sum.astype(f32) + b_down.astype(f32))).astype(jnp.bfloat16)

    replicated = P(None)
    in_specs = (P('dp', None), P('dp', None), P('tp', None), replicated, replicated, replicated, replicated, P(None, 'tp', None, None), P('tp', None, None), P('tp', None), replicated, replicated, replicated, P(None, 'tp'), P('tp'), P('tp', None), replicated)
    return jax.shard_map(local_step, mesh=mesh, in_specs=in_specs, out_specs=P('dp', 'tp', None), check_vma=False)
```

```python
import functools
import math
import jax
import jax.numpy as jnp
from jax import lax
from jax.experimental import pallas as pl
from jax.experimental.pallas import tpu as pltpu
from jax.sharding import PartitionSpec as P

LN_EPS = 1e-5
LOG2E = 1.4426950408889634
MESH = pl.DeviceIdType.MESH


def alibi_slopes(n_heads):
    closest = 2 ** int(math.floor(math.log2(n_heads)))
    base_ratio = 2.0 ** (-(2.0 ** -(math.log2(closest) - 3)))
    extra_ratio = 2.0 ** (-(2.0 ** -(math.log2(2 * closest) - 3)))
    first_part = [base_ratio ** step_k for step_k in range(1, closest + 1)]
    second_part = [extra_ratio ** step_k for step_k in range(1, 2 * (n_heads - closest), 2)]
    return first_part + second_part


def layer_norm(values_in, ln_gain, ln_shift):
    values_in = values_in.astype(jnp.float32)
    mean_v = jnp.mean(values_in, axis=-1, keepdims=True)
    centered = values_in - mean_v
    var_v = jnp.mean(centered * centered, axis=-1, keepdims=True)
    scaled = centered * lax.rsqrt(var_v + LN_EPS)
    return (scaled * ln_gain.astype(jnp.float32) + ln_shift.astype(jnp.float32)).astype(jnp.bfloat16)


def bloom_gelu(values_in):
    return values_in * 0.5 * (1.0 + jnp.tanh(0.79788456 * values_in * (1.0 + 0.044715 * values_in * values_in)))


GROUP = 64
SUB = 32
SLOTS = 4


def lookup_kernel(tile_ref, sel_ref, table_ref, out_ref, buf, sems):
    step = pl.program_id(0)
    steps = pl.num_programs(0)

    def issue(grp):
        slot = lax.rem(grp, SLOTS)
        for i in range(GROUP):
            row = pl.multiple_of(tile_ref[grp * GROUP + i] * 8, 8)
            pltpu.make_async_copy(table_ref.at[pl.ds(row, 8), :], buf.at[slot, pl.ds(i * 8, 8), :], sems.at[slot]).start()

    @pl.when(step == 0)
    def _():
        for grp in range(SLOTS - 1):
            issue(grp)

    @pl.when(step + SLOTS - 1 < steps)
    def _():
        issue(step + SLOTS - 1)

    slot = lax.rem(step, SLOTS)
    pltpu.make_async_copy(table_ref.at[pl.ds(0, GROUP * 8), :], buf.at[slot], sems.at[slot]).wait()
    for j in range(GROUP // SUB):
        cols = lax.broadcasted_iota(jnp.int32, (SUB, SUB * 8), 1)
        onehot = (cols == sel_ref[pl.ds(j * SUB, SUB), :]).astype(jnp.float32).astype(jnp.bfloat16)
        rows = jnp.dot(onehot, buf[slot, pl.ds(j * SUB * 8, SUB * 8), :], preferred_element_type=jnp.float32)
        out_ref[pl.ds(j * SUB, SUB), :] = rows.astype(jnp.bfloat16)


def lookup(ids, table, tp_rank):
    n_tok = ids.shape[0]
    vocab_loc, d = table.shape
    loc = ids - tp_rank * vocab_loc
    held = (loc >= 0) & (loc < vocab_loc)
    spread = (jnp.arange(n_tok, dtype=jnp.int32) * 5) % (vocab_loc // 8)
    tile = jnp.where(held, loc // 8, spread)
    sel = jnp.where(held, (jnp.arange(n_tok, dtype=jnp.int32) % SUB) * 8 + loc % 8, -1)[:, None]
    return pl.pallas_call(
        lookup_kernel,
        out_shape=jax.ShapeDtypeStruct((n_tok, d), jnp.bfloat16),
        grid_spec=pltpu.PrefetchScalarGridSpec(
            num_scalar_prefetch=1,
            grid=(n_tok // GROUP,),
            in_specs=[pl.BlockSpec((GROUP, 1), lambda i, t: (i, 0)), pl.BlockSpec(memory_space=pl.ANY)],
            out_specs=pl.BlockSpec((GROUP, d), lambda i, t: (i, 0)),
            scratch_shapes=[pltpu.VMEM((SLOTS, GROUP * 8, d), jnp.bfloat16), pltpu.SemaphoreType.DMA((SLOTS,))],
        ),
        compiler_params=pltpu.CompilerParams(dimension_semantics=("arbitrary",)),
        cost_estimate=pl.CostEstimate(flops=n_tok * d * 40000, bytes_accessed=n_tok * d * 18, transcendentals=0),
        name="lookup",
    )(tile, sel, table)


CHUNK = 64
LN_ROWS = 16


def norm_rows(x, gain, shift):
    n = x.shape[-1]
    mean_v = jnp.sum(x, axis=-1, keepdims=True) * (1.0 / n)
    centered = x - mean_v
    var_v = jnp.sum(centered * centered, axis=-1, keepdims=True) * (1.0 / n)
    return (centered * lax.rsqrt(var_v + LN_EPS) * gain + shift).astype(jnp.bfloat16)


def chain_kernel(n_tp, part_ref, ln_ref, a_ref, r0_ref, own, pre, rgt, lft, abuf, r0buf,
                 own_sem, pre_send, pre_recv, r_send, r_recv, l_send, l_recv, a_loc, a_send, a_recv, r0_loc, r0_send, r0_recv):
    seq = part_ref.shape[1]
    n_chunk = seq // CHUNK
    n_z = n_tp // 2
    me = lax.axis_index("tp")
    z = me // 2
    c = lax.rem(me, 2)
    peer = me + 1 - 2 * c
    pos_per = r0_ref.shape[1]
    per_dev = pos_per // CHUNK
    last = n_z - 1

    barrier = pltpu.get_barrier_semaphore()
    pl.semaphore_signal(barrier, inc=1, device_id={"tp": peer}, device_id_type=MESH)

    @pl.when(z > 0)
    def _():
        pl.semaphore_signal(barrier, inc=1, device_id={"tp": me - 2}, device_id_type=MESH)

    @pl.when(z < last)
    def _():
        pl.semaphore_signal(barrier, inc=1, device_id={"tp": me + 2}, device_id_type=MESH)

    @pl.when((z > 0) & (z < last))
    def _():
        pl.semaphore_wait(barrier, 3)

    @pl.when((z == 0) | (z == last))
    def _():
        pl.semaphore_wait(barrier, 2)

    def rows(k):
        return pl.ds(pl.multiple_of(k * CHUNK, CHUNK), CHUNK)

    def own_copy(k):
        return pltpu.make_async_copy(part_ref.at[c, rows(k), :], own.at[rows(k), :], own_sem.at[k])

    def pre_copy(k):
        return pltpu.make_async_remote_copy(part_ref.at[1 - c, rows(k), :], pre.at[rows(k), :], pre_send.at[k], pre_recv.at[k], device_id={"tp": peer}, device_id_type=MESH)

    def right_copy(src, k):
        return pltpu.make_async_remote_copy(src.at[rows(k), :], rgt.at[rows(k), :], r_send.at[k], r_recv.at[k], device_id={"tp": me + 2}, device_id_type=MESH)

    def left_copy(k):
        return pltpu.make_async_remote_copy(pre.at[rows(k), :], lft.at[rows(k), :], l_send.at[k], l_recv.at[k], device_id={"tp": me - 2}, device_id_type=MESH)

    def a_local(k):
        return pltpu.make_async_copy(abuf.at[rows(k), :], a_ref.at[c, rows(k), :], a_loc.at[k])

    def a_peer(k):
        return pltpu.make_async_remote_copy(abuf.at[rows(k), :], a_ref.at[c, rows(k), :], a_send.at[k], a_recv.at[k], device_id={"tp": peer}, device_id_type=MESH)

    def r0_local(i):
        return pltpu.make_async_copy(r0buf.at[c, rows(i), :], r0_ref.at[c, rows(i), :], r0_loc.at[i])

    def r0_peer(i):
        return pltpu.make_async_remote_copy(r0buf.at[1 - c, rows(i), :], r0_ref.at[c, rows(i), :], r0_send.at[i], r0_recv.at[i], device_id={"tp": peer}, device_id_type=MESH)

    def start(k, carry):
        own_copy(k).start()
        pre_copy(k).start()
        return carry

    lax.fori_loop(0, n_chunk, start, 0)

    def step_body(s, carry):
        @pl.when(s < n_chunk)
        def _():
            own_copy(s).wait()
            pre_copy(s).wait_recv()
            own[rows(s), :] = own[rows(s), :] + pre[rows(s), :]

        kr = s - z

        @pl.when((kr >= 0) & (kr < n_chunk))
        def _():
            @pl.when(z == 0)
            def _():
                right_copy(own, kr).start()

            @pl.when(z > 0)
            def _():
                right_copy(rgt, kr).wait_recv()
                rgt[rows(kr), :] = rgt[rows(kr), :] + own[rows(kr), :]

                @pl.when(z < last)
                def _():
                    right_copy(rgt, kr).start()

        kl = s - (last - z)

        @pl.when((kl >= 0) & (kl < n_chunk))
        def _():
            @pl.when(z < last)
            def _():
                left_copy(kl).wait_recv()

                @pl.when(z > 0)
                def _():
                    pre[rows(kl), :] = lft[rows(kl), :] + own[rows(kl), :]

            @pl.when(z == last)
            def _():
                pre[rows(kl), :] = own[rows(kl), :]

            @pl.when(z > 0)
            def _():
                left_copy(kl).start()

        kt = s - jnp.maximum(z, last - z)

        @pl.when((kt >= 0) & (kt < n_chunk))
        def _():
            base = kt * CHUNK
            first = kt - z * 2 * per_dev
            near = (first >= 0) & (first < 2 * per_dev)
            side = jnp.where(near, first // per_dev, 0)
            inner = jnp.where(near, lax.rem(first, per_dev), 0)

            def norm(i, carry):
                sl = pl.ds(pl.multiple_of(base + i * LN_ROWS, LN_ROWS), LN_ROWS)

                @pl.when(z == 0)
                def _():
                    abuf[sl, :] = own[sl, :] + lft[sl, :]

                @pl.when((z > 0) & (z < last))
                def _():
                    abuf[sl, :] = rgt[sl, :] + lft[sl, :]

                @pl.when(z == last)
                def _():
                    abuf[sl, :] = rgt[sl, :]

                r0 = norm_rows(abuf[sl, :].astype(jnp.float32), ln_ref[0:1, :], ln_ref[1:2, :])
                abuf[sl, :] = norm_rows(r0.astype(jnp.float32), ln_ref[2:3, :], ln_ref[3:4, :])

                @pl.when(near)
                def _():
                    r0buf[side, pl.ds(pl.multiple_of(inner * CHUNK + i * LN_ROWS, LN_ROWS), LN_ROWS), :] = r0

                return carry

            lax.fori_loop(0, CHUNK // LN_ROWS, norm, 0)
            a_local(kt).start()
            a_peer(kt).start()

            @pl.when(near & (side == c))
            def _():
                r0_local(inner).start()

            @pl.when(near & (side != c))
            def _():
                r0_peer(inner).start()

        return carry

    lax.fori_loop(0, n_chunk + last, step_body, 0)

    def drain(k, carry):
        pre_copy(k).wait_send()
        a_local(k).wait()
        a_peer(k).wait()

        @pl.when(z < last)
        def _():
            right_copy(rgt, k).wait_send()

        @pl.when(z > 0)
        def _():
            left_copy(k).wait_send()

        return carry

    lax.fori_loop(0, n_chunk, drain, 0)

    def drain_r0(i, carry):
        r0_local(i).wait()
        r0_peer(i).wait()
        return carry

    lax.fori_loop(0, per_dev, drain_r0, 0)


def chain(part, ln_pack, n_tp):
    n_seq, seq, d = part.shape
    n_chunk = seq // CHUNK
    per_dev = seq // n_tp // CHUNK
    dma = pltpu.SemaphoreType.DMA
    big = pltpu.VMEM((seq, d), jnp.bfloat16)
    return pl.pallas_call(
        functools.partial(chain_kernel, n_tp),
        out_shape=(jax.ShapeDtypeStruct((n_seq, seq, d), jnp.bfloat16), jax.ShapeDtypeStruct((n_seq, seq // n_tp, d), jnp.bfloat16)),
        in_specs=[pl.BlockSpec(memory_space=pl.ANY), pl.BlockSpec(memory_space=pltpu.VMEM)],
        out_specs=(pl.BlockSpec(memory_space=pl.ANY), pl.BlockSpec(memory_space=pl.ANY)),
        scratch_shapes=[big, big, big, big, big, pltpu.VMEM((2, seq // n_tp, d), jnp.bfloat16)]
        + [dma((n_chunk,))] * 10 + [dma((per_dev,))] * 3,
        compiler_params=pltpu.CompilerParams(collective_id=0, has_side_effects=True, vmem_limit_bytes=60000 * 1024),
        cost_estimate=pl.CostEstimate(flops=10 ** 12, bytes_accessed=8 * part.size, transcendentals=0),
        name="chain",
    )(part, ln_pack)


def attend_kernel(n_tp, head_dim, qkv_ref, pad_ref, slope_ref, bup_ref, ctx_ref, ball_ref, cbuf, send_sem, recv_sem, loc_sem, b_send, b_recv, b_loc):
    n_seq, heads = qkv_ref.shape[1], qkv_ref.shape[2]
    seq = qkv_ref.shape[3]
    blk = seq // n_tp
    feat = heads * head_dim
    me = lax.axis_index("tp")

    barrier = pltpu.get_barrier_semaphore()
    for r in range(1, n_tp):
        pl.semaphore_signal(barrier, inc=1, device_id={"tp": lax.rem(me + r, n_tp)}, device_id_type=MESH)
    pl.semaphore_wait(barrier, n_tp - 1)

    def cols(t):
        return pl.ds(pl.multiple_of(t * feat, feat), feat)

    def bias_copy(r):
        return pltpu.make_async_remote_copy(bup_ref, ball_ref.at[me], b_send.at[r], b_recv.at[r], device_id={"tp": lax.rem(me + r, n_tp)}, device_id_type=MESH)

    for r in range(1, n_tp):
        bias_copy(r).start()
    own_bias = pltpu.make_async_copy(bup_ref, ball_ref.at[me], b_loc.at[0])
    own_bias.start()

    def ctx_copy(b, r):
        return pltpu.make_async_remote_copy(cbuf.at[b, r], ctx_ref.at[b, :, cols(me)], send_sem.at[b, r], recv_sem.at[b, r], device_id={"tp": lax.rem(me + r, n_tp)}, device_id_type=MESH)

    def ctx_local(b):
        return pltpu.make_async_copy(cbuf.at[b, 0], ctx_ref.at[b, :, cols(me)], loc_sem.at[b])

    def one(i, carry):
        b = lax.rem(i, n_seq)
        r = n_tp - 1 - i // n_seq
        dest = lax.rem(me + r, n_tp)
        for j in range(n_tp):
            @pl.when(dest == j)
            def _(j=j):
                span = (j + 1) * blk
                lo = j * blk
                key_pos = lax.broadcasted_iota(jnp.int32, (1, span), 1)
                key_ok = pad_ref[b, :, 0:span] == 1
                row_in = lax.broadcasted_iota(jnp.int32, (blk, blk), 0)
                col_in = lax.broadcasted_iota(jnp.int32, (blk, blk), 1)
                diag_ok = ((col_in < row_in) & (pad_ref[b, :, lo:span] == 1)) | (col_in == row_in)
                for h in range(heads):
                    slope = slope_ref[0, h] * LOG2E
                    rel = slope * (key_pos - lo).astype(jnp.float32)
                    far = jnp.where(key_ok, rel, -1e30)
                    q = qkv_ref[0, b, h, lo:span, :]
                    scale = head_dim ** -0.5 * LOG2E
                    diag = lax.dot_general(q, qkv_ref[1, b, h, lo:span, :], (((1,), (1,)), ((), ())), preferred_element_type=jnp.float32)
                    diag = jnp.where(diag_ok, diag * scale + rel[:, lo:span], -1e30)
                    top = jnp.max(diag, axis=-1, keepdims=True)
                    if j:
                        past = lax.dot_general(q, qkv_ref[1, b, h, 0:lo, :], (((1,), (1,)), ((), ())), preferred_element_type=jnp.float32)
                        past = past * scale + far[:, 0:lo]
                        top = jnp.maximum(top, jnp.max(past, axis=-1, keepdims=True))
                        past = jnp.exp2(past - top)
                    diag = jnp.exp2(diag - top)
                    total = jnp.sum(diag, axis=-1, keepdims=True)
                    if j:
                        total = total + jnp.sum(past, axis=-1, keepdims=True)
                    inv = 1.0 / total
                    out = jnp.dot((diag * inv).astype(jnp.bfloat16), qkv_ref[2, b, h, lo:span, :], preferred_element_type=jnp.float32)
                    if j:
                        out = out + jnp.dot((past * inv).astype(jnp.bfloat16), qkv_ref[2, b, h, 0:lo, :], preferred_element_type=jnp.float32)
                    cbuf[b, r, :, h * head_dim:(h + 1) * head_dim] = out.astype(jnp.bfloat16)

        @pl.when(r > 0)
        def _():
            ctx_copy(b, r).start()

        @pl.when(r == 0)
        def _():
            ctx_local(b).start()

        return carry

    lax.fori_loop(0, n_seq * n_tp, one, 0)

    for b in range(n_seq):
        ctx_local(b).wait()
        for r in range(1, n_tp):
            ctx_copy(b, r).wait()
    own_bias.wait()
    for r in range(1, n_tp):
        bias_copy(r).wait()


def attend(qkv, pad_mask, slopes, b_up, n_tp):
    _, n_seq, heads, seq, head_dim = qkv.shape
    blk = seq // n_tp
    feat = heads * head_dim
    dma = pltpu.SemaphoreType.DMA
    vmem = pl.BlockSpec(memory_space=pltpu.VMEM)
    return pl.pallas_call(
        functools.partial(attend_kernel, n_tp, head_dim),
        out_shape=(jax.ShapeDtypeStruct((n_seq, blk, n_tp * feat), jnp.bfloat16), jax.ShapeDtypeStruct((n_tp,) + b_up.shape, jnp.bfloat16)),
        in_specs=[vmem, vmem, pl.BlockSpec(memory_space=pltpu.SMEM), vmem],
        out_specs=(pl.BlockSpec(memory_space=pl.ANY), pl.BlockSpec(memory_space=pl.ANY)),
        scratch_shapes=[pltpu.VMEM((n_seq, n_tp, blk, feat), jnp.bfloat16), dma((n_seq, n_tp)), dma((n_seq, n_tp)), dma((n_seq,)), dma((n_tp,)), dma((n_tp,)), dma((1,))],
        compiler_params=pltpu.CompilerParams(collective_id=1, has_side_effects=True, vmem_limit_bytes=56000 * 1024),
        cost_estimate=pl.CostEstimate(flops=30 * 10 ** 9, bytes_accessed=2 * qkv.size, transcendentals=seq * seq * 2),
        name="attend",
    )(qkv, pad_mask[:, None, :], slopes[None, :], b_up)


SUBROWS = 128


def mlp_kernel(n_dp, n2_ref, wup_ref, wdn_ref, fup_ref, fdn_ref, bias_ref, bdn_ref, r1_ref, out_ref,
               xbuf, ptl, up_w, dn_w, act, from_peer, pre, from_far, obuf,
               w_sem, x_sem, px_send, px_recv, fx_send, fx_recv, fw_send, fw_recv, lp_send, lp_recv, pr_send, pr_recv, rf_send, rf_recv, o_sem):
    me = lax.axis_index("tp")
    peer = me + 1 - 2 * lax.rem(me, 2)
    far = me + 2 - 4 * lax.rem(me // 2, 2)
    mid = 2 * SUBROWS
    n_loc = n2_ref.shape[0] // mid
    n_sub = n2_ref.shape[0] // SUBROWS
    steps = 2 * n_loc + n_sub
    first_far = 2 * n_loc
    wide = up_w.shape[2]
    n_up = wup_ref.shape[1] // wide
    n_blk = up_w.shape[0]
    d_loc = wdn_ref.shape[0]
    slim = fup_ref.shape[2]

    barrier = pltpu.get_barrier_semaphore()
    pl.semaphore_signal(barrier, inc=1, device_id={"tp": peer}, device_id_type=MESH)
    pl.semaphore_signal(barrier, inc=1, device_id={"tp": far}, device_id_type=MESH)

    loads = [pltpu.make_async_copy(n2_ref.at[pl.ds(i * mid, mid), :], xbuf.at[i], x_sem.at[i]) for i in range(n_loc)]
    for i in range(n_up):
        loads.append(pltpu.make_async_copy(wup_ref.at[:, pl.ds(i * wide, wide)], up_w.at[i], w_sem.at[len(loads)]))
    for i in range(n_dp):
        loads.append(pltpu.make_async_copy(fup_ref.at[i], up_w.at[n_up + i * slim // wide, :, pl.ds(i * slim % wide, slim)], w_sem.at[len(loads)]))
    loads.append(pltpu.make_async_copy(wdn_ref, dn_w.at[pl.ds(0, d_loc), :], w_sem.at[len(loads)]))
    loads.append(pltpu.make_async_copy(fdn_ref, dn_w.at[pl.ds(d_loc, d_loc), :], w_sem.at[len(loads)]))
    for load in loads:
        load.start()
    pl.semaphore_wait(barrier, 2)

    def remote(src, dst, send, recv, to):
        return pltpu.make_async_remote_copy(src, dst, send, recv, device_id={"tp": to}, device_id_type=MESH)

    def sub(i):
        return pl.ds(pl.multiple_of(i * SUBROWS, SUBROWS), SUBROWS)

    def x_far(i):
        return remote(n2_ref.at[sub(i), :], xbuf.at[first_far + i, pl.ds(0, SUBROWS), :], fx_send.at[i], fx_recv.at[i], far)

    def x_peer(i):
        return remote(n2_ref.at[pl.ds(i * mid, mid), :], xbuf.at[n_loc + i], px_send.at[i], px_recv.at[i], peer)

    def x_pass(i):
        return remote(xbuf.at[first_far + i, pl.ds(0, SUBROWS), :], xbuf.at[first_far + i, pl.ds(SUBROWS, SUBROWS), :], fw_send.at[i], fw_recv.at[i], peer)

    def back_peer(i):
        return remote(ptl.at[n_loc + i], from_peer.at[i], lp_send.at[i], lp_recv.at[i], peer)

    def back_pre(i):
        return remote(ptl.at[first_far + i, pl.ds(SUBROWS, SUBROWS), :], pre.at[i], pr_send.at[i], pr_recv.at[i], peer)

    def back_far(i):
        return remote(ptl.at[first_far + i, pl.ds(0, SUBROWS), :], from_far.at[i], rf_send.at[i], rf_recv.at[i], far)

    for i in range(n_sub):
        x_far(i).start()
    for i in range(n_loc):
        x_peer(i).start()
    for load in loads:
        load.wait()

    def body(s, carry):
        @pl.when((s >= 2) & (s < 2 + n_sub))
        def _():
            x_far(s - 2).wait_recv()
            x_pass(s - 2).start()

        @pl.when((s >= n_loc) & (s < first_far))
        def _():
            x_peer(s - n_loc).wait_recv()

        @pl.when((s >= first_far) & (s < steps))
        def _():
            x_pass(s - first_far).wait_recv()

        @pl.when(s < steps)
        def _():
            def up(n, carry):
                hid = jnp.dot(xbuf[s], up_w[n], preferred_element_type=jnp.float32) + bias_ref[n]
                act[:, pl.ds(pl.multiple_of(n * wide, wide), wide)] = bloom_gelu(hid).astype(jnp.bfloat16)
                return carry

            lax.fori_loop(0, n_blk, up, 0)

            def down(n, carry):
                sl = pl.ds(pl.multiple_of(n * wide, wide), wide)
                ptl[s, :, sl] = jnp.dot(act[...], dn_w[:, sl], preferred_element_type=jnp.float32).astype(jnp.bfloat16)
                return carry

            lax.fori_loop(0, dn_w.shape[1] // wide, down, 0)

        @pl.when((s >= n_loc) & (s < first_far))
        def _():
            back_peer(s - n_loc).start()

        @pl.when((s >= first_far) & (s < steps))
        def _():
            back_pre(s - first_far).start()

        @pl.when(s > first_far)
        def _():
            i = s - first_far - 1
            back_pre(i).wait_recv()
            for r in range(0, SUBROWS, 32):
                sl = pl.ds(r, 32)
                ptl[first_far + i, sl, :] = (ptl[first_far + i, sl, :].astype(jnp.float32) + pre[i, sl, :].astype(jnp.float32)).astype(jnp.bfloat16)
            back_far(i).start()

        return carry

    lax.fori_loop(0, steps + 1, body, 0)

    for i in range(n_loc):
        back_peer(i).wait_recv()

    def out_copy(i):
        return pltpu.make_async_copy(obuf.at[sub(i), :], out_ref.at[sub(i), :], o_sem.at[i])

    def finish(i, carry):
        back_far(i).wait_recv()
        for r in range(0, SUBROWS, 16):
            own = pl.ds(pl.multiple_of(lax.rem(i, 2) * SUBROWS + r, 16), 16)
            row = pl.ds(pl.multiple_of(i * SUBROWS + r, 16), 16)
            total = ptl[i // 2, own, :].astype(jnp.float32) + from_peer[i // 2, own, :].astype(jnp.float32) + from_far[i, pl.ds(r, 16), :].astype(jnp.float32)
            obuf[row, :] = (r1_ref[row, :].astype(jnp.float32) + (total + bdn_ref[...])).astype(jnp.bfloat16)
        out_copy(i).start()
        return carry

    lax.fori_loop(0, n_sub, finish, 0)
    for i in range(n_loc):
        x_peer(i).wait_send()
        back_peer(i).wait_send()
    for i in range(n_sub):
        x_far(i).wait_send()
        x_pass(i).wait_send()
        back_pre(i).wait_send()
        back_far(i).wait_send()
        out_copy(i).wait()


def mlp(n2, w_up, w_down, far_up, far_down, bias, b_down, r1):
    rows, d = n2.shape
    ff = w_up.shape[1]
    wide = 512
    mid = 2 * SUBROWS
    n_loc, n_sub = rows // mid, rows // SUBROWS
    steps = 2 * n_loc + n_sub
    n_dp = far_up.shape[0]
    bf = jnp.bfloat16
    dma = pltpu.SemaphoreType.DMA
    hbm = pl.BlockSpec(memory_space=pl.ANY)
    vmem = pl.BlockSpec(memory_space=pltpu.VMEM)
    return pl.pallas_call(
        functools.partial(mlp_kernel, n_dp),
        out_shape=jax.ShapeDtypeStruct((rows, d), bf),
        in_specs=[hbm] * 5 + [vmem] * 3,
        out_specs=hbm,
        scratch_shapes=[
            pltpu.VMEM((steps, mid, d), bf), pltpu.VMEM((steps, mid, d), bf), pltpu.VMEM((2 * ff // wide, d, wide), bf), pltpu.VMEM((2 * ff, d), bf),
            pltpu.VMEM((mid, 2 * ff), bf), pltpu.VMEM((n_loc, mid, d), bf), pltpu.VMEM((n_sub, SUBROWS, d), bf), pltpu.VMEM((n_sub, SUBROWS, d), bf), pltpu.VMEM((rows, d), bf),
            dma((32,)), dma((n_loc,)), dma((n_loc,)), dma((n_loc,)), dma((n_sub,)), dma((n_sub,)), dma((n_sub,)), dma((n_sub,)),
            dma((n_loc,)), dma((n_loc,)), dma((n_sub,)), dma((n_sub,)), dma((n_sub,)), dma((n_sub,)), dma((n_sub,)),
        ],
        compiler_params=pltpu.CompilerParams(collective_id=2, has_side_effects=True, vmem_limit_bytes=61000 * 1024),
        cost_estimate=pl.CostEstimate(flops=10 ** 12, bytes_accessed=40 * 10 ** 6, transcendentals=0),
        name="mlp",
    )(n2, w_up, w_down, far_up, far_down, bias.reshape(2 * ff // wide, 1, wide), b_down[None, :], r1)


def solution(mesh):
    n_tp = mesh.shape['tp']
    n_dp = mesh.shape['dp']

    def local_step(tok_ids, pad_mask, emb_shard, ln_emb_w, ln_emb_b, ln1_w, ln1_b, w_qkv, b_qkv, w_out, b_out, ln2_w, ln2_b, w_up, b_up, w_down, b_down):
        f32 = jnp.float32
        tp_rank = lax.axis_index('tp')
        dp_rank = lax.axis_index('dp')
        n_seq, seq = tok_ids.shape
        d = emb_shard.shape[1]
        heads_loc = w_qkv.shape[1]

        def part(w, axis):
            size = w.shape[axis] // n_dp
            return lax.dynamic_slice_in_dim(w, dp_rank * size, size, axis)

        half = n_tp // 2
        swap = [(t, (t + half) % n_tp) for t in range(n_tp)]
        wo = lax.all_gather(part(w_out, 0), ('tp', 'dp'), axis=0, tiled=True)
        up_part = lax.ppermute(part(w_up, 1), 'tp', swap)
        down_part = lax.ppermute(part(w_down, 0), 'tp', swap)

        part_emb = lookup(tok_ids.reshape(-1), emb_shard, tp_rank).reshape(n_seq, seq, d)
        part_emb, up_part, down_part = lax.optimization_barrier((part_emb, up_part, down_part))
        wu = lax.all_gather(up_part, 'dp', axis=0, tiled=False)
        wd = lax.all_gather(down_part, 'dp', axis=0, tiled=True)
        ln_pack = jnp.stack([ln_emb_w, ln_emb_b, ln1_w, ln1_b]).astype(f32)
        normed_all, resid_in = chain(part_emb, ln_pack, n_tp)
        normed_all, wu, wd = lax.optimization_barrier((normed_all, wu, wd))
        qkv = (jnp.einsum('bsd,dhce->cbhse', normed_all, w_qkv, preferred_element_type=f32) + b_qkv.astype(f32).transpose(1, 0, 2)[:, None, :, None, :]).astype(jnp.bfloat16)
        all_slopes = jnp.array(alibi_slopes(heads_loc * n_tp), f32)
        head_slopes = lax.dynamic_slice_in_dim(all_slopes, tp_rank * heads_loc, heads_loc)
        context, b_all = attend(qkv, pad_mask, head_slopes, b_up.reshape(8, -1), n_tp)
        attn = jnp.einsum('bsk,kc->bsc', context, wo, preferred_element_type=f32)
        resid_mid = (resid_in.astype(f32) + (attn + b_out.astype(f32))).astype(jnp.bfloat16)
        normed2 = layer_norm(resid_mid, ln2_w, ln2_b)
        far_bias = lax.dynamic_index_in_dim(b_all, (tp_rank + half) % n_tp, 0, keepdims=False).reshape(-1)
        bias = jnp.concatenate([b_up, far_bias]).astype(f32)
        rows = n_seq * seq // n_tp
        out = mlp(normed2.reshape(rows, d), w_up, w_down, wu, wd, bias, b_down.astype(f32), resid_mid.reshape(rows, d))
        return out.reshape(n_seq, seq // n_tp, d)

    replicated = P(None)
    in_specs = (P('dp', None), P('dp', None), P('tp', None), replicated, replicated, replicated, replicated, P(None, 'tp', None, None), P('tp', None, None), P('tp', None), replicated, replicated, replicated, P(None, 'tp'), P('tp'), P('tp', None), replicated)
    return jax.shard_map(local_step, mesh=mesh, in_specs=in_specs, out_specs=P('dp', 'tp', None), check_vma=False)
```

```python
import functools
import math
import jax
import jax.numpy as jnp
from jax import lax
from jax.experimental import pallas as pl
from jax.experimental.pallas import tpu as pltpu
from jax.sharding import PartitionSpec as P

LN_EPS = 1e-5
LOG2E = 1.4426950408889634
MESH = pl.DeviceIdType.MESH


def alibi_slopes(n_heads):
    closest = 2 ** int(math.floor(math.log2(n_heads)))
    base_ratio = 2.0 ** (-(2.0 ** -(math.log2(closest) - 3)))
    extra_ratio = 2.0 ** (-(2.0 ** -(math.log2(2 * closest) - 3)))
    first_part = [base_ratio ** step_k for step_k in range(1, closest + 1)]
    second_part = [extra_ratio ** step_k for step_k in range(1, 2 * (n_heads - closest), 2)]
    return first_part + second_part


def layer_norm(values_in, ln_gain, ln_shift):
    values_in = values_in.astype(jnp.float32)
    mean_v = jnp.mean(values_in, axis=-1, keepdims=True)
    centered = values_in - mean_v
    var_v = jnp.mean(centered * centered, axis=-1, keepdims=True)
    scaled = centered * lax.rsqrt(var_v + LN_EPS)
    return (scaled * ln_gain.astype(jnp.float32) + ln_shift.astype(jnp.float32)).astype(jnp.bfloat16)


def bloom_gelu(values_in):
    return values_in * 0.5 * (1.0 + jnp.tanh(0.79788456 * values_in * (1.0 + 0.044715 * values_in * values_in)))


GROUP = 64
SUB = 32
SLOTS = 4


def lookup_kernel(tile_ref, sel_ref, table_ref, out_ref, buf, sems):
    step = pl.program_id(0)
    steps = pl.num_programs(0)

    def issue(grp):
        slot = lax.rem(grp, SLOTS)
        for i in range(GROUP):
            row = pl.multiple_of(tile_ref[grp * GROUP + i] * 8, 8)
            pltpu.make_async_copy(table_ref.at[pl.ds(row, 8), :], buf.at[slot, pl.ds(i * 8, 8), :], sems.at[slot]).start()

    @pl.when(step == 0)
    def _():
        for grp in range(SLOTS - 1):
            issue(grp)

    @pl.when(step + SLOTS - 1 < steps)
    def _():
        issue(step + SLOTS - 1)

    slot = lax.rem(step, SLOTS)
    pltpu.make_async_copy(table_ref.at[pl.ds(0, GROUP * 8), :], buf.at[slot], sems.at[slot]).wait()
    for j in range(GROUP // SUB):
        cols = lax.broadcasted_iota(jnp.int32, (SUB, SUB * 8), 1)
        onehot = (cols == sel_ref[pl.ds(j * SUB, SUB), :]).astype(jnp.float32).astype(jnp.bfloat16)
        rows = jnp.dot(onehot, buf[slot, pl.ds(j * SUB * 8, SUB * 8), :], preferred_element_type=jnp.float32)
        out_ref[pl.ds(j * SUB, SUB), :] = rows.astype(jnp.bfloat16)


def lookup(ids, table, tp_rank):
    n_tok = ids.shape[0]
    vocab_loc, d = table.shape
    loc = ids - tp_rank * vocab_loc
    held = (loc >= 0) & (loc < vocab_loc)
    spread = (jnp.arange(n_tok, dtype=jnp.int32) * 5) % (vocab_loc // 8)
    tile = jnp.where(held, loc // 8, spread)
    sel = jnp.where(held, (jnp.arange(n_tok, dtype=jnp.int32) % SUB) * 8 + loc % 8, -1)[:, None]
    return pl.pallas_call(
        lookup_kernel,
        out_shape=jax.ShapeDtypeStruct((n_tok, d), jnp.bfloat16),
        grid_spec=pltpu.PrefetchScalarGridSpec(
            num_scalar_prefetch=1,
            grid=(n_tok // GROUP,),
            in_specs=[pl.BlockSpec((GROUP, 1), lambda i, t: (i, 0)), pl.BlockSpec(memory_space=pl.ANY)],
            out_specs=pl.BlockSpec((GROUP, d), lambda i, t: (i, 0)),
            scratch_shapes=[pltpu.VMEM((SLOTS, GROUP * 8, d), jnp.bfloat16), pltpu.SemaphoreType.DMA((SLOTS,))],
        ),
        compiler_params=pltpu.CompilerParams(dimension_semantics=("arbitrary",)),
        cost_estimate=pl.CostEstimate(flops=n_tok * d * 40000, bytes_accessed=n_tok * d * 18, transcendentals=0),
        name="lookup",
    )(tile, sel, table)


CHUNK = 32
LAG = 3
LN_ROWS = 16


def norm_rows(x, gain, shift):
    n = x.shape[-1]
    mean_v = jnp.sum(x, axis=-1, keepdims=True) * (1.0 / n)
    centered = x - mean_v
    var_v = jnp.sum(centered * centered, axis=-1, keepdims=True) * (1.0 / n)
    return (centered * lax.rsqrt(var_v + LN_EPS) * gain + shift).astype(jnp.bfloat16)


def chain_kernel(n_tp, part_ref, ln_ref, a_ref, r0_ref, own, pre, rgt, lft, abuf, r0buf,
                 own_sem, pre_send, pre_recv, r_send, r_recv, l_send, l_recv, a_loc, a_send, a_recv, r0_loc, r0_send, r0_recv):
    seq = part_ref.shape[1]
    n_chunk = seq // CHUNK
    n_z = n_tp // 2
    me = lax.axis_index("tp")
    z = me // 2
    c = lax.rem(me, 2)
    peer = me + 1 - 2 * c
    pos_per = r0_ref.shape[1]
    per_dev = pos_per // CHUNK
    last = n_z - 1

    barrier = pltpu.get_barrier_semaphore()
    pl.semaphore_signal(barrier, inc=1, device_id={"tp": peer}, device_id_type=MESH)

    @pl.when(z > 0)
    def _():
        pl.semaphore_signal(barrier, inc=1, device_id={"tp": me - 2}, device_id_type=MESH)

    @pl.when(z < last)
    def _():
        pl.semaphore_signal(barrier, inc=1, device_id={"tp": me + 2}, device_id_type=MESH)

    @pl.when((z > 0) & (z < last))
    def _():
        pl.semaphore_wait(barrier, 3)

    @pl.when((z == 0) | (z == last))
    def _():
        pl.semaphore_wait(barrier, 2)

    def rows(k):
        return pl.ds(pl.multiple_of(k * CHUNK, CHUNK), CHUNK)

    def own_copy(k):
        return pltpu.make_async_copy(part_ref.at[c, rows(k), :], own.at[rows(k), :], own_sem.at[k])

    def pre_copy(k):
        return pltpu.make_async_remote_copy(part_ref.at[1 - c, rows(k), :], pre.at[rows(k), :], pre_send.at[k], pre_recv.at[k], device_id={"tp": peer}, device_id_type=MESH)

    def right_copy(src, k):
        return pltpu.make_async_remote_copy(src.at[rows(k), :], rgt.at[rows(k), :], r_send.at[k], r_recv.at[k], device_id={"tp": me + 2}, device_id_type=MESH)

    def left_copy(k):
        return pltpu.make_async_remote_copy(pre.at[rows(k), :], lft.at[rows(k), :], l_send.at[k], l_recv.at[k], device_id={"tp": me - 2}, device_id_type=MESH)

    def a_local(k):
        return pltpu.make_async_copy(abuf.at[rows(k), :], a_ref.at[c, rows(k), :], a_loc.at[k])

    def a_peer(k):
        return pltpu.make_async_remote_copy(abuf.at[rows(k), :], a_ref.at[c, rows(k), :], a_send.at[k], a_recv.at[k], device_id={"tp": peer}, device_id_type=MESH)

    def r0_local(i):
        return pltpu.make_async_copy(r0buf.at[c, rows(i), :], r0_ref.at[c, rows(i), :], r0_loc.at[i])

    def r0_peer(i):
        return pltpu.make_async_remote_copy(r0buf.at[1 - c, rows(i), :], r0_ref.at[c, rows(i), :], r0_send.at[i], r0_recv.at[i], device_id={"tp": peer}, device_id_type=MESH)

    def start(k, carry):
        own_copy(k).start()
        pre_copy(k).start()
        return carry

    lax.fori_loop(0, n_chunk, start, 0)

    def step_body(s, carry):
        @pl.when(s < n_chunk)
        def _():
            own_copy(s).wait()
            pre_copy(s).wait_recv()
            own[rows(s), :] = own[rows(s), :] + pre[rows(s), :]

        kr = s - LAG * z

        @pl.when((kr >= 0) & (kr < n_chunk))
        def _():
            @pl.when(z == 0)
            def _():
                right_copy(own, kr).start()

            @pl.when(z > 0)
            def _():
                right_copy(rgt, kr).wait_recv()
                rgt[rows(kr), :] = rgt[rows(kr), :] + own[rows(kr), :]

                @pl.when(z < last)
                def _():
                    right_copy(rgt, kr).start()

        kl = s - LAG * (last - z)

        @pl.when((kl >= 0) & (kl < n_chunk))
        def _():
            @pl.when(z < last)
            def _():
                left_copy(kl).wait_recv()

                @pl.when(z > 0)
                def _():
                    pre[rows(kl), :] = lft[rows(kl), :] + own[rows(kl), :]

            @pl.when(z == last)
            def _():
                pre[rows(kl), :] = own[rows(kl), :]

            @pl.when(z > 0)
            def _():
                left_copy(kl).start()

        kt = s - LAG * jnp.maximum(z, last - z)

        @pl.when((kt >= 0) & (kt < n_chunk))
        def _():
            base = kt * CHUNK
            first = kt - z * 2 * per_dev
            near = (first >= 0) & (first < 2 * per_dev)
            side = jnp.where(near, first // per_dev, 0)
            inner = jnp.where(near, lax.rem(first, per_dev), 0)

            def norm(i, carry):
                sl = pl.ds(pl.multiple_of(base + i * LN_ROWS, LN_ROWS), LN_ROWS)

                @pl.when(z == 0)
                def _():
                    abuf[sl, :] = own[sl, :] + lft[sl, :]

                @pl.when((z > 0) & (z < last))
                def _():
                    abuf[sl, :] = rgt[sl, :] + lft[sl, :]

                @pl.when(z == last)
                def _():
                    abuf[sl, :] = rgt[sl, :]

                r0 = norm_rows(abuf[sl, :].astype(jnp.float32), ln_ref[0:1, :], ln_ref[1:2, :])
                abuf[sl, :] = norm_rows(r0.astype(jnp.float32), ln_ref[2:3, :], ln_ref[3:4, :])

                @pl.when(near)
                def _():
                    r0buf[side, pl.ds(pl.multiple_of(inner * CHUNK + i * LN_ROWS, LN_ROWS), LN_ROWS), :] = r0

                return carry

            lax.fori_loop(0, CHUNK // LN_ROWS, norm, 0)
            a_local(kt).start()
            a_peer(kt).start()

            @pl.when(near & (side == c))
            def _():
                r0_local(inner).start()

            @pl.when(near & (side != c))
            def _():
                r0_peer(inner).start()

        return carry

    lax.fori_loop(0, n_chunk + LAG * last, step_body, 0)

    def drain(k, carry):
        pre_copy(k).wait_send()
        a_local(k).wait()
        a_peer(k).wait()

        @pl.when(z < last)
        def _():
            right_copy(rgt, k).wait_send()

        @pl.when(z > 0)
        def _():
            left_copy(k).wait_send()

        return carry

    lax.fori_loop(0, n_chunk, drain, 0)

    def drain_r0(i, carry):
        r0_local(i).wait()
        r0_peer(i).wait()
        return carry

    lax.fori_loop(0, per_dev, drain_r0, 0)


def chain(part, ln_pack, n_tp):
    n_seq, seq, d = part.shape
    n_chunk = seq // CHUNK
    per_dev = seq // n_tp // CHUNK
    dma = pltpu.SemaphoreType.DMA
    big = pltpu.VMEM((seq, d), jnp.bfloat16)
    return pl.pallas_call(
        functools.partial(chain_kernel, n_tp),
        out_shape=(jax.ShapeDtypeStruct((n_seq, seq, d), jnp.bfloat16), jax.ShapeDtypeStruct((n_seq, seq // n_tp, d), jnp.bfloat16)),
        in_specs=[pl.BlockSpec(memory_space=pl.ANY), pl.BlockSpec(memory_space=pltpu.VMEM)],
        out_specs=(pl.BlockSpec(memory_space=pl.ANY), pl.BlockSpec(memory_space=pl.ANY)),
        scratch_shapes=[big, big, big, big, big, pltpu.VMEM((2, seq // n_tp, d), jnp.bfloat16)]
        + [dma((n_chunk,))] * 10 + [dma((per_dev,))] * 3,
        compiler_params=pltpu.CompilerParams(collective_id=0, has_side_effects=True, vmem_limit_bytes=60000 * 1024),
        cost_estimate=pl.CostEstimate(flops=10 ** 12, bytes_accessed=8 * part.size, transcendentals=0),
        name="chain",
    )(part, ln_pack)


def attend_kernel(n_tp, head_dim, qkv_ref, pad_ref, slope_ref, bup_ref, ctx_ref, ball_ref, cbuf, send_sem, recv_sem, loc_sem, b_send, b_recv, b_loc):
    n_seq, heads = qkv_ref.shape[1], qkv_ref.shape[2]
    seq = qkv_ref.shape[3]
    blk = seq // n_tp
    feat = heads * head_dim
    me = lax.axis_index("tp")

    barrier = pltpu.get_barrier_semaphore()
    for r in range(1, n_tp):
        pl.semaphore_signal(barrier, inc=1, device_id={"tp": lax.rem(me + r, n_tp)}, device_id_type=MESH)
    pl.semaphore_wait(barrier, n_tp - 1)

    def cols(t):
        return pl.ds(pl.multiple_of(t * feat, feat), feat)

    def bias_copy(r):
        return pltpu.make_async_remote_copy(bup_ref, ball_ref.at[me], b_send.at[r], b_recv.at[r], device_id={"tp": lax.rem(me + r, n_tp)}, device_id_type=MESH)

    for r in range(1, n_tp):
        bias_copy(r).start()
    own_bias = pltpu.make_async_copy(bup_ref, ball_ref.at[me], b_loc.at[0])
    own_bias.start()

    def ctx_copy(b, r):
        return pltpu.make_async_remote_copy(cbuf.at[b, r], ctx_ref.at[b, :, cols(me)], send_sem.at[b, r], recv_sem.at[b, r], device_id={"tp": lax.rem(me + r, n_tp)}, device_id_type=MESH)

    def ctx_local(b):
        return pltpu.make_async_copy(cbuf.at[b, 0], ctx_ref.at[b, :, cols(me)], loc_sem.at[b])

    def one(i, carry):
        b = lax.rem(i, n_seq)
        r = n_tp - 1 - i // n_seq
        dest = lax.rem(me + r, n_tp)
        for j in range(n_tp):
            @pl.when(dest == j)
            def _(j=j):
                span = (j + 1) * blk
                lo = j * blk
                key_pos = lax.broadcasted_iota(jnp.int32, (1, span), 1)
                key_ok = pad_ref[b, :, 0:span] == 1
                row_in = lax.broadcasted_iota(jnp.int32, (blk, blk), 0)
                col_in = lax.broadcasted_iota(jnp.int32, (blk, blk), 1)
                diag_ok = ((col_in < row_in) & (pad_ref[b, :, lo:span] == 1)) | (col_in == row_in)
                for h in range(heads):
                    slope = slope_ref[0, h] * LOG2E
                    rel = slope * (key_pos - lo).astype(jnp.float32)
                    far = jnp.where(key_ok, rel, -1e30)
                    q = qkv_ref[0, b, h, lo:span, :]
                    scale = head_dim ** -0.5 * LOG2E
                    diag = lax.dot_general(q, qkv_ref[1, b, h, lo:span, :], (((1,), (1,)), ((), ())), preferred_element_type=jnp.float32)
                    diag = jnp.where(diag_ok, diag * scale + rel[:, lo:span], -1e30)
                    top = jnp.max(diag, axis=-1, keepdims=True)
                    if j:
                        past = lax.dot_general(q, qkv_ref[1, b, h, 0:lo, :], (((1,), (1,)), ((), ())), preferred_element_type=jnp.float32)
                        past = past * scale + far[:, 0:lo]
                        top = jnp.maximum(top, jnp.max(past, axis=-1, keepdims=True))
                        past = jnp.exp2(past - top)
                    diag = jnp.exp2(diag - top)
                    total = jnp.sum(diag, axis=-1, keepdims=True)
                    if j:
                        total = total + jnp.sum(past, axis=-1, keepdims=True)
                    inv = 1.0 / total
                    out = jnp.dot((diag * inv).astype(jnp.bfloat16), qkv_ref[2, b, h, lo:span, :], preferred_element_type=jnp.float32)
                    if j:
                        out = out + jnp.dot((past * inv).astype(jnp.bfloat16), qkv_ref[2, b, h, 0:lo, :], preferred_element_type=jnp.float32)
                    cbuf[b, r, :, h * head_dim:(h + 1) * head_dim] = out.astype(jnp.bfloat16)

        @pl.when(r > 0)
        def _():
            ctx_copy(b, r).start()

        @pl.when(r == 0)
        def _():
            ctx_local(b).start()

        return carry

    lax.fori_loop(0, n_seq * n_tp, one, 0)

    for b in range(n_seq):
        ctx_local(b).wait()
        for r in range(1, n_tp):
            ctx_copy(b, r).wait()
    own_bias.wait()
    for r in range(1, n_tp):
        bias_copy(r).wait()


def attend(qkv, pad_mask, slopes, b_up, n_tp):
    _, n_seq, heads, seq, head_dim = qkv.shape
    blk = seq // n_tp
    feat = heads * head_dim
    dma = pltpu.SemaphoreType.DMA
    vmem = pl.BlockSpec(memory_space=pltpu.VMEM)
    return pl.pallas_call(
        functools.partial(attend_kernel, n_tp, head_dim),
        out_shape=(jax.ShapeDtypeStruct((n_seq, blk, n_tp * feat), jnp.bfloat16), jax.ShapeDtypeStruct((n_tp,) + b_up.shape, jnp.bfloat16)),
        in_specs=[vmem, vmem, pl.BlockSpec(memory_space=pltpu.SMEM), vmem],
        out_specs=(pl.BlockSpec(memory_space=pl.ANY), pl.BlockSpec(memory_space=pl.ANY)),
        scratch_shapes=[pltpu.VMEM((n_seq, n_tp, blk, feat), jnp.bfloat16), dma((n_seq, n_tp)), dma((n_seq, n_tp)), dma((n_seq,)), dma((n_tp,)), dma((n_tp,)), dma((1,))],
        compiler_params=pltpu.CompilerParams(collective_id=1, has_side_effects=True, vmem_limit_bytes=56000 * 1024),
        cost_estimate=pl.CostEstimate(flops=30 * 10 ** 9, bytes_accessed=2 * qkv.size, transcendentals=seq * seq * 2),
        name="attend",
    )(qkv, pad_mask[:, None, :], slopes[None, :], b_up)


SUBROWS = 128


def mlp_kernel(n_dp, n2_ref, wup_ref, wdn_ref, fup_ref, fdn_ref, bias_ref, bdn_ref, r1_ref, out_ref,
               xbuf, ptl, up_w, dn_w, act, from_peer, pre, from_far, obuf,
               w_sem, x_sem, px_send, px_recv, fx_send, fx_recv, fw_send, fw_recv, lp_send, lp_recv, pr_send, pr_recv, rf_send, rf_recv, o_sem):
    me = lax.axis_index("tp")
    peer = me + 1 - 2 * lax.rem(me, 2)
    far = me + 2 - 4 * lax.rem(me // 2, 2)
    mid = 2 * SUBROWS
    n_loc = n2_ref.shape[0] // mid
    n_sub = n2_ref.shape[0] // SUBROWS
    steps = 2 * n_loc + n_sub
    first_far = 2 * n_loc
    wide = up_w.shape[2]
    n_up = wup_ref.shape[1] // wide
    n_blk = up_w.shape[0]
    d_loc = wdn_ref.shape[0]
    slim = fup_ref.shape[2]

    barrier = pltpu.get_barrier_semaphore()
    pl.semaphore_signal(barrier, inc=1, device_id={"tp": peer}, device_id_type=MESH)
    pl.semaphore_signal(barrier, inc=1, device_id={"tp": far}, device_id_type=MESH)

    loads = [pltpu.make_async_copy(n2_ref.at[pl.ds(i * mid, mid), :], xbuf.at[i], x_sem.at[i]) for i in range(n_loc)]
    for i in range(n_up):
        loads.append(pltpu.make_async_copy(wup_ref.at[:, pl.ds(i * wide, wide)], up_w.at[i], w_sem.at[len(loads)]))
    for i in range(n_dp):
        loads.append(pltpu.make_async_copy(fup_ref.at[i], up_w.at[n_up + i * slim // wide, :, pl.ds(i * slim % wide, slim)], w_sem.at[len(loads)]))
    loads.append(pltpu.make_async_copy(wdn_ref, dn_w.at[pl.ds(0, d_loc), :], w_sem.at[len(loads)]))
    loads.append(pltpu.make_async_copy(fdn_ref, dn_w.at[pl.ds(d_loc, d_loc), :], w_sem.at[len(loads)]))
    for load in loads:
        load.start()
    pl.semaphore_wait(barrier, 2)

    def remote(src, dst, send, recv, to):
        return pltpu.make_async_remote_copy(src, dst, send, recv, device_id={"tp": to}, device_id_type=MESH)

    def sub(i):
        return pl.ds(pl.multiple_of(i * SUBROWS, SUBROWS), SUBROWS)

    def x_far(i):
        return remote(n2_ref.at[sub(i), :], xbuf.at[first_far + i, pl.ds(0, SUBROWS), :], fx_send.at[i], fx_recv.at[i], far)

    def x_peer(i):
        return remote(n2_ref.at[pl.ds(i * mid, mid), :], xbuf.at[n_loc + i], px_send.at[i], px_recv.at[i], peer)

    def x_pass(i):
        return remote(xbuf.at[first_far + i, pl.ds(0, SUBROWS), :], xbuf.at[first_far + i, pl.ds(SUBROWS, SUBROWS), :], fw_send.at[i], fw_recv.at[i], peer)

    def back_peer(i):
        return remote(ptl.at[n_loc + i], from_peer.at[i], lp_send.at[i], lp_recv.at[i], peer)

    def back_pre(i):
        return remote(ptl.at[first_far + i, pl.ds(SUBROWS, SUBROWS), :], pre.at[i], pr_send.at[i], pr_recv.at[i], peer)

    def back_far(i):
        return remote(ptl.at[first_far + i, pl.ds(0, SUBROWS), :], from_far.at[i], rf_send.at[i], rf_recv.at[i], far)

    for i in range(n_sub):
        x_far(i).start()
    for i in range(n_loc):
        x_peer(i).start()
    for load in loads:
        load.wait()

    def body(s, carry):
        @pl.when((s >= 2) & (s < 2 + n_sub))
        def _():
            x_far(s - 2).wait_recv()
            x_pass(s - 2).start()

        @pl.when((s >= n_loc) & (s < first_far))
        def _():
            x_peer(s - n_loc).wait_recv()

        @pl.when((s >= first_far) & (s < steps))
        def _():
            x_pass(s - first_far).wait_recv()

        @pl.when(s < steps)
        def _():
            def up(n, carry):
                hid = jnp.dot(xbuf[s], up_w[n], preferred_element_type=jnp.float32) + bias_ref[n]
                act[:, pl.ds(pl.multiple_of(n * wide, wide), wide)] = bloom_gelu(hid).astype(jnp.bfloat16)
                return carry

            lax.fori_loop(0, n_blk, up, 0)

            def down(n, carry):
                sl = pl.ds(pl.multiple_of(n * wide, wide), wide)
                ptl[s, :, sl] = jnp.dot(act[...], dn_w[:, sl], preferred_element_type=jnp.float32).astype(jnp.bfloat16)
                return carry

            lax.fori_loop(0, dn_w.shape[1] // wide, down, 0)

        @pl.when((s >= n_loc) & (s < first_far))
        def _():
            back_peer(s - n_loc).start()

        @pl.when((s >= first_far) & (s < steps))
        def _():
            back_pre(s - first_far).start()

        @pl.when(s > first_far)
        def _():
            i = s - first_far - 1
            back_pre(i).wait_recv()
            for r in range(0, SUBROWS, 32):
                sl = pl.ds(r, 32)
                ptl[first_far + i, sl, :] = (ptl[first_far + i, sl, :].astype(jnp.float32) + pre[i, sl, :].astype(jnp.float32)).astype(jnp.bfloat16)
            back_far(i).start()

        return carry

    lax.fori_loop(0, steps + 1, body, 0)

    for i in range(n_loc):
        back_peer(i).wait_recv()

    def out_copy(i):
        return pltpu.make_async_copy(obuf.at[sub(i), :], out_ref.at[sub(i), :], o_sem.at[i])

    def finish(i, carry):
        back_far(i).wait_recv()
        for r in range(0, SUBROWS, 16):
            own = pl.ds(pl.multiple_of(lax.rem(i, 2) * SUBROWS + r, 16), 16)
            row = pl.ds(pl.multiple_of(i * SUBROWS + r, 16), 16)
            total = ptl[i // 2, own, :].astype(jnp.float32) + from_peer[i // 2, own, :].astype(jnp.float32) + from_far[i, pl.ds(r, 16), :].astype(jnp.float32)
            obuf[row, :] = (r1_ref[row, :].astype(jnp.float32) + (total + bdn_ref[...])).astype(jnp.bfloat16)
        out_copy(i).start()
        return carry

    lax.fori_loop(0, n_sub, finish, 0)
    for i in range(n_loc):
        x_peer(i).wait_send()
        back_peer(i).wait_send()
    for i in range(n_sub):
        x_far(i).wait_send()
        x_pass(i).wait_send()
        back_pre(i).wait_send()
        back_far(i).wait_send()
        out_copy(i).wait()


def mlp(n2, w_up, w_down, far_up, far_down, bias, b_down, r1):
    rows, d = n2.shape
    ff = w_up.shape[1]
    wide = 512
    mid = 2 * SUBROWS
    n_loc, n_sub = rows // mid, rows // SUBROWS
    steps = 2 * n_loc + n_sub
    n_dp = far_up.shape[0]
    bf = jnp.bfloat16
    dma = pltpu.SemaphoreType.DMA
    hbm = pl.BlockSpec(memory_space=pl.ANY)
    vmem = pl.BlockSpec(memory_space=pltpu.VMEM)
    return pl.pallas_call(
        functools.partial(mlp_kernel, n_dp),
        out_shape=jax.ShapeDtypeStruct((rows, d), bf),
        in_specs=[hbm] * 5 + [vmem] * 3,
        out_specs=hbm,
        scratch_shapes=[
            pltpu.VMEM((steps, mid, d), bf), pltpu.VMEM((steps, mid, d), bf), pltpu.VMEM((2 * ff // wide, d, wide), bf), pltpu.VMEM((2 * ff, d), bf),
            pltpu.VMEM((mid, 2 * ff), bf), pltpu.VMEM((n_loc, mid, d), bf), pltpu.VMEM((n_sub, SUBROWS, d), bf), pltpu.VMEM((n_sub, SUBROWS, d), bf), pltpu.VMEM((rows, d), bf),
            dma((32,)), dma((n_loc,)), dma((n_loc,)), dma((n_loc,)), dma((n_sub,)), dma((n_sub,)), dma((n_sub,)), dma((n_sub,)),
            dma((n_loc,)), dma((n_loc,)), dma((n_sub,)), dma((n_sub,)), dma((n_sub,)), dma((n_sub,)), dma((n_sub,)),
        ],
        compiler_params=pltpu.CompilerParams(collective_id=2, has_side_effects=True, vmem_limit_bytes=61000 * 1024),
        cost_estimate=pl.CostEstimate(flops=10 ** 12, bytes_accessed=40 * 10 ** 6, transcendentals=0),
        name="mlp",
    )(n2, w_up, w_down, far_up, far_down, bias.reshape(2 * ff // wide, 1, wide), b_down[None, :], r1)


def solution(mesh):
    n_tp = mesh.shape['tp']
    n_dp = mesh.shape['dp']

    def local_step(tok_ids, pad_mask, emb_shard, ln_emb_w, ln_emb_b, ln1_w, ln1_b, w_qkv, b_qkv, w_out, b_out, ln2_w, ln2_b, w_up, b_up, w_down, b_down):
        f32 = jnp.float32
        tp_rank = lax.axis_index('tp')
        dp_rank = lax.axis_index('dp')
        n_seq, seq = tok_ids.shape
        d = emb_shard.shape[1]
        heads_loc = w_qkv.shape[1]

        def part(w, axis):
            size = w.shape[axis] // n_dp
            return lax.dynamic_slice_in_dim(w, dp_rank * size, size, axis)

        half = n_tp // 2
        swap = [(t, (t + half) % n_tp) for t in range(n_tp)]
        wo = lax.all_gather(part(w_out, 0), ('tp', 'dp'), axis=0, tiled=True)
        up_part = lax.ppermute(part(w_up, 1), 'tp', swap)
        down_part = lax.ppermute(part(w_down, 0), 'tp', swap)

        part_emb = lookup(tok_ids.reshape(-1), emb_shard, tp_rank).reshape(n_seq, seq, d)
        part_emb, up_part = lax.optimization_barrier((part_emb, up_part))
        wu = lax.all_gather(up_part, 'dp', axis=0, tiled=False)
        ln_pack = jnp.stack([ln_emb_w, ln_emb_b, ln1_w, ln1_b]).astype(f32)
        normed_all, resid_in = chain(part_emb, ln_pack, n_tp)
        normed_all, wu, wo, down_part = lax.optimization_barrier((normed_all, wu, wo, down_part))
        wd = lax.all_gather(down_part, 'dp', axis=0, tiled=True)
        qkv = (jnp.einsum('bsd,dhce->cbhse', normed_all, w_qkv, preferred_element_type=f32) + b_qkv.astype(f32).transpose(1, 0, 2)[:, None, :, None, :]).astype(jnp.bfloat16)
        all_slopes = jnp.array(alibi_slopes(heads_loc * n_tp), f32)
        head_slopes = lax.dynamic_slice_in_dim(all_slopes, tp_rank * heads_loc, heads_loc)
        context, b_all = attend(qkv, pad_mask, head_slopes, b_up.reshape(8, -1), n_tp)
        context, wd = lax.optimization_barrier((context, wd))
        attn = jnp.einsum('bsk,kc->bsc', context, wo, preferred_element_type=f32)
        resid_mid = (resid_in.astype(f32) + (attn + b_out.astype(f32))).astype(jnp.bfloat16)
        normed2 = layer_norm(resid_mid, ln2_w, ln2_b)
        far_bias = lax.dynamic_index_in_dim(b_all, (tp_rank + half) % n_tp, 0, keepdims=False).reshape(-1)
        bias = jnp.concatenate([b_up, far_bias]).astype(f32)
        rows = n_seq * seq // n_tp
        out = mlp(normed2.reshape(rows, d), w_up, w_down, wu, wd, bias, b_down.astype(f32), resid_mid.reshape(rows, d))
        return out.reshape(n_seq, seq // n_tp, d)

    replicated = P(None)
    in_specs = (P('dp', None), P('dp', None), P('tp', None), replicated, replicated, replicated, replicated, P(None, 'tp', None, None), P('tp', None, None), P('tp', None), replicated, replicated, replicated, P(None, 'tp'), P('tp'), P('tp', None), replicated)
    return jax.shard_map(local_step, mesh=mesh, in_specs=in_specs, out_specs=P('dp', 'tp', None), check_vma=False)
```

```python
import functools
import math
import jax
import jax.numpy as jnp
from jax import lax
from jax.experimental import pallas as pl
from jax.experimental.pallas import tpu as pltpu
from jax.sharding import PartitionSpec as P

LN_EPS = 1e-5
LOG2E = 1.4426950408889634
MESH = pl.DeviceIdType.MESH


def alibi_slopes(n_heads):
    closest = 2 ** int(math.floor(math.log2(n_heads)))
    base_ratio = 2.0 ** (-(2.0 ** -(math.log2(closest) - 3)))
    extra_ratio = 2.0 ** (-(2.0 ** -(math.log2(2 * closest) - 3)))
    first_part = [base_ratio ** step_k for step_k in range(1, closest + 1)]
    second_part = [extra_ratio ** step_k for step_k in range(1, 2 * (n_heads - closest), 2)]
    return first_part + second_part


def bloom_gelu(values_in):
    return values_in * 0.5 * (1.0 + jnp.tanh(0.79788456 * values_in * (1.0 + 0.044715 * values_in * values_in)))


GROUP = 64
SUB = 32
SLOTS = 4


def lookup_kernel(tile_ref, sel_ref, table_ref, out_ref, buf, sems):
    step = pl.program_id(0)
    steps = pl.num_programs(0)

    def issue(grp):
        slot = lax.rem(grp, SLOTS)
        for i in range(GROUP):
            row = pl.multiple_of(tile_ref[grp * GROUP + i] * 8, 8)
            pltpu.make_async_copy(table_ref.at[pl.ds(row, 8), :], buf.at[slot, pl.ds(i * 8, 8), :], sems.at[slot]).start()

    @pl.when(step == 0)
    def _():
        for grp in range(SLOTS - 1):
            issue(grp)

    @pl.when(step + SLOTS - 1 < steps)
    def _():
        issue(step + SLOTS - 1)

    slot = lax.rem(step, SLOTS)
    pltpu.make_async_copy(table_ref.at[pl.ds(0, GROUP * 8), :], buf.at[slot], sems.at[slot]).wait()
    for j in range(GROUP // SUB):
        cols = lax.broadcasted_iota(jnp.int32, (SUB, SUB * 8), 1)
        onehot = (cols == sel_ref[pl.ds(j * SUB, SUB), :]).astype(jnp.float32).astype(jnp.bfloat16)
        rows = jnp.dot(onehot, buf[slot, pl.ds(j * SUB * 8, SUB * 8), :], preferred_element_type=jnp.float32)
        out_ref[pl.ds(j * SUB, SUB), :] = rows.astype(jnp.bfloat16)


def lookup(ids, table, tp_rank):
    n_tok = ids.shape[0]
    vocab_loc, d = table.shape
    loc = ids - tp_rank * vocab_loc
    held = (loc >= 0) & (loc < vocab_loc)
    spread = (jnp.arange(n_tok, dtype=jnp.int32) * 5) % (vocab_loc // 8)
    tile = jnp.where(held, loc // 8, spread)
    sel = jnp.where(held, (jnp.arange(n_tok, dtype=jnp.int32) % SUB) * 8 + loc % 8, -1)[:, None]
    return pl.pallas_call(
        lookup_kernel,
        out_shape=jax.ShapeDtypeStruct((n_tok, d), jnp.bfloat16),
        grid_spec=pltpu.PrefetchScalarGridSpec(
            num_scalar_prefetch=1,
            grid=(n_tok // GROUP,),
            in_specs=[pl.BlockSpec((GROUP, 1), lambda i, t: (i, 0)), pl.BlockSpec(memory_space=pl.ANY)],
            out_specs=pl.BlockSpec((GROUP, d), lambda i, t: (i, 0)),
            scratch_shapes=[pltpu.VMEM((SLOTS, GROUP * 8, d), jnp.bfloat16), pltpu.SemaphoreType.DMA((SLOTS,))],
        ),
        compiler_params=pltpu.CompilerParams(dimension_semantics=("arbitrary",)),
        cost_estimate=pl.CostEstimate(flops=n_tok * d * 40000, bytes_accessed=n_tok * d * 18, transcendentals=0),
        name="lookup",
    )(tile, sel, table)


CHUNK = 32
LAG = 3
LN_ROWS = 16


def norm_rows(x, gain, shift):
    n = x.shape[-1]
    mean_v = jnp.sum(x, axis=-1, keepdims=True) * (1.0 / n)
    centered = x - mean_v
    var_v = jnp.sum(centered * centered, axis=-1, keepdims=True) * (1.0 / n)
    return (centered * lax.rsqrt(var_v + LN_EPS) * gain + shift).astype(jnp.bfloat16)


def chain_kernel(n_tp, part_ref, ln_ref, a_ref, r0_ref, own, pre, rgt, lft, abuf, r0buf,
                 own_sem, pre_send, pre_recv, r_send, r_recv, l_send, l_recv, a_loc, a_send, a_recv, r0_loc, r0_send, r0_recv):
    seq = part_ref.shape[1]
    n_chunk = seq // CHUNK
    n_z = n_tp // 2
    me = lax.axis_index("tp")
    z = me // 2
    c = lax.rem(me, 2)
    peer = me + 1 - 2 * c
    pos_per = r0_ref.shape[1]
    per_dev = pos_per // CHUNK
    last = n_z - 1

    barrier = pltpu.get_barrier_semaphore()
    pl.semaphore_signal(barrier, inc=1, device_id={"tp": peer}, device_id_type=MESH)

    @pl.when(z > 0)
    def _():
        pl.semaphore_signal(barrier, inc=1, device_id={"tp": me - 2}, device_id_type=MESH)

    @pl.when(z < last)
    def _():
        pl.semaphore_signal(barrier, inc=1, device_id={"tp": me + 2}, device_id_type=MESH)

    @pl.when((z > 0) & (z < last))
    def _():
        pl.semaphore_wait(barrier, 3)

    @pl.when((z == 0) | (z == last))
    def _():
        pl.semaphore_wait(barrier, 2)

    def rows(k):
        return pl.ds(pl.multiple_of(k * CHUNK, CHUNK), CHUNK)

    def own_copy(k):
        return pltpu.make_async_copy(part_ref.at[c, rows(k), :], own.at[rows(k), :], own_sem.at[k])

    def pre_copy(k):
        return pltpu.make_async_remote_copy(part_ref.at[1 - c, rows(k), :], pre.at[rows(k), :], pre_send.at[k], pre_recv.at[k], device_id={"tp": peer}, device_id_type=MESH)

    def right_copy(src, k):
        return pltpu.make_async_remote_copy(src.at[rows(k), :], rgt.at[rows(k), :], r_send.at[k], r_recv.at[k], device_id={"tp": me + 2}, device_id_type=MESH)

    def left_copy(k):
        return pltpu.make_async_remote_copy(pre.at[rows(k), :], lft.at[rows(k), :], l_send.at[k], l_recv.at[k], device_id={"tp": me - 2}, device_id_type=MESH)

    def a_local(k):
        return pltpu.make_async_copy(abuf.at[rows(k), :], a_ref.at[c, rows(k), :], a_loc.at[k])

    def a_peer(k):
        return pltpu.make_async_remote_copy(abuf.at[rows(k), :], a_ref.at[c, rows(k), :], a_send.at[k], a_recv.at[k], device_id={"tp": peer}, device_id_type=MESH)

    def r0_local(i):
        return pltpu.make_async_copy(r0buf.at[c, rows(i), :], r0_ref.at[c, rows(i), :], r0_loc.at[i])

    def r0_peer(i):
        return pltpu.make_async_remote_copy(r0buf.at[1 - c, rows(i), :], r0_ref.at[c, rows(i), :], r0_send.at[i], r0_recv.at[i], device_id={"tp": peer}, device_id_type=MESH)

    def start(k, carry):
        own_copy(k).start()
        pre_copy(k).start()
        return carry

    lax.fori_loop(0, n_chunk, start, 0)

    def step_body(s, carry):
        @pl.when(s < n_chunk)
        def _():
            own_copy(s).wait()
            pre_copy(s).wait_recv()
            own[rows(s), :] = own[rows(s), :] + pre[rows(s), :]

        kr = s - LAG * z

        @pl.when((kr >= 0) & (kr < n_chunk))
        def _():
            @pl.when(z == 0)
            def _():
                right_copy(own, kr).start()

            @pl.when(z > 0)
            def _():
                right_copy(rgt, kr).wait_recv()
                rgt[rows(kr), :] = rgt[rows(kr), :] + own[rows(kr), :]

                @pl.when(z < last)
                def _():
                    right_copy(rgt, kr).start()

        kl = s - LAG * (last - z)

        @pl.when((kl >= 0) & (kl < n_chunk))
        def _():
            @pl.when(z < last)
            def _():
                left_copy(kl).wait_recv()

                @pl.when(z > 0)
                def _():
                    pre[rows(kl), :] = lft[rows(kl), :] + own[rows(kl), :]

            @pl.when(z == last)
            def _():
                pre[rows(kl), :] = own[rows(kl), :]

            @pl.when(z > 0)
            def _():
                left_copy(kl).start()

        kt = s - LAG * jnp.maximum(z, last - z)

        @pl.when((kt >= 0) & (kt < n_chunk))
        def _():
            base = kt * CHUNK
            first = kt - z * 2 * per_dev
            near = (first >= 0) & (first < 2 * per_dev)
            side = jnp.where(near, first // per_dev, 0)
            inner = jnp.where(near, lax.rem(first, per_dev), 0)

            def norm(i, carry):
                sl = pl.ds(pl.multiple_of(base + i * LN_ROWS, LN_ROWS), LN_ROWS)

                @pl.when(z == 0)
                def _():
                    abuf[sl, :] = own[sl, :] + lft[sl, :]

                @pl.when((z > 0) & (z < last))
                def _():
                    abuf[sl, :] = rgt[sl, :] + lft[sl, :]

                @pl.when(z == last)
                def _():
                    abuf[sl, :] = rgt[sl, :]

                r0 = norm_rows(abuf[sl, :].astype(jnp.float32), ln_ref[0:1, :], ln_ref[1:2, :])
                abuf[sl, :] = norm_rows(r0.astype(jnp.float32), ln_ref[2:3, :], ln_ref[3:4, :])

                @pl.when(near)
                def _():
                    r0buf[side, pl.ds(pl.multiple_of(inner * CHUNK + i * LN_ROWS, LN_ROWS), LN_ROWS), :] = r0

                return carry

            lax.fori_loop(0, CHUNK // LN_ROWS, norm, 0)
            a_local(kt).start()
            a_peer(kt).start()

            @pl.when(near & (side == c))
            def _():
                r0_local(inner).start()

            @pl.when(near & (side != c))
            def _():
                r0_peer(inner).start()

        return carry

    lax.fori_loop(0, n_chunk + LAG * last, step_body, 0)

    def drain(k, carry):
        pre_copy(k).wait_send()
        a_local(k).wait()
        a_peer(k).wait()

        @pl.when(z < last)
        def _():
            right_copy(rgt, k).wait_send()

        @pl.when(z > 0)
        def _():
            left_copy(k).wait_send()

        return carry

    lax.fori_loop(0, n_chunk, drain, 0)

    def drain_r0(i, carry):
        r0_local(i).wait()
        r0_peer(i).wait()
        return carry

    lax.fori_loop(0, per_dev, drain_r0, 0)


def chain(part, ln_pack, n_tp):
    n_seq, seq, d = part.shape
    n_chunk = seq // CHUNK
    per_dev = seq // n_tp // CHUNK
    dma = pltpu.SemaphoreType.DMA
    big = pltpu.VMEM((seq, d), jnp.bfloat16)
    return pl.pallas_call(
        functools.partial(chain_kernel, n_tp),
        out_shape=(jax.ShapeDtypeStruct((n_seq, seq, d), jnp.bfloat16), jax.ShapeDtypeStruct((n_seq, seq // n_tp, d), jnp.bfloat16)),
        in_specs=[pl.BlockSpec(memory_space=pl.ANY), pl.BlockSpec(memory_space=pltpu.VMEM)],
        out_specs=(pl.BlockSpec(memory_space=pl.ANY), pl.BlockSpec(memory_space=pl.ANY)),
        scratch_shapes=[big, big, big, big, big, pltpu.VMEM((2, seq // n_tp, d), jnp.bfloat16)]
        + [dma((n_chunk,))] * 10 + [dma((per_dev,))] * 3,
        compiler_params=pltpu.CompilerParams(collective_id=0, has_side_effects=True, vmem_limit_bytes=60000 * 1024),
        cost_estimate=pl.CostEstimate(flops=10 ** 12, bytes_accessed=8 * part.size, transcendentals=0),
        name="chain",
    )(part, ln_pack)


def attend_kernel(n_tp, head_dim, qkv_ref, pad_ref, slope_ref, bup_ref, ctx_ref, ball_ref, cbuf, send_sem, recv_sem, loc_sem, b_send, b_recv, b_loc):
    n_seq, heads = qkv_ref.shape[1], qkv_ref.shape[2]
    seq = qkv_ref.shape[3]
    blk = seq // n_tp
    feat = heads * head_dim
    me = lax.axis_index("tp")

    barrier = pltpu.get_barrier_semaphore()
    for r in range(1, n_tp):
        pl.semaphore_signal(barrier, inc=1, device_id={"tp": lax.rem(me + r, n_tp)}, device_id_type=MESH)
    pl.semaphore_wait(barrier, n_tp - 1)

    def cols(t):
        return pl.ds(pl.multiple_of(t * feat, feat), feat)

    def bias_copy(r):
        return pltpu.make_async_remote_copy(bup_ref, ball_ref.at[me], b_send.at[r], b_recv.at[r], device_id={"tp": lax.rem(me + r, n_tp)}, device_id_type=MESH)

    for r in range(1, n_tp):
        bias_copy(r).start()
    own_bias = pltpu.make_async_copy(bup_ref, ball_ref.at[me], b_loc.at[0])
    own_bias.start()

    def ctx_copy(b, r):
        return pltpu.make_async_remote_copy(cbuf.at[b, r], ctx_ref.at[b, :, cols(me)], send_sem.at[b, r], recv_sem.at[b, r], device_id={"tp": lax.rem(me + r, n_tp)}, device_id_type=MESH)

    def ctx_local(b):
        return pltpu.make_async_copy(cbuf.at[b, 0], ctx_ref.at[b, :, cols(me)], loc_sem.at[b])

    def one(i, carry):
        b = lax.rem(i, n_seq)
        r = n_tp - 1 - i // n_seq
        dest = lax.rem(me + r, n_tp)
        for j in range(n_tp):
            @pl.when(dest == j)
            def _(j=j):
                span = (j + 1) * blk
                lo = j * blk
                key_pos = lax.broadcasted_iota(jnp.int32, (1, span), 1)
                key_ok = pad_ref[b, :, 0:span] == 1
                row_in = lax.broadcasted_iota(jnp.int32, (blk, blk), 0)
                col_in = lax.broadcasted_iota(jnp.int32, (blk, blk), 1)
                diag_ok = ((col_in < row_in) & (pad_ref[b, :, lo:span] == 1)) | (col_in == row_in)
                for h in range(heads):
                    slope = slope_ref[0, h] * LOG2E
                    rel = slope * (key_pos - lo).astype(jnp.float32)
                    far = jnp.where(key_ok, rel, -1e30)
                    q = qkv_ref[0, b, h, lo:span, :]
                    scale = head_dim ** -0.5 * LOG2E
                    diag = lax.dot_general(q, qkv_ref[1, b, h, lo:span, :], (((1,), (1,)), ((), ())), preferred_element_type=jnp.float32)
                    diag = jnp.where(diag_ok, diag * scale + rel[:, lo:span], -1e30)
                    top = jnp.max(diag, axis=-1, keepdims=True)
                    if j:
                        past = lax.dot_general(q, qkv_ref[1, b, h, 0:lo, :], (((1,), (1,)), ((), ())), preferred_element_type=jnp.float32)
                        past = past * scale + far[:, 0:lo]
                        top = jnp.maximum(top, jnp.max(past, axis=-1, keepdims=True))
                        past = jnp.exp2(past - top)
                    diag = jnp.exp2(diag - top)
                    total = jnp.sum(diag, axis=-1, keepdims=True)
                    if j:
                        total = total + jnp.sum(past, axis=-1, keepdims=True)
                    inv = 1.0 / total
                    out = jnp.dot((diag * inv).astype(jnp.bfloat16), qkv_ref[2, b, h, lo:span, :], preferred_element_type=jnp.float32)
                    if j:
                        out = out + jnp.dot((past * inv).astype(jnp.bfloat16), qkv_ref[2, b, h, 0:lo, :], preferred_element_type=jnp.float32)
                    cbuf[b, r, :, h * head_dim:(h + 1) * head_dim] = out.astype(jnp.bfloat16)

        @pl.when(r > 0)
        def _():
            ctx_copy(b, r).start()

        @pl.when(r == 0)
        def _():
            ctx_local(b).start()

        return carry

    lax.fori_loop(0, n_seq * n_tp, one, 0)

    for b in range(n_seq):
        ctx_local(b).wait()
        for r in range(1, n_tp):
            ctx_copy(b, r).wait()
    own_bias.wait()
    for r in range(1, n_tp):
        bias_copy(r).wait()


def attend(qkv, pad_mask, slopes, b_up, n_tp):
    _, n_seq, heads, seq, head_dim = qkv.shape
    blk = seq // n_tp
    feat = heads * head_dim
    dma = pltpu.SemaphoreType.DMA
    vmem = pl.BlockSpec(memory_space=pltpu.VMEM)
    return pl.pallas_call(
        functools.partial(attend_kernel, n_tp, head_dim),
        out_shape=(jax.ShapeDtypeStruct((n_seq, blk, n_tp * feat), jnp.bfloat16), jax.ShapeDtypeStruct((n_tp,) + b_up.shape, jnp.bfloat16)),
        in_specs=[vmem, vmem, pl.BlockSpec(memory_space=pltpu.SMEM), vmem],
        out_specs=(pl.BlockSpec(memory_space=pl.ANY), pl.BlockSpec(memory_space=pl.ANY)),
        scratch_shapes=[pltpu.VMEM((n_seq, n_tp, blk, feat), jnp.bfloat16), dma((n_seq, n_tp)), dma((n_seq, n_tp)), dma((n_seq,)), dma((n_tp,)), dma((n_tp,)), dma((1,))],
        compiler_params=pltpu.CompilerParams(collective_id=1, has_side_effects=True, vmem_limit_bytes=56000 * 1024),
        cost_estimate=pl.CostEstimate(flops=30 * 10 ** 9, bytes_accessed=2 * qkv.size, transcendentals=seq * seq * 2),
        name="attend",
    )(qkv, pad_mask[:, None, :], slopes[None, :], b_up)


SUBROWS = 128


def mlp_kernel(n_dp, ctx_ref, r0_ref, wo_ref, wup_ref, wdn_ref, fup_ref, fdn_ref, bias_ref, vec_ref, out_ref,
               ctx, r0, r1, wo_w, xbuf, ptl, up_w, dn_w, act, from_peer, pre, from_far, obuf,
               w_sem, x_sem, px_send, px_recv, fx_send, fx_recv, fw_send, fw_recv, lp_send, lp_recv, pr_send, pr_recv, rf_send, rf_recv, o_sem):
    me = lax.axis_index("tp")
    peer = me + 1 - 2 * lax.rem(me, 2)
    far = me + 2 - 4 * lax.rem(me // 2, 2)
    mid = 2 * SUBROWS
    n_loc = ctx.shape[0] // mid
    n_sub = ctx.shape[0] // SUBROWS
    steps = 2 * n_loc + n_sub
    first_far = 2 * n_loc
    wide = up_w.shape[2]
    n_up = wup_ref.shape[1] // wide
    n_blk = up_w.shape[0]
    d_loc = wdn_ref.shape[0]
    slim = fup_ref.shape[2]

    barrier = pltpu.get_barrier_semaphore()
    pl.semaphore_signal(barrier, inc=1, device_id={"tp": peer}, device_id_type=MESH)
    pl.semaphore_signal(barrier, inc=1, device_id={"tp": far}, device_id_type=MESH)

    first = [pltpu.make_async_copy(src, dst, x_sem.at[i]) for i, (src, dst) in enumerate([(ctx_ref, ctx), (r0_ref, r0), (wo_ref, wo_w)])]
    for load in first:
        load.start()
    loads = []
    for i in range(n_up):
        loads.append(pltpu.make_async_copy(wup_ref.at[:, pl.ds(i * wide, wide)], up_w.at[i], w_sem.at[len(loads)]))
    for i in range(n_dp):
        loads.append(pltpu.make_async_copy(fup_ref.at[i], up_w.at[n_up + i * slim // wide, :, pl.ds(i * slim % wide, slim)], w_sem.at[len(loads)]))
    loads.append(pltpu.make_async_copy(wdn_ref, dn_w.at[pl.ds(0, d_loc), :], w_sem.at[len(loads)]))
    loads.append(pltpu.make_async_copy(fdn_ref, dn_w.at[pl.ds(d_loc, d_loc), :], w_sem.at[len(loads)]))
    for load in loads:
        load.start()
    pl.semaphore_wait(barrier, 2)

    def remote(src, dst, send, recv, to):
        return pltpu.make_async_remote_copy(src, dst, send, recv, device_id={"tp": to}, device_id_type=MESH)

    def sub(i):
        return pl.ds(pl.multiple_of(i * SUBROWS, SUBROWS), SUBROWS)

    def x_far(i):
        return remote(xbuf.at[i // 2, sub(lax.rem(i, 2)), :], xbuf.at[first_far + i, pl.ds(0, SUBROWS), :], fx_send.at[i], fx_recv.at[i], far)

    def x_peer(i):
        return remote(xbuf.at[i], xbuf.at[n_loc + i], px_send.at[i], px_recv.at[i], peer)

    def x_pass(i):
        return remote(xbuf.at[first_far + i, pl.ds(0, SUBROWS), :], xbuf.at[first_far + i, pl.ds(SUBROWS, SUBROWS), :], fw_send.at[i], fw_recv.at[i], peer)

    def back_peer(i):
        return remote(ptl.at[n_loc + i], from_peer.at[i], lp_send.at[i], lp_recv.at[i], peer)

    def back_pre(i):
        return remote(ptl.at[first_far + i, pl.ds(SUBROWS, SUBROWS), :], pre.at[i], pr_send.at[i], pr_recv.at[i], peer)

    def back_far(i):
        return remote(ptl.at[first_far + i, pl.ds(0, SUBROWS), :], from_far.at[i], rf_send.at[i], rf_recv.at[i], far)

    for load in first:
        load.wait()

    def project(i, carry):
        for g in range(n_dp):
            sl = pl.ds(g * wo_w.shape[2], wo_w.shape[2])
            attn = jnp.dot(ctx[sub(i), :], wo_w[g], preferred_element_type=jnp.float32)
            r1[sub(i), sl] = (r0[sub(i), sl].astype(jnp.float32) + (attn + vec_ref[0:1, sl])).astype(jnp.bfloat16)
        for r in range(0, SUBROWS, 16):
            rows = r1[pl.ds(pl.multiple_of(i * SUBROWS + r, 16), 16), :].astype(jnp.float32)
            xbuf[i // 2, pl.ds(pl.multiple_of(lax.rem(i, 2) * SUBROWS + r, 16), 16), :] = norm_rows(rows, vec_ref[1:2, :], vec_ref[2:3, :])
        x_far(i).start()

        @pl.when(lax.rem(i, 2) == 1)
        def _():
            x_peer(i // 2).start()

        return carry

    lax.fori_loop(0, n_sub, project, 0)
    for load in loads:
        load.wait()

    def body(s, carry):
        @pl.when((s >= 2) & (s < 2 + n_sub))
        def _():
            x_far(s - 2).wait_recv()
            x_pass(s - 2).start()

        @pl.when((s >= n_loc) & (s < first_far))
        def _():
            x_peer(s - n_loc).wait_recv()

        @pl.when((s >= first_far) & (s < steps))
        def _():
            x_pass(s - first_far).wait_recv()

        @pl.when(s < steps)
        def _():
            def up(n, carry):
                hid = jnp.dot(xbuf[s], up_w[n], preferred_element_type=jnp.float32) + bias_ref[n]
                act[:, pl.ds(pl.multiple_of(n * wide, wide), wide)] = bloom_gelu(hid).astype(jnp.bfloat16)
                return carry

            lax.fori_loop(0, n_blk, up, 0)

            def down(n, carry):
                sl = pl.ds(pl.multiple_of(n * wide, wide), wide)
                ptl[s, :, sl] = jnp.dot(act[...], dn_w[:, sl], preferred_element_type=jnp.float32).astype(jnp.bfloat16)
                return carry

            lax.fori_loop(0, dn_w.shape[1] // wide, down, 0)

        @pl.when((s >= n_loc) & (s < first_far))
        def _():
            back_peer(s - n_loc).start()

        @pl.when((s >= first_far) & (s < steps))
        def _():
            back_pre(s - first_far).start()

        @pl.when(s > first_far)
        def _():
            i = s - first_far - 1
            back_pre(i).wait_recv()
            for r in range(0, SUBROWS, 32):
                sl = pl.ds(r, 32)
                ptl[first_far + i, sl, :] = (ptl[first_far + i, sl, :].astype(jnp.float32) + pre[i, sl, :].astype(jnp.float32)).astype(jnp.bfloat16)
            back_far(i).start()

        return carry

    lax.fori_loop(0, steps + 1, body, 0)

    for i in range(n_loc):
        back_peer(i).wait_recv()

    def out_copy(i):
        return pltpu.make_async_copy(obuf.at[sub(i), :], out_ref.at[sub(i), :], o_sem.at[i])

    def finish(i, carry):
        back_far(i).wait_recv()
        for r in range(0, SUBROWS, 16):
            own = pl.ds(pl.multiple_of(lax.rem(i, 2) * SUBROWS + r, 16), 16)
            row = pl.ds(pl.multiple_of(i * SUBROWS + r, 16), 16)
            total = ptl[i // 2, own, :].astype(jnp.float32) + from_peer[i // 2, own, :].astype(jnp.float32) + from_far[i, pl.ds(r, 16), :].astype(jnp.float32)
            obuf[row, :] = (r1[row, :].astype(jnp.float32) + (total + vec_ref[3:4, :])).astype(jnp.bfloat16)
        out_copy(i).start()
        return carry

    lax.fori_loop(0, n_sub, finish, 0)
    for i in range(n_loc):
        x_peer(i).wait_send()
        back_peer(i).wait_send()
    for i in range(n_sub):
        x_far(i).wait_send()
        x_pass(i).wait_send()
        back_pre(i).wait_send()
        back_far(i).wait_send()
        out_copy(i).wait()


def mlp(context, r0, wo, w_up, w_down, far_up, far_down, bias, vecs):
    rows, d = context.shape
    ff = w_up.shape[1]
    wide = 512
    mid = 2 * SUBROWS
    n_loc, n_sub = rows // mid, rows // SUBROWS
    steps = 2 * n_loc + n_sub
    n_dp = far_up.shape[0]
    bf = jnp.bfloat16
    dma = pltpu.SemaphoreType.DMA
    hbm = pl.BlockSpec(memory_space=pl.ANY)
    vmem = pl.BlockSpec(memory_space=pltpu.VMEM)
    return pl.pallas_call(
        functools.partial(mlp_kernel, n_dp),
        out_shape=jax.ShapeDtypeStruct((rows, d), bf),
        in_specs=[hbm] * 7 + [vmem] * 2,
        out_specs=hbm,
        scratch_shapes=[
            pltpu.VMEM((rows, d), bf), pltpu.VMEM((rows, d), bf), pltpu.VMEM((rows, d), bf), pltpu.VMEM(wo.shape, bf), pltpu.VMEM((steps, mid, d), bf), pltpu.VMEM((steps, mid, d), bf), pltpu.VMEM((2 * ff // wide, d, wide), bf), pltpu.VMEM((2 * ff, d), bf),
            pltpu.VMEM((mid, 2 * ff), bf), pltpu.VMEM((n_loc, mid, d), bf), pltpu.VMEM((n_sub, SUBROWS, d), bf), pltpu.VMEM((n_sub, SUBROWS, d), bf), pltpu.VMEM((rows, d), bf),
            dma((32,)), dma((3,)), dma((n_loc,)), dma((n_loc,)), dma((n_sub,)), dma((n_sub,)), dma((n_sub,)), dma((n_sub,)),
            dma((n_loc,)), dma((n_loc,)), dma((n_sub,)), dma((n_sub,)), dma((n_sub,)), dma((n_sub,)), dma((n_sub,)),
        ],
        compiler_params=pltpu.CompilerParams(collective_id=2, has_side_effects=True, vmem_limit_bytes=61900 * 1024),
        cost_estimate=pl.CostEstimate(flops=10 ** 12, bytes_accessed=40 * 10 ** 6, transcendentals=0),
        name="mlp",
    )(context, r0, wo, w_up, w_down, far_up, far_down, bias.reshape(2 * ff // wide, 1, wide), vecs)


def solution(mesh):
    n_tp = mesh.shape['tp']
    n_dp = mesh.shape['dp']

    def local_step(tok_ids, pad_mask, emb_shard, ln_emb_w, ln_emb_b, ln1_w, ln1_b, w_qkv, b_qkv, w_out, b_out, ln2_w, ln2_b, w_up, b_up, w_down, b_down):
        f32 = jnp.float32
        tp_rank = lax.axis_index('tp')
        dp_rank = lax.axis_index('dp')
        n_seq, seq = tok_ids.shape
        d = emb_shard.shape[1]
        heads_loc = w_qkv.shape[1]

        def part(w, axis):
            size = w.shape[axis] // n_dp
            return lax.dynamic_slice_in_dim(w, dp_rank * size, size, axis)

        half = n_tp // 2
        swap = [(t, (t + half) % n_tp) for t in range(n_tp)]
        out_part = lax.all_gather(part(w_out, 1), 'tp', axis=0, tiled=True)
        up_part = lax.ppermute(part(w_up, 1), 'tp', swap)
        down_part = lax.ppermute(part(w_down, 0), 'tp', swap)

        part_emb = lookup(tok_ids.reshape(-1), emb_shard, tp_rank).reshape(n_seq, seq, d)
        part_emb, up_part, down_part, out_part = lax.optimization_barrier((part_emb, up_part, down_part, out_part))
        wo = lax.all_gather(out_part, 'dp', axis=0, tiled=False)
        wu = lax.all_gather(up_part, 'dp', axis=0, tiled=False)
        ln_pack = jnp.stack([ln_emb_w, ln_emb_b, ln1_w, ln1_b]).astype(f32)
        normed_all, resid_in = chain(part_emb, ln_pack, n_tp)
        normed_all, wu, wo, down_part = lax.optimization_barrier((normed_all, wu, wo, down_part))
        wd = lax.all_gather(down_part, 'dp', axis=0, tiled=True)
        qkv = (jnp.einsum('bsd,dhce->cbhse', normed_all, w_qkv, preferred_element_type=f32) + b_qkv.astype(f32).transpose(1, 0, 2)[:, None, :, None, :]).astype(jnp.bfloat16)
        all_slopes = jnp.array(alibi_slopes(heads_loc * n_tp), f32)
        head_slopes = lax.dynamic_slice_in_dim(all_slopes, tp_rank * heads_loc, heads_loc)
        context, b_all = attend(qkv, pad_mask, head_slopes, b_up.reshape(8, -1), n_tp)
        context, wd = lax.optimization_barrier((context, wd))
        far_bias = lax.dynamic_index_in_dim(b_all, (tp_rank + half) % n_tp, 0, keepdims=False).reshape(-1)
        bias = jnp.concatenate([b_up, far_bias]).astype(f32)
        rows = n_seq * seq // n_tp
        vecs = jnp.stack([b_out, ln2_w, ln2_b, b_down]).astype(f32)
        out = mlp(context.reshape(rows, d), resid_in.reshape(rows, d), wo, w_up, w_down, wu, wd, bias, vecs)
        return out.reshape(n_seq, seq // n_tp, d)

    replicated = P(None)
    in_specs = (P('dp', None), P('dp', None), P('tp', None), replicated, replicated, replicated, replicated, P(None, 'tp', None, None), P('tp', None, None), P('tp', None), replicated, replicated, replicated, P(None, 'tp'), P('tp'), P('tp', None), replicated)
    return jax.shard_map(local_step, mesh=mesh, in_specs=in_specs, out_specs=P('dp', 'tp', None), check_vma=False)
```

```python
import functools
import math
import jax
import jax.numpy as jnp
from jax import lax
from jax.experimental import pallas as pl
from jax.experimental.pallas import tpu as pltpu
from jax.sharding import PartitionSpec as P

LN_EPS = 1e-5
LOG2E = 1.4426950408889634
MESH = pl.DeviceIdType.MESH


def alibi_slopes(n_heads):
    closest = 2 ** int(math.floor(math.log2(n_heads)))
    base_ratio = 2.0 ** (-(2.0 ** -(math.log2(closest) - 3)))
    extra_ratio = 2.0 ** (-(2.0 ** -(math.log2(2 * closest) - 3)))
    first_part = [base_ratio ** step_k for step_k in range(1, closest + 1)]
    second_part = [extra_ratio ** step_k for step_k in range(1, 2 * (n_heads - closest), 2)]
    return first_part + second_part


def bloom_gelu(values_in):
    return values_in * 0.5 * (1.0 + jnp.tanh(0.79788456 * values_in * (1.0 + 0.044715 * values_in * values_in)))


GROUP = 64
SUB = 32
SLOTS = 4


def lookup_kernel(tile_ref, sel_ref, table_ref, out_ref, buf, sems):
    step = pl.program_id(0)
    steps = pl.num_programs(0)

    def issue(grp):
        slot = lax.rem(grp, SLOTS)
        for i in range(GROUP):
            row = pl.multiple_of(tile_ref[grp * GROUP + i] * 8, 8)
            pltpu.make_async_copy(table_ref.at[pl.ds(row, 8), :], buf.at[slot, pl.ds(i * 8, 8), :], sems.at[slot]).start()

    @pl.when(step == 0)
    def _():
        for grp in range(SLOTS - 1):
            issue(grp)

    @pl.when(step + SLOTS - 1 < steps)
    def _():
        issue(step + SLOTS - 1)

    slot = lax.rem(step, SLOTS)
    pltpu.make_async_copy(table_ref.at[pl.ds(0, GROUP * 8), :], buf.at[slot], sems.at[slot]).wait()
    for j in range(GROUP // SUB):
        cols = lax.broadcasted_iota(jnp.int32, (SUB, SUB * 8), 1)
        onehot = (cols == sel_ref[pl.ds(j * SUB, SUB), :]).astype(jnp.float32).astype(jnp.bfloat16)
        rows = jnp.dot(onehot, buf[slot, pl.ds(j * SUB * 8, SUB * 8), :], preferred_element_type=jnp.float32)
        out_ref[pl.ds(j * SUB, SUB), :] = rows.astype(jnp.bfloat16)


def lookup(ids, table, tp_rank):
    n_tok = ids.shape[0]
    vocab_loc, d = table.shape
    loc = ids - tp_rank * vocab_loc
    held = (loc >= 0) & (loc < vocab_loc)
    spread = (jnp.arange(n_tok, dtype=jnp.int32) * 5) % (vocab_loc // 8)
    tile = jnp.where(held, loc // 8, spread)
    sel = jnp.where(held, (jnp.arange(n_tok, dtype=jnp.int32) % SUB) * 8 + loc % 8, -1)[:, None]
    return pl.pallas_call(
        lookup_kernel,
        out_shape=jax.ShapeDtypeStruct((n_tok, d), jnp.bfloat16),
        grid_spec=pltpu.PrefetchScalarGridSpec(
            num_scalar_prefetch=1,
            grid=(n_tok // GROUP,),
            in_specs=[pl.BlockSpec((GROUP, 1), lambda i, t: (i, 0)), pl.BlockSpec(memory_space=pl.ANY)],
            out_specs=pl.BlockSpec((GROUP, d), lambda i, t: (i, 0)),
            scratch_shapes=[pltpu.VMEM((SLOTS, GROUP * 8, d), jnp.bfloat16), pltpu.SemaphoreType.DMA((SLOTS,))],
        ),
        compiler_params=pltpu.CompilerParams(dimension_semantics=("arbitrary",)),
        cost_estimate=pl.CostEstimate(flops=n_tok * d * 40000, bytes_accessed=n_tok * d * 18, transcendentals=0),
        name="lookup",
    )(tile, sel, table)


CHUNK = 32
LAG = 3
LN_ROWS = 16


def norm_rows(x, gain, shift):
    n = x.shape[-1]
    mean_v = jnp.sum(x, axis=-1, keepdims=True) * (1.0 / n)
    centered = x - mean_v
    var_v = jnp.sum(centered * centered, axis=-1, keepdims=True) * (1.0 / n)
    return (centered * lax.rsqrt(var_v + LN_EPS) * gain + shift).astype(jnp.bfloat16)


def chain_kernel(n_tp, part_ref, ln_ref, a_ref, r0_ref, own, pre, rgt, lft, abuf, r0buf,
                 own_sem, pre_send, pre_recv, r_send, r_recv, l_send, l_recv, a_loc, a_send, a_recv, r0_loc, r0_send, r0_recv):
    seq = part_ref.shape[1]
    n_chunk = seq // CHUNK
    n_z = n_tp // 2
    me = lax.axis_index("tp")
    z = me // 2
    c = lax.rem(me, 2)
    peer = me + 1 - 2 * c
    pos_per = r0_ref.shape[1]
    per_dev = pos_per // CHUNK
    last = n_z - 1

    barrier = pltpu.get_barrier_semaphore()
    pl.semaphore_signal(barrier, inc=1, device_id={"tp": peer}, device_id_type=MESH)

    @pl.when(z > 0)
    def _():
        pl.semaphore_signal(barrier, inc=1, device_id={"tp": me - 2}, device_id_type=MESH)

    @pl.when(z < last)
    def _():
        pl.semaphore_signal(barrier, inc=1, device_id={"tp": me + 2}, device_id_type=MESH)

    @pl.when((z > 0) & (z < last))
    def _():
        pl.semaphore_wait(barrier, 3)

    @pl.when((z == 0) | (z == last))
    def _():
        pl.semaphore_wait(barrier, 2)

    def rows(k):
        return pl.ds(pl.multiple_of(k * CHUNK, CHUNK), CHUNK)

    def own_copy(k):
        return pltpu.make_async_copy(part_ref.at[c, rows(k), :], own.at[rows(k), :], own_sem.at[k])

    def pre_copy(k):
        return pltpu.make_async_remote_copy(part_ref.at[1 - c, rows(k), :], pre.at[rows(k), :], pre_send.at[k], pre_recv.at[k], device_id={"tp": peer}, device_id_type=MESH)

    def right_copy(src, k):
        return pltpu.make_async_remote_copy(src.at[rows(k), :], rgt.at[rows(k), :], r_send.at[k], r_recv.at[k], device_id={"tp": me + 2}, device_id_type=MESH)

    def left_copy(k):
        return pltpu.make_async_remote_copy(pre.at[rows(k), :], lft.at[rows(k), :], l_send.at[k], l_recv.at[k], device_id={"tp": me - 2}, device_id_type=MESH)

    def a_local(k):
        return pltpu.make_async_copy(abuf.at[rows(k), :], a_ref.at[c, rows(k), :], a_loc.at[k])

    def a_peer(k):
        return pltpu.make_async_remote_copy(abuf.at[rows(k), :], a_ref.at[c, rows(k), :], a_send.at[k], a_recv.at[k], device_id={"tp": peer}, device_id_type=MESH)

    def r0_local(i):
        return pltpu.make_async_copy(r0buf.at[c, rows(i), :], r0_ref.at[c, rows(i), :], r0_loc.at[i])

    def r0_peer(i):
        return pltpu.make_async_remote_copy(r0buf.at[1 - c, rows(i), :], r0_ref.at[c, rows(i), :], r0_send.at[i], r0_recv.at[i], device_id={"tp": peer}, device_id_type=MESH)

    def start(k, carry):
        own_copy(k).start()
        pre_copy(k).start()
        return carry

    lax.fori_loop(0, n_chunk, start, 0)

    def step_body(s, carry):
        @pl.when(s < n_chunk)
        def _():
            own_copy(s).wait()
            pre_copy(s).wait_recv()
            own[rows(s), :] = own[rows(s), :] + pre[rows(s), :]

        kr = s - LAG * z

        @pl.when((kr >= 0) & (kr < n_chunk))
        def _():
            @pl.when(z == 0)
            def _():
                right_copy(own, kr).start()

            @pl.when(z > 0)
            def _():
                right_copy(rgt, kr).wait_recv()
                rgt[rows(kr), :] = rgt[rows(kr), :] + own[rows(kr), :]

                @pl.when(z < last)
                def _():
                    right_copy(rgt, kr).start()

        kl = s - LAG * (last - z)

        @pl.when((kl >= 0) & (kl < n_chunk))
        def _():
            @pl.when(z < last)
            def _():
                left_copy(kl).wait_recv()

                @pl.when(z > 0)
                def _():
                    pre[rows(kl), :] = lft[rows(kl), :] + own[rows(kl), :]

            @pl.when(z == last)
            def _():
                pre[rows(kl), :] = own[rows(kl), :]

            @pl.when(z > 0)
            def _():
                left_copy(kl).start()

        kt = s - LAG * jnp.maximum(z, last - z)

        @pl.when((kt >= 0) & (kt < n_chunk))
        def _():
            base = kt * CHUNK
            first = kt - z * 2 * per_dev
            near = (first >= 0) & (first < 2 * per_dev)
            side = jnp.where(near, first // per_dev, 0)
            inner = jnp.where(near, lax.rem(first, per_dev), 0)

            def norm(i, carry):
                sl = pl.ds(pl.multiple_of(base + i * LN_ROWS, LN_ROWS), LN_ROWS)

                @pl.when(z == 0)
                def _():
                    abuf[sl, :] = own[sl, :] + lft[sl, :]

                @pl.when((z > 0) & (z < last))
                def _():
                    abuf[sl, :] = rgt[sl, :] + lft[sl, :]

                @pl.when(z == last)
                def _():
                    abuf[sl, :] = rgt[sl, :]

                r0 = norm_rows(abuf[sl, :].astype(jnp.float32), ln_ref[0:1, :], ln_ref[1:2, :])
                abuf[sl, :] = norm_rows(r0.astype(jnp.float32), ln_ref[2:3, :], ln_ref[3:4, :])

                @pl.when(near)
                def _():
                    r0buf[side, pl.ds(pl.multiple_of(inner * CHUNK + i * LN_ROWS, LN_ROWS), LN_ROWS), :] = r0

                return carry

            lax.fori_loop(0, CHUNK // LN_ROWS, norm, 0)
            a_local(kt).start()
            a_peer(kt).start()

            @pl.when(near & (side == c))
            def _():
                r0_local(inner).start()

            @pl.when(near & (side != c))
            def _():
                r0_peer(inner).start()

        return carry

    lax.fori_loop(0, n_chunk + LAG * last, step_body, 0)

    def drain(k, carry):
        pre_copy(k).wait_send()
        a_local(k).wait()
        a_peer(k).wait()

        @pl.when(z < last)
        def _():
            right_copy(rgt, k).wait_send()

        @pl.when(z > 0)
        def _():
            left_copy(k).wait_send()

        return carry

    lax.fori_loop(0, n_chunk, drain, 0)

    def drain_r0(i, carry):
        r0_local(i).wait()
        r0_peer(i).wait()
        return carry

    lax.fori_loop(0, per_dev, drain_r0, 0)


def chain(part, ln_pack, n_tp):
    n_seq, seq, d = part.shape
    n_chunk = seq // CHUNK
    per_dev = seq // n_tp // CHUNK
    dma = pltpu.SemaphoreType.DMA
    big = pltpu.VMEM((seq, d), jnp.bfloat16)
    return pl.pallas_call(
        functools.partial(chain_kernel, n_tp),
        out_shape=(jax.ShapeDtypeStruct((n_seq, seq, d), jnp.bfloat16), jax.ShapeDtypeStruct((n_seq, seq // n_tp, d), jnp.bfloat16)),
        in_specs=[pl.BlockSpec(memory_space=pl.ANY), pl.BlockSpec(memory_space=pltpu.VMEM)],
        out_specs=(pl.BlockSpec(memory_space=pl.ANY), pl.BlockSpec(memory_space=pl.ANY)),
        scratch_shapes=[big, big, big, big, big, pltpu.VMEM((2, seq // n_tp, d), jnp.bfloat16)]
        + [dma((n_chunk,))] * 10 + [dma((per_dev,))] * 3,
        compiler_params=pltpu.CompilerParams(collective_id=0, has_side_effects=True, vmem_limit_bytes=58 * 1024 * 1024),
        cost_estimate=pl.CostEstimate(flops=10 ** 6, bytes_accessed=8 * part.size, transcendentals=0),
        name="chain",
    )(part, ln_pack)


def attend_kernel(n_tp, head_dim, qkv_ref, pad_ref, slope_ref, bup_ref, ctx_ref, ball_ref, cbuf, send_sem, recv_sem, loc_sem, b_send, b_recv, b_loc):
    n_seq, heads = qkv_ref.shape[1], qkv_ref.shape[2]
    seq = qkv_ref.shape[3]
    blk = seq // n_tp
    feat = heads * head_dim
    me = lax.axis_index("tp")

    barrier = pltpu.get_barrier_semaphore()
    for r in range(1, n_tp):
        pl.semaphore_signal(barrier, inc=1, device_id={"tp": lax.rem(me + r, n_tp)}, device_id_type=MESH)
    pl.semaphore_wait(barrier, n_tp - 1)

    def cols(t):
        return pl.ds(pl.multiple_of(t * feat, feat), feat)

    def bias_copy(r):
        return pltpu.make_async_remote_copy(bup_ref, ball_ref.at[me], b_send.at[r], b_recv.at[r], device_id={"tp": lax.rem(me + r, n_tp)}, device_id_type=MESH)

    for r in range(1, n_tp):
        bias_copy(r).start()
    own_bias = pltpu.make_async_copy(bup_ref, ball_ref.at[me], b_loc.at[0])
    own_bias.start()

    def ctx_copy(b, r):
        return pltpu.make_async_remote_copy(cbuf.at[b, r], ctx_ref.at[b, :, cols(me)], send_sem.at[b, r], recv_sem.at[b, r], device_id={"tp": lax.rem(me + r, n_tp)}, device_id_type=MESH)

    def ctx_local(b):
        return pltpu.make_async_copy(cbuf.at[b, 0], ctx_ref.at[b, :, cols(me)], loc_sem.at[b])

    def one(i, carry):
        b = lax.rem(i, n_seq)
        r = n_tp - 1 - i // n_seq
        dest = lax.rem(me + r, n_tp)
        for j in range(n_tp):
            @pl.when(dest == j)
            def _(j=j):
                span = (j + 1) * blk
                lo = j * blk
                key_pos = lax.broadcasted_iota(jnp.int32, (1, span), 1)
                key_ok = pad_ref[b, :, 0:span] == 1
                row_in = lax.broadcasted_iota(jnp.int32, (blk, blk), 0)
                col_in = lax.broadcasted_iota(jnp.int32, (blk, blk), 1)
                diag_ok = ((col_in < row_in) & (pad_ref[b, :, lo:span] == 1)) | (col_in == row_in)
                for h in range(heads):
                    slope = slope_ref[0, h] * LOG2E
                    rel = slope * (key_pos - lo).astype(jnp.float32)
                    far = jnp.where(key_ok, rel, -1e30)
                    q = qkv_ref[0, b, h, lo:span, :]
                    scale = head_dim ** -0.5 * LOG2E
                    diag = lax.dot_general(q, qkv_ref[1, b, h, lo:span, :], (((1,), (1,)), ((), ())), preferred_element_type=jnp.float32)
                    diag = jnp.where(diag_ok, diag * scale + rel[:, lo:span], -1e30)
                    top = jnp.max(diag, axis=-1, keepdims=True)
                    if j:
                        past = lax.dot_general(q, qkv_ref[1, b, h, 0:lo, :], (((1,), (1,)), ((), ())), preferred_element_type=jnp.float32)
                        past = past * scale + far[:, 0:lo]
                        top = jnp.maximum(top, jnp.max(past, axis=-1, keepdims=True))
                        past = jnp.exp2(past - top)
                    diag = jnp.exp2(diag - top)
                    total = jnp.sum(diag, axis=-1, keepdims=True)
                    if j:
                        total = total + jnp.sum(past, axis=-1, keepdims=True)
                    inv = 1.0 / total
                    out = jnp.dot((diag * inv).astype(jnp.bfloat16), qkv_ref[2, b, h, lo:span, :], preferred_element_type=jnp.float32)
                    if j:
                        out = out + jnp.dot((past * inv).astype(jnp.bfloat16), qkv_ref[2, b, h, 0:lo, :], preferred_element_type=jnp.float32)
                    cbuf[b, r, :, h * head_dim:(h + 1) * head_dim] = out.astype(jnp.bfloat16)

        @pl.when(r > 0)
        def _():
            ctx_copy(b, r).start()

        @pl.when(r == 0)
        def _():
            ctx_local(b).start()

        return carry

    lax.fori_loop(0, n_seq * n_tp, one, 0)

    for b in range(n_seq):
        ctx_local(b).wait()
        for r in range(1, n_tp):
            ctx_copy(b, r).wait()
    own_bias.wait()
    for r in range(1, n_tp):
        bias_copy(r).wait()


def attend(qkv, pad_mask, slopes, b_up, n_tp):
    _, n_seq, heads, seq, head_dim = qkv.shape
    blk = seq // n_tp
    feat = heads * head_dim
    dma = pltpu.SemaphoreType.DMA
    vmem = pl.BlockSpec(memory_space=pltpu.VMEM)
    return pl.pallas_call(
        functools.partial(attend_kernel, n_tp, head_dim),
        out_shape=(jax.ShapeDtypeStruct((n_seq, blk, n_tp * feat), jnp.bfloat16), jax.ShapeDtypeStruct((n_tp,) + b_up.shape, jnp.bfloat16)),
        in_specs=[vmem, vmem, pl.BlockSpec(memory_space=pltpu.SMEM), vmem],
        out_specs=(pl.BlockSpec(memory_space=pl.ANY), pl.BlockSpec(memory_space=pl.ANY)),
        scratch_shapes=[pltpu.VMEM((n_seq, n_tp, blk, feat), jnp.bfloat16), dma((n_seq, n_tp)), dma((n_seq, n_tp)), dma((n_seq,)), dma((n_tp,)), dma((n_tp,)), dma((1,))],
        compiler_params=pltpu.CompilerParams(collective_id=1, has_side_effects=True, vmem_limit_bytes=56000 * 1024),
        cost_estimate=pl.CostEstimate(flops=30 * 10 ** 9, bytes_accessed=2 * qkv.size, transcendentals=seq * seq * 2),
        name="attend",
    )(qkv, pad_mask[:, None, :], slopes[None, :], b_up)


SUBROWS = 128


def mlp_kernel(n_dp, ctx_ref, r0_ref, wo_ref, wup_ref, wdn_ref, fup_ref, fdn_ref, bias_ref, vec_ref, out_ref,
               ctx, r0, r1, wo_w, xbuf, ptl, up_w, dn_w, act, from_peer, pre, from_far, obuf,
               w_sem, x_sem, px_send, px_recv, fx_send, fx_recv, fw_send, fw_recv, lp_send, lp_recv, pr_send, pr_recv, rf_send, rf_recv, o_sem):
    me = lax.axis_index("tp")
    peer = me + 1 - 2 * lax.rem(me, 2)
    far = me + 2 - 4 * lax.rem(me // 2, 2)
    mid = 2 * SUBROWS
    n_loc = ctx.shape[0] // mid
    n_sub = ctx.shape[0] // SUBROWS
    steps = 2 * n_loc + n_sub
    first_far = 2 * n_loc
    wide = up_w.shape[2]
    n_up = wup_ref.shape[1] // wide
    n_blk = up_w.shape[0]
    d_loc = wdn_ref.shape[0]
    slim = fup_ref.shape[2]

    barrier = pltpu.get_barrier_semaphore()
    pl.semaphore_signal(barrier, inc=1, device_id={"tp": peer}, device_id_type=MESH)
    pl.semaphore_signal(barrier, inc=1, device_id={"tp": far}, device_id_type=MESH)

    first = [pltpu.make_async_copy(src, dst, x_sem.at[i]) for i, (src, dst) in enumerate([(ctx_ref, ctx), (r0_ref, r0), (wo_ref, wo_w)])]
    for load in first:
        load.start()
    loads = []
    for i in range(n_up):
        loads.append(pltpu.make_async_copy(wup_ref.at[:, pl.ds(i * wide, wide)], up_w.at[i], w_sem.at[len(loads)]))
    for i in range(n_dp):
        loads.append(pltpu.make_async_copy(fup_ref.at[i], up_w.at[n_up + i * slim // wide, :, pl.ds(i * slim % wide, slim)], w_sem.at[len(loads)]))
    loads.append(pltpu.make_async_copy(wdn_ref, dn_w.at[pl.ds(0, d_loc), :], w_sem.at[len(loads)]))
    loads.append(pltpu.make_async_copy(fdn_ref, dn_w.at[pl.ds(d_loc, d_loc), :], w_sem.at[len(loads)]))
    pl.semaphore_wait(barrier, 2)

    def remote(src, dst, send, recv, to):
        return pltpu.make_async_remote_copy(src, dst, send, recv, device_id={"tp": to}, device_id_type=MESH)

    def sub(i):
        return pl.ds(pl.multiple_of(i * SUBROWS, SUBROWS), SUBROWS)

    def x_far(i):
        return remote(xbuf.at[i // 2, sub(lax.rem(i, 2)), :], xbuf.at[first_far + i, pl.ds(0, SUBROWS), :], fx_send.at[i], fx_recv.at[i], far)

    def x_peer(i):
        return remote(xbuf.at[i], xbuf.at[n_loc + i], px_send.at[i], px_recv.at[i], peer)

    def x_pass(i):
        return remote(xbuf.at[first_far + i, pl.ds(0, SUBROWS), :], xbuf.at[first_far + i, pl.ds(SUBROWS, SUBROWS), :], fw_send.at[i], fw_recv.at[i], peer)

    def back_peer(i):
        return remote(ptl.at[n_loc + i], from_peer.at[i], lp_send.at[i], lp_recv.at[i], peer)

    def back_pre(i):
        return remote(ptl.at[first_far + i, pl.ds(SUBROWS, SUBROWS), :], pre.at[i], pr_send.at[i], pr_recv.at[i], peer)

    def back_far(i):
        return remote(ptl.at[first_far + i, pl.ds(0, SUBROWS), :], from_far.at[i], rf_send.at[i], rf_recv.at[i], far)

    for load in first:
        load.wait()
    for load in loads:
        load.start()

    def project(i, carry):
        for g in range(n_dp):
            sl = pl.ds(g * wo_w.shape[2], wo_w.shape[2])
            attn = jnp.dot(ctx[sub(i), :], wo_w[g], preferred_element_type=jnp.float32)
            r1[sub(i), sl] = (r0[sub(i), sl].astype(jnp.float32) + (attn + vec_ref[0:1, sl])).astype(jnp.bfloat16)
        for r in range(0, SUBROWS, 16):
            rows = r1[pl.ds(pl.multiple_of(i * SUBROWS + r, 16), 16), :].astype(jnp.float32)
            xbuf[i // 2, pl.ds(pl.multiple_of(lax.rem(i, 2) * SUBROWS + r, 16), 16), :] = norm_rows(rows, vec_ref[1:2, :], vec_ref[2:3, :])
        x_far(i).start()

        @pl.when(lax.rem(i, 2) == 1)
        def _():
            x_peer(i // 2).start()

        return carry

    lax.fori_loop(0, n_sub, project, 0)
    for load in loads:
        load.wait()

    def body(s, carry):
        @pl.when((s >= 2) & (s < 2 + n_sub))
        def _():
            x_far(s - 2).wait_recv()
            x_pass(s - 2).start()

        @pl.when((s >= n_loc) & (s < first_far))
        def _():
            x_peer(s - n_loc).wait_recv()

        @pl.when((s >= first_far) & (s < steps))
        def _():
            x_pass(s - first_far).wait_recv()

        @pl.when(s < steps)
        def _():
            def up(n, carry):
                hid = jnp.dot(xbuf[s], up_w[n], preferred_element_type=jnp.float32) + bias_ref[n]
                act[:, pl.ds(pl.multiple_of(n * wide, wide), wide)] = bloom_gelu(hid).astype(jnp.bfloat16)
                return carry

            lax.fori_loop(0, n_blk, up, 0)

            def down(n, carry):
                sl = pl.ds(pl.multiple_of(n * wide, wide), wide)
                ptl[s, :, sl] = jnp.dot(act[...], dn_w[:, sl], preferred_element_type=jnp.float32).astype(jnp.bfloat16)
                return carry

            lax.fori_loop(0, dn_w.shape[1] // wide, down, 0)

        @pl.when((s >= n_loc) & (s < first_far))
        def _():
            back_peer(s - n_loc).start()

        @pl.when((s >= first_far) & (s < steps))
        def _():
            back_pre(s - first_far).start()

        @pl.when(s > first_far)
        def _():
            i = s - first_far - 1
            back_pre(i).wait_recv()
            for r in range(0, SUBROWS, 32):
                sl = pl.ds(r, 32)
                ptl[first_far + i, sl, :] = (ptl[first_far + i, sl, :].astype(jnp.float32) + pre[i, sl, :].astype(jnp.float32)).astype(jnp.bfloat16)
            back_far(i).start()

        return carry

    lax.fori_loop(0, steps + 1, body, 0)

    for i in range(n_loc):
        back_peer(i).wait_recv()

    def out_copy(i):
        return pltpu.make_async_copy(obuf.at[sub(i), :], out_ref.at[sub(i), :], o_sem.at[i])

    def finish(i, carry):
        back_far(i).wait_recv()
        for r in range(0, SUBROWS, 16):
            own = pl.ds(pl.multiple_of(lax.rem(i, 2) * SUBROWS + r, 16), 16)
            row = pl.ds(pl.multiple_of(i * SUBROWS + r, 16), 16)
            total = ptl[i // 2, own, :].astype(jnp.float32) + from_peer[i // 2, own, :].astype(jnp.float32) + from_far[i, pl.ds(r, 16), :].astype(jnp.float32)
            obuf[row, :] = (r1[row, :].astype(jnp.float32) + (total + vec_ref[3:4, :])).astype(jnp.bfloat16)
        out_copy(i).start()
        return carry

    lax.fori_loop(0, n_sub, finish, 0)
    for i in range(n_loc):
        x_peer(i).wait_send()
        back_peer(i).wait_send()
    for i in range(n_sub):
        x_far(i).wait_send()
        x_pass(i).wait_send()
        back_pre(i).wait_send()
        back_far(i).wait_send()
        out_copy(i).wait()


def mlp(context, r0, wo, w_up, w_down, far_up, far_down, bias, vecs):
    rows, d = context.shape
    ff = w_up.shape[1]
    wide = 512
    mid = 2 * SUBROWS
    n_loc, n_sub = rows // mid, rows // SUBROWS
    steps = 2 * n_loc + n_sub
    n_dp = far_up.shape[0]
    bf = jnp.bfloat16
    dma = pltpu.SemaphoreType.DMA
    hbm = pl.BlockSpec(memory_space=pl.ANY)
    vmem = pl.BlockSpec(memory_space=pltpu.VMEM)
    return pl.pallas_call(
        functools.partial(mlp_kernel, n_dp),
        out_shape=jax.ShapeDtypeStruct((rows, d), bf),
        in_specs=[hbm] * 7 + [vmem] * 2,
        out_specs=hbm,
        scratch_shapes=[
            pltpu.VMEM((rows, d), bf), pltpu.VMEM((rows, d), bf), pltpu.VMEM((rows, d), bf), pltpu.VMEM(wo.shape, bf), pltpu.VMEM((steps, mid, d), bf), pltpu.VMEM((steps, mid, d), bf), pltpu.VMEM((2 * ff // wide, d, wide), bf), pltpu.VMEM((2 * ff, d), bf),
            pltpu.VMEM((mid, 2 * ff), bf), pltpu.VMEM((n_loc, mid, d), bf), pltpu.VMEM((n_sub, SUBROWS, d), bf), pltpu.VMEM((n_sub, SUBROWS, d), bf), pltpu.VMEM((rows, d), bf),
            dma((32,)), dma((3,)), dma((n_loc,)), dma((n_loc,)), dma((n_sub,)), dma((n_sub,)), dma((n_sub,)), dma((n_sub,)),
            dma((n_loc,)), dma((n_loc,)), dma((n_sub,)), dma((n_sub,)), dma((n_sub,)), dma((n_sub,)), dma((n_sub,)),
        ],
        compiler_params=pltpu.CompilerParams(collective_id=2, has_side_effects=True, vmem_limit_bytes=61900 * 1024),
        cost_estimate=pl.CostEstimate(flops=10 ** 12, bytes_accessed=40 * 10 ** 6, transcendentals=0),
        name="mlp",
    )(context, r0, wo, w_up, w_down, far_up, far_down, bias.reshape(2 * ff // wide, 1, wide), vecs)


def solution(mesh):
    n_tp = mesh.shape['tp']
    n_dp = mesh.shape['dp']

    def local_step(tok_ids, pad_mask, emb_shard, ln_emb_w, ln_emb_b, ln1_w, ln1_b, w_qkv, b_qkv, w_out, b_out, ln2_w, ln2_b, w_up, b_up, w_down, b_down):
        f32 = jnp.float32
        tp_rank = lax.axis_index('tp')
        dp_rank = lax.axis_index('dp')
        n_seq, seq = tok_ids.shape
        d = emb_shard.shape[1]
        heads_loc = w_qkv.shape[1]

        def part(w, axis):
            size = w.shape[axis] // n_dp
            return lax.dynamic_slice_in_dim(w, dp_rank * size, size, axis)

        half = n_tp // 2
        swap = [(t, (t + half) % n_tp) for t in range(n_tp)]
        out_part = lax.all_gather(part(w_out, 1), 'tp', axis=0, tiled=True)
        up_part = lax.ppermute(part(w_up, 1), 'tp', swap)
        down_part = lax.ppermute(part(w_down, 0), 'tp', swap)

        part_emb = lookup(tok_ids.reshape(-1), emb_shard, tp_rank)
        part_emb = part_emb.reshape(n_seq, seq, d)
        part_emb, up_part, out_part = lax.optimization_barrier((part_emb, up_part, out_part))
        wo = lax.all_gather(out_part, 'dp', axis=0, tiled=False)
        wu = lax.all_gather(up_part, 'dp', axis=0, tiled=False)
        ln_pack = jnp.stack([ln_emb_w, ln_emb_b, ln1_w, ln1_b]).astype(f32)
        normed_all, resid_in = chain(part_emb, ln_pack, n_tp)
        normed_all, wu, wo, down_part = lax.optimization_barrier((normed_all, wu, wo, down_part))
        wd = lax.all_gather(down_part, 'dp', axis=0, tiled=True)
        qkv = (jnp.einsum('bsd,dhce->cbhse', normed_all, w_qkv, preferred_element_type=f32) + b_qkv.astype(f32).transpose(1, 0, 2)[:, None, :, None, :]).astype(jnp.bfloat16)
        all_slopes = jnp.array(alibi_slopes(heads_loc * n_tp), f32)
        head_slopes = lax.dynamic_slice_in_dim(all_slopes, tp_rank * heads_loc, heads_loc)
        context, b_all = attend(qkv, pad_mask, head_slopes, b_up.reshape(8, -1), n_tp)
        context, wd = lax.optimization_barrier((context, wd))
        far_bias = lax.dynamic_index_in_dim(b_all, (tp_rank + half) % n_tp, 0, keepdims=False).reshape(-1)
        bias = jnp.concatenate([b_up, far_bias]).astype(f32)
        rows = n_seq * seq // n_tp
        vecs = jnp.stack([b_out, ln2_w, ln2_b, b_down]).astype(f32)
        out = mlp(context.reshape(rows, d), resid_in.reshape(rows, d), wo, w_up, w_down, wu, wd, bias, vecs)
        return out.reshape(n_seq, seq // n_tp, d)

    replicated = P(None)
    in_specs = (P('dp', None), P('dp', None), P('tp', None), replicated, replicated, replicated, replicated, P(None, 'tp', None, None), P('tp', None, None), P('tp', None), replicated, replicated, replicated, P(None, 'tp'), P('tp'), P('tp', None), replicated)
    return jax.shard_map(local_step, mesh=mesh, in_specs=in_specs, out_specs=P('dp', 'tp', None), check_vma=False)
```

```python
import functools
import math
import jax
import jax.numpy as jnp
from jax import lax
from jax.experimental import pallas as pl
from jax.experimental.pallas import tpu as pltpu
from jax.sharding import PartitionSpec as P

LN_EPS = 1e-5
LOG2E = 1.4426950408889634
MESH = pl.DeviceIdType.MESH


def alibi_slopes(n_heads):
    closest = 2 ** int(math.floor(math.log2(n_heads)))
    base_ratio = 2.0 ** (-(2.0 ** -(math.log2(closest) - 3)))
    extra_ratio = 2.0 ** (-(2.0 ** -(math.log2(2 * closest) - 3)))
    first_part = [base_ratio ** step_k for step_k in range(1, closest + 1)]
    second_part = [extra_ratio ** step_k for step_k in range(1, 2 * (n_heads - closest), 2)]
    return first_part + second_part


def bloom_gelu(values_in):
    return values_in * 0.5 * (1.0 + jnp.tanh(0.79788456 * values_in * (1.0 + 0.044715 * values_in * values_in)))


GROUP = 64
SUB = 32
SLOTS = 4


def lookup_kernel(tile_ref, sel_ref, table_ref, out_ref, buf, sems):
    step = pl.program_id(0)
    steps = pl.num_programs(0)

    def issue(grp):
        slot = lax.rem(grp, SLOTS)
        for i in range(GROUP):
            row = pl.multiple_of(tile_ref[grp * GROUP + i] * 8, 8)
            pltpu.make_async_copy(table_ref.at[pl.ds(row, 8), :], buf.at[slot, pl.ds(i * 8, 8), :], sems.at[slot]).start()

    @pl.when(step == 0)
    def _():
        for grp in range(SLOTS - 1):
            issue(grp)

    @pl.when(step + SLOTS - 1 < steps)
    def _():
        issue(step + SLOTS - 1)

    slot = lax.rem(step, SLOTS)
    pltpu.make_async_copy(table_ref.at[pl.ds(0, GROUP * 8), :], buf.at[slot], sems.at[slot]).wait()
    for j in range(GROUP // SUB):
        cols = lax.broadcasted_iota(jnp.int32, (SUB, SUB * 8), 1)
        onehot = (cols == sel_ref[pl.ds(j * SUB, SUB), :]).astype(jnp.float32).astype(jnp.bfloat16)
        rows = jnp.dot(onehot, buf[slot, pl.ds(j * SUB * 8, SUB * 8), :], preferred_element_type=jnp.float32)
        out_ref[pl.ds(j * SUB, SUB), :] = rows.astype(jnp.bfloat16)


def lookup(ids, table, tp_rank):
    n_tok = ids.shape[0]
    vocab_loc, d = table.shape
    loc = ids - tp_rank * vocab_loc
    held = (loc >= 0) & (loc < vocab_loc)
    spread = (jnp.arange(n_tok, dtype=jnp.int32) * 5) % (vocab_loc // 8)
    tile = jnp.where(held, loc // 8, spread)
    sel = jnp.where(held, (jnp.arange(n_tok, dtype=jnp.int32) % SUB) * 8 + loc % 8, -1)[:, None]
    return pl.pallas_call(
        lookup_kernel,
        out_shape=jax.ShapeDtypeStruct((n_tok, d), jnp.bfloat16),
        grid_spec=pltpu.PrefetchScalarGridSpec(
            num_scalar_prefetch=1,
            grid=(n_tok // GROUP,),
            in_specs=[pl.BlockSpec((GROUP, 1), lambda i, t: (i, 0)), pl.BlockSpec(memory_space=pl.ANY)],
            out_specs=pl.BlockSpec((GROUP, d), lambda i, t: (i, 0)),
            scratch_shapes=[pltpu.VMEM((SLOTS, GROUP * 8, d), jnp.bfloat16), pltpu.SemaphoreType.DMA((SLOTS,))],
        ),
        compiler_params=pltpu.CompilerParams(dimension_semantics=("arbitrary",)),
        cost_estimate=pl.CostEstimate(flops=n_tok * d * 40000, bytes_accessed=n_tok * d * 18, transcendentals=0),
        name="lookup",
    )(tile, sel, table)


CHUNK = 32
LAG = 2
LN_ROWS = 16


def norm_rows(x, gain, shift):
    n = x.shape[-1]
    mean_v = jnp.sum(x, axis=-1, keepdims=True) * (1.0 / n)
    centered = x - mean_v
    var_v = jnp.sum(centered * centered, axis=-1, keepdims=True) * (1.0 / n)
    return (centered * lax.rsqrt(var_v + LN_EPS) * gain + shift).astype(jnp.bfloat16)


def chain_kernel(n_tp, part_ref, ln_ref, a_ref, r0_ref, own, pre, rgt, lft, abuf, r0buf,
                 own_sem, pre_send, pre_recv, r_send, r_recv, l_send, l_recv, a_loc, a_send, a_recv, r0_loc, r0_send, r0_recv):
    seq = part_ref.shape[1]
    n_chunk = seq // CHUNK
    n_z = n_tp // 2
    me = lax.axis_index("tp")
    z = me // 2
    c = lax.rem(me, 2)
    peer = me + 1 - 2 * c
    pos_per = r0_ref.shape[1]
    per_dev = pos_per // CHUNK
    last = n_z - 1

    barrier = pltpu.get_barrier_semaphore()
    pl.semaphore_signal(barrier, inc=1, device_id={"tp": peer}, device_id_type=MESH)

    @pl.when(z > 0)
    def _():
        pl.semaphore_signal(barrier, inc=1, device_id={"tp": me - 2}, device_id_type=MESH)

    @pl.when(z < last)
    def _():
        pl.semaphore_signal(barrier, inc=1, device_id={"tp": me + 2}, device_id_type=MESH)

    @pl.when((z > 0) & (z < last))
    def _():
        pl.semaphore_wait(barrier, 3)

    @pl.when((z == 0) | (z == last))
    def _():
        pl.semaphore_wait(barrier, 2)

    def rows(k):
        return pl.ds(pl.multiple_of(k * CHUNK, CHUNK), CHUNK)

    def own_copy(k):
        return pltpu.make_async_copy(part_ref.at[c, rows(k), :], own.at[rows(k), :], own_sem.at[k])

    def pre_copy(k):
        return pltpu.make_async_remote_copy(part_ref.at[1 - c, rows(k), :], pre.at[rows(k), :], pre_send.at[k], pre_recv.at[k], device_id={"tp": peer}, device_id_type=MESH)

    def right_copy(src, k):
        return pltpu.make_async_remote_copy(src.at[rows(k), :], rgt.at[rows(k), :], r_send.at[k], r_recv.at[k], device_id={"tp": me + 2}, device_id_type=MESH)

    def left_copy(k):
        return pltpu.make_async_remote_copy(pre.at[rows(k), :], lft.at[rows(k), :], l_send.at[k], l_recv.at[k], device_id={"tp": me - 2}, device_id_type=MESH)

    def a_local(k):
        return pltpu.make_async_copy(abuf.at[rows(k), :], a_ref.at[c, rows(k), :], a_loc.at[k])

    def a_peer(k):
        return pltpu.make_async_remote_copy(abuf.at[rows(k), :], a_ref.at[c, rows(k), :], a_send.at[k], a_recv.at[k], device_id={"tp": peer}, device_id_type=MESH)

    def r0_local(i):
        return pltpu.make_async_copy(r0buf.at[c, rows(i), :], r0_ref.at[c, rows(i), :], r0_loc.at[i])

    def r0_peer(i):
        return pltpu.make_async_remote_copy(r0buf.at[1 - c, rows(i), :], r0_ref.at[c, rows(i), :], r0_send.at[i], r0_recv.at[i], device_id={"tp": peer}, device_id_type=MESH)

    def start(k, carry):
        own_copy(k).start()
        pre_copy(k).start()
        return carry

    lax.fori_loop(0, n_chunk, start, 0)

    def step_body(s, carry):
        @pl.when(s < n_chunk)
        def _():
            own_copy(s).wait()
            pre_copy(s).wait_recv()
            own[rows(s), :] = own[rows(s), :] + pre[rows(s), :]

        kr = s - LAG * z

        @pl.when((kr >= 0) & (kr < n_chunk))
        def _():
            @pl.when(z == 0)
            def _():
                right_copy(own, kr).start()

            @pl.when(z > 0)
            def _():
                right_copy(rgt, kr).wait_recv()
                rgt[rows(kr), :] = rgt[rows(kr), :] + own[rows(kr), :]

                @pl.when(z < last)
                def _():
                    right_copy(rgt, kr).start()

        kl = s - LAG * (last - z)

        @pl.when((kl >= 0) & (kl < n_chunk))
        def _():
            @pl.when(z < last)
            def _():
                left_copy(kl).wait_recv()

                @pl.when(z > 0)
                def _():
                    pre[rows(kl), :] = lft[rows(kl), :] + own[rows(kl), :]

            @pl.when(z == last)
            def _():
                pre[rows(kl), :] = own[rows(kl), :]

            @pl.when(z > 0)
            def _():
                left_copy(kl).start()

        kt = s - LAG * jnp.maximum(z, last - z)

        @pl.when((kt >= 0) & (kt < n_chunk))
        def _():
            base = kt * CHUNK
            first = kt - z * 2 * per_dev
            near = (first >= 0) & (first < 2 * per_dev)
            side = jnp.where(near, first // per_dev, 0)
            inner = jnp.where(near, lax.rem(first, per_dev), 0)

            def norm(i, carry):
                sl = pl.ds(pl.multiple_of(base + i * LN_ROWS, LN_ROWS), LN_ROWS)

                @pl.when(z == 0)
                def _():
                    abuf[sl, :] = own[sl, :] + lft[sl, :]

                @pl.when((z > 0) & (z < last))
                def _():
                    abuf[sl, :] = rgt[sl, :] + lft[sl, :]

                @pl.when(z == last)
                def _():
                    abuf[sl, :] = rgt[sl, :]

                r0 = norm_rows(abuf[sl, :].astype(jnp.float32), ln_ref[0:1, :], ln_ref[1:2, :])
                abuf[sl, :] = norm_rows(r0.astype(jnp.float32), ln_ref[2:3, :], ln_ref[3:4, :])

                @pl.when(near)
                def _():
                    r0buf[side, pl.ds(pl.multiple_of(inner * CHUNK + i * LN_ROWS, LN_ROWS), LN_ROWS), :] = r0

                return carry

            lax.fori_loop(0, CHUNK // LN_ROWS, norm, 0)
            a_local(kt).start()
            a_peer(kt).start()

            @pl.when(near & (side == c))
            def _():
                r0_local(inner).start()

            @pl.when(near & (side != c))
            def _():
                r0_peer(inner).start()

        return carry

    lax.fori_loop(0, n_chunk + LAG * last, step_body, 0)

    def drain(k, carry):
        pre_copy(k).wait_send()
        a_local(k).wait()
        a_peer(k).wait()

        @pl.when(z < last)
        def _():
            right_copy(rgt, k).wait_send()

        @pl.when(z > 0)
        def _():
            left_copy(k).wait_send()

        return carry

    lax.fori_loop(0, n_chunk, drain, 0)

    def drain_r0(i, carry):
        r0_local(i).wait()
        r0_peer(i).wait()
        return carry

    lax.fori_loop(0, per_dev, drain_r0, 0)


def chain(part, ln_pack, n_tp):
    n_seq, seq, d = part.shape
    n_chunk = seq // CHUNK
    per_dev = seq // n_tp // CHUNK
    dma = pltpu.SemaphoreType.DMA
    big = pltpu.VMEM((seq, d), jnp.bfloat16)
    return pl.pallas_call(
        functools.partial(chain_kernel, n_tp),
        out_shape=(jax.ShapeDtypeStruct((n_seq, seq, d), jnp.bfloat16), jax.ShapeDtypeStruct((n_seq, seq // n_tp, d), jnp.bfloat16)),
        in_specs=[pl.BlockSpec(memory_space=pl.ANY), pl.BlockSpec(memory_space=pltpu.VMEM)],
        out_specs=(pl.BlockSpec(memory_space=pl.ANY), pl.BlockSpec(memory_space=pl.ANY)),
        scratch_shapes=[big, big, big, big, big, pltpu.VMEM((2, seq // n_tp, d), jnp.bfloat16)]
        + [dma((n_chunk,))] * 10 + [dma((per_dev,))] * 3,
        compiler_params=pltpu.CompilerParams(collective_id=0, has_side_effects=True, vmem_limit_bytes=58 * 1024 * 1024),
        cost_estimate=pl.CostEstimate(flops=10 ** 6, bytes_accessed=8 * part.size, transcendentals=0),
        name="chain",
    )(part, ln_pack)


def attend_kernel(n_tp, head_dim, qkv_ref, pad_ref, slope_ref, bup_ref, ctx_ref, ball_ref, cbuf, send_sem, recv_sem, loc_sem, b_send, b_recv, b_loc):
    n_seq, heads = qkv_ref.shape[1], qkv_ref.shape[2]
    seq = qkv_ref.shape[3]
    blk = seq // n_tp
    feat = heads * head_dim
    me = lax.axis_index("tp")

    barrier = pltpu.get_barrier_semaphore()
    for r in range(1, n_tp):
        pl.semaphore_signal(barrier, inc=1, device_id={"tp": lax.rem(me + r, n_tp)}, device_id_type=MESH)
    pl.semaphore_wait(barrier, n_tp - 1)

    def cols(t):
        return pl.ds(pl.multiple_of(t * feat, feat), feat)

    def bias_copy(r):
        return pltpu.make_async_remote_copy(bup_ref, ball_ref.at[me], b_send.at[r], b_recv.at[r], device_id={"tp": lax.rem(me + r, n_tp)}, device_id_type=MESH)

    for r in range(1, n_tp):
        bias_copy(r).start()
    own_bias = pltpu.make_async_copy(bup_ref, ball_ref.at[me], b_loc.at[0])
    own_bias.start()

    def ctx_copy(b, r):
        return pltpu.make_async_remote_copy(cbuf.at[b, r], ctx_ref.at[b, :, cols(me)], send_sem.at[b, r], recv_sem.at[b, r], device_id={"tp": lax.rem(me + r, n_tp)}, device_id_type=MESH)

    def ctx_local(b):
        return pltpu.make_async_copy(cbuf.at[b, 0], ctx_ref.at[b, :, cols(me)], loc_sem.at[b])

    def one(i, carry):
        b = lax.rem(i, n_seq)
        turn = i // n_seq
        r = n_tp // 2 + (turn + 1) // 2 * (1 - 2 * lax.rem(turn, 2))
        dest = lax.rem(me + r, n_tp)
        for j in range(n_tp):
            @pl.when(dest == j)
            def _(j=j):
                span = (j + 1) * blk
                lo = j * blk
                key_pos = lax.broadcasted_iota(jnp.int32, (1, span), 1)
                key_ok = pad_ref[b, :, 0:span] == 1
                row_in = lax.broadcasted_iota(jnp.int32, (blk, blk), 0)
                col_in = lax.broadcasted_iota(jnp.int32, (blk, blk), 1)
                diag_ok = ((col_in < row_in) & (pad_ref[b, :, lo:span] == 1)) | (col_in == row_in)
                for h in range(heads):
                    slope = slope_ref[0, h] * LOG2E
                    rel = slope * (key_pos - lo).astype(jnp.float32)
                    far = jnp.where(key_ok, rel, -1e30)
                    q = qkv_ref[0, b, h, lo:span, :]
                    scale = head_dim ** -0.5 * LOG2E
                    diag = lax.dot_general(q, qkv_ref[1, b, h, lo:span, :], (((1,), (1,)), ((), ())), preferred_element_type=jnp.float32)
                    diag = jnp.where(diag_ok, diag * scale + rel[:, lo:span], -1e30)
                    top = jnp.max(diag, axis=-1, keepdims=True)
                    if j:
                        past = lax.dot_general(q, qkv_ref[1, b, h, 0:lo, :], (((1,), (1,)), ((), ())), preferred_element_type=jnp.float32)
                        past = past * scale + far[:, 0:lo]
                        top = jnp.maximum(top, jnp.max(past, axis=-1, keepdims=True))
                        past = jnp.exp2(past - top)
                    diag = jnp.exp2(diag - top)
                    total = jnp.sum(diag, axis=-1, keepdims=True)
                    if j:
                        total = total + jnp.sum(past, axis=-1, keepdims=True)
                    inv = 1.0 / total
                    out = jnp.dot((diag * inv).astype(jnp.bfloat16), qkv_ref[2, b, h, lo:span, :], preferred_element_type=jnp.float32)
                    if j:
                        out = out + jnp.dot((past * inv).astype(jnp.bfloat16), qkv_ref[2, b, h, 0:lo, :], preferred_element_type=jnp.float32)
                    cbuf[b, r, :, h * head_dim:(h + 1) * head_dim] = out.astype(jnp.bfloat16)

        @pl.when(r > 0)
        def _():
            ctx_copy(b, r).start()

        @pl.when(r == 0)
        def _():
            ctx_local(b).start()

        return carry

    lax.fori_loop(0, n_seq * n_tp, one, 0)

    for b in range(n_seq):
        ctx_local(b).wait()
        for r in range(1, n_tp):
            ctx_copy(b, r).wait()
    own_bias.wait()
    for r in range(1, n_tp):
        bias_copy(r).wait()


def attend(qkv, pad_mask, slopes, b_up, n_tp):
    _, n_seq, heads, seq, head_dim = qkv.shape
    blk = seq // n_tp
    feat = heads * head_dim
    dma = pltpu.SemaphoreType.DMA
    vmem = pl.BlockSpec(memory_space=pltpu.VMEM)
    return pl.pallas_call(
        functools.partial(attend_kernel, n_tp, head_dim),
        out_shape=(jax.ShapeDtypeStruct((n_seq, blk, n_tp * feat), jnp.bfloat16), jax.ShapeDtypeStruct((n_tp,) + b_up.shape, jnp.bfloat16)),
        in_specs=[vmem, vmem, pl.BlockSpec(memory_space=pltpu.SMEM), vmem],
        out_specs=(pl.BlockSpec(memory_space=pl.ANY), pl.BlockSpec(memory_space=pl.ANY)),
        scratch_shapes=[pltpu.VMEM((n_seq, n_tp, blk, feat), jnp.bfloat16), dma((n_seq, n_tp)), dma((n_seq, n_tp)), dma((n_seq,)), dma((n_tp,)), dma((n_tp,)), dma((1,))],
        compiler_params=pltpu.CompilerParams(collective_id=1, has_side_effects=True, vmem_limit_bytes=56000 * 1024),
        cost_estimate=pl.CostEstimate(flops=30 * 10 ** 9, bytes_accessed=2 * qkv.size, transcendentals=seq * seq * 2),
        name="attend",
    )(qkv, pad_mask[:, None, :], slopes[None, :], b_up)


SUBROWS = 128


def mlp_kernel(n_dp, ctx_ref, r0_ref, wo_ref, wup_ref, wdn_ref, fup_ref, fdn_ref, bias_ref, vec_ref, out_ref,
               ctx, r0, r1, wo_w, xbuf, ptl, up_w, dn_w, act, from_peer, pre, from_far, obuf,
               w_sem, x_sem, px_send, px_recv, fx_send, fx_recv, fw_send, fw_recv, lp_send, lp_recv, pr_send, pr_recv, rf_send, rf_recv, o_sem):
    me = lax.axis_index("tp")
    peer = me + 1 - 2 * lax.rem(me, 2)
    far = me + 2 - 4 * lax.rem(me // 2, 2)
    mid = 2 * SUBROWS
    n_loc = ctx.shape[0] // mid
    n_sub = ctx.shape[0] // SUBROWS
    steps = 2 * n_loc + n_sub
    first_far = 2 * n_loc
    wide = up_w.shape[2]
    n_up = wup_ref.shape[1] // wide
    n_blk = up_w.shape[0]
    d_loc = wdn_ref.shape[0]
    slim = fup_ref.shape[2]

    barrier = pltpu.get_barrier_semaphore()
    pl.semaphore_signal(barrier, inc=1, device_id={"tp": peer}, device_id_type=MESH)
    pl.semaphore_signal(barrier, inc=1, device_id={"tp": far}, device_id_type=MESH)

    first = [pltpu.make_async_copy(src, dst, x_sem.at[i]) for i, (src, dst) in enumerate([(ctx_ref, ctx), (r0_ref, r0), (wo_ref, wo_w)])]
    for load in first:
        load.start()
    loads = []
    for i in range(n_up):
        loads.append(pltpu.make_async_copy(wup_ref.at[:, pl.ds(i * wide, wide)], up_w.at[i], w_sem.at[len(loads)]))
    for i in range(n_dp):
        loads.append(pltpu.make_async_copy(fup_ref.at[i], up_w.at[n_up + i * slim // wide, :, pl.ds(i * slim % wide, slim)], w_sem.at[len(loads)]))
    loads.append(pltpu.make_async_copy(wdn_ref, dn_w.at[pl.ds(0, d_loc), :], w_sem.at[len(loads)]))
    loads.append(pltpu.make_async_copy(fdn_ref, dn_w.at[pl.ds(d_loc, d_loc), :], w_sem.at[len(loads)]))
    pl.semaphore_wait(barrier, 2)

    def remote(src, dst, send, recv, to):
        return pltpu.make_async_remote_copy(src, dst, send, recv, device_id={"tp": to}, device_id_type=MESH)

    def sub(i):
        return pl.ds(pl.multiple_of(i * SUBROWS, SUBROWS), SUBROWS)

    def x_far(i):
        return remote(xbuf.at[i // 2, sub(lax.rem(i, 2)), :], xbuf.at[first_far + i, pl.ds(0, SUBROWS), :], fx_send.at[i], fx_recv.at[i], far)

    def x_peer(i):
        return remote(xbuf.at[i], xbuf.at[n_loc + i], px_send.at[i], px_recv.at[i], peer)

    def x_pass(i):
        return remote(xbuf.at[first_far + i, pl.ds(0, SUBROWS), :], xbuf.at[first_far + i, pl.ds(SUBROWS, SUBROWS), :], fw_send.at[i], fw_recv.at[i], peer)

    def back_peer(i):
        return remote(ptl.at[n_loc + i], from_peer.at[i], lp_send.at[i], lp_recv.at[i], peer)

    def back_pre(i):
        return remote(ptl.at[first_far + i, pl.ds(SUBROWS, SUBROWS), :], pre.at[i], pr_send.at[i], pr_recv.at[i], peer)

    def back_far(i):
        return remote(ptl.at[first_far + i, pl.ds(0, SUBROWS), :], from_far.at[i], rf_send.at[i], rf_recv.at[i], far)

    for load in first:
        load.wait()
    for load in loads:
        load.start()

    def project(i, carry):
        for g in range(n_dp):
            sl = pl.ds(g * wo_w.shape[2], wo_w.shape[2])
            attn = jnp.dot(ctx[sub(i), :], wo_w[g], preferred_element_type=jnp.float32)
            r1[sub(i), sl] = (r0[sub(i), sl].astype(jnp.float32) + (attn + vec_ref[0:1, sl])).astype(jnp.bfloat16)
        for r in range(0, SUBROWS, 16):
            rows = r1[pl.ds(pl.multiple_of(i * SUBROWS + r, 16), 16), :].astype(jnp.float32)
            xbuf[i // 2, pl.ds(pl.multiple_of(lax.rem(i, 2) * SUBROWS + r, 16), 16), :] = norm_rows(rows, vec_ref[1:2, :], vec_ref[2:3, :])
        x_far(i).start()

        @pl.when(lax.rem(i, 2) == 1)
        def _():
            x_peer(i // 2).start()

        return carry

    lax.fori_loop(0, n_sub, project, 0)
    for load in loads:
        load.wait()

    def body(s, carry):
        @pl.when((s >= 2) & (s < 2 + n_sub))
        def _():
            x_far(s - 2).wait_recv()
            x_pass(s - 2).start()

        @pl.when((s >= n_loc) & (s < first_far))
        def _():
            x_peer(s - n_loc).wait_recv()

        @pl.when((s >= first_far) & (s < steps))
        def _():
            x_pass(s - first_far).wait_recv()

        @pl.when(s < steps)
        def _():
            def up(n, carry):
                hid = jnp.dot(xbuf[s], up_w[n], preferred_element_type=jnp.float32) + bias_ref[n]
                act[:, pl.ds(pl.multiple_of(n * wide, wide), wide)] = bloom_gelu(hid).astype(jnp.bfloat16)
                return carry

            lax.fori_loop(0, n_blk, up, 0)

            def down(n, carry):
                sl = pl.ds(pl.multiple_of(n * wide, wide), wide)
                ptl[s, :, sl] = jnp.dot(act[...], dn_w[:, sl], preferred_element_type=jnp.float32).astype(jnp.bfloat16)
                return carry

            lax.fori_loop(0, dn_w.shape[1] // wide, down, 0)

        @pl.when((s >= n_loc) & (s < first_far))
        def _():
            back_peer(s - n_loc).start()

        @pl.when((s >= first_far) & (s < steps))
        def _():
            back_pre(s - first_far).start()

        @pl.when(s > first_far)
        def _():
            i = s - first_far - 1
            back_pre(i).wait_recv()
            for r in range(0, SUBROWS, 32):
                sl = pl.ds(r, 32)
                ptl[first_far + i, sl, :] = (ptl[first_far + i, sl, :].astype(jnp.float32) + pre[i, sl, :].astype(jnp.float32)).astype(jnp.bfloat16)
            back_far(i).start()

        return carry

    lax.fori_loop(0, steps + 1, body, 0)

    for i in range(n_loc):
        back_peer(i).wait_recv()

    def out_copy(i):
        return pltpu.make_async_copy(obuf.at[sub(i), :], out_ref.at[sub(i), :], o_sem.at[i])

    def finish(i, carry):
        back_far(i).wait_recv()
        for r in range(0, SUBROWS, 16):
            own = pl.ds(pl.multiple_of(lax.rem(i, 2) * SUBROWS + r, 16), 16)
            row = pl.ds(pl.multiple_of(i * SUBROWS + r, 16), 16)
            total = ptl[i // 2, own, :].astype(jnp.float32) + from_peer[i // 2, own, :].astype(jnp.float32) + from_far[i, pl.ds(r, 16), :].astype(jnp.float32)
            obuf[row, :] = (r1[row, :].astype(jnp.float32) + (total + vec_ref[3:4, :])).astype(jnp.bfloat16)
        out_copy(i).start()
        return carry

    lax.fori_loop(0, n_sub, finish, 0)
    for i in range(n_loc):
        x_peer(i).wait_send()
        back_peer(i).wait_send()
    for i in range(n_sub):
        x_far(i).wait_send()
        x_pass(i).wait_send()
        back_pre(i).wait_send()
        back_far(i).wait_send()
        out_copy(i).wait()


def mlp(context, r0, wo, w_up, w_down, far_up, far_down, bias, vecs):
    rows, d = context.shape
    ff = w_up.shape[1]
    wide = 512
    mid = 2 * SUBROWS
    n_loc, n_sub = rows // mid, rows // SUBROWS
    steps = 2 * n_loc + n_sub
    n_dp = far_up.shape[0]
    bf = jnp.bfloat16
    dma = pltpu.SemaphoreType.DMA
    hbm = pl.BlockSpec(memory_space=pl.ANY)
    vmem = pl.BlockSpec(memory_space=pltpu.VMEM)
    return pl.pallas_call(
        functools.partial(mlp_kernel, n_dp),
        out_shape=jax.ShapeDtypeStruct((rows, d), bf),
        in_specs=[hbm] * 7 + [vmem] * 2,
        out_specs=hbm,
        scratch_shapes=[
            pltpu.VMEM((rows, d), bf), pltpu.VMEM((rows, d), bf), pltpu.VMEM((rows, d), bf), pltpu.VMEM(wo.shape, bf), pltpu.VMEM((steps, mid, d), bf), pltpu.VMEM((steps, mid, d), bf), pltpu.VMEM((2 * ff // wide, d, wide), bf), pltpu.VMEM((2 * ff, d), bf),
            pltpu.VMEM((mid, 2 * ff), bf), pltpu.VMEM((n_loc, mid, d), bf), pltpu.VMEM((n_sub, SUBROWS, d), bf), pltpu.VMEM((n_sub, SUBROWS, d), bf), pltpu.VMEM((rows, d), bf),
            dma((32,)), dma((3,)), dma((n_loc,)), dma((n_loc,)), dma((n_sub,)), dma((n_sub,)), dma((n_sub,)), dma((n_sub,)),
            dma((n_loc,)), dma((n_loc,)), dma((n_sub,)), dma((n_sub,)), dma((n_sub,)), dma((n_sub,)), dma((n_sub,)),
        ],
        compiler_params=pltpu.CompilerParams(collective_id=2, has_side_effects=True, vmem_limit_bytes=61900 * 1024),
        cost_estimate=pl.CostEstimate(flops=10 ** 12, bytes_accessed=40 * 10 ** 6, transcendentals=0),
        name="mlp",
    )(context, r0, wo, w_up, w_down, far_up, far_down, bias.reshape(2 * ff // wide, 1, wide), vecs)


def solution(mesh):
    n_tp = mesh.shape['tp']
    n_dp = mesh.shape['dp']

    def local_step(tok_ids, pad_mask, emb_shard, ln_emb_w, ln_emb_b, ln1_w, ln1_b, w_qkv, b_qkv, w_out, b_out, ln2_w, ln2_b, w_up, b_up, w_down, b_down):
        f32 = jnp.float32
        tp_rank = lax.axis_index('tp')
        dp_rank = lax.axis_index('dp')
        n_seq, seq = tok_ids.shape
        d = emb_shard.shape[1]
        heads_loc = w_qkv.shape[1]

        def part(w, axis):
            size = w.shape[axis] // n_dp
            return lax.dynamic_slice_in_dim(w, dp_rank * size, size, axis)

        half = n_tp // 2
        swap = [(t, (t + half) % n_tp) for t in range(n_tp)]
        out_part = lax.all_gather(part(w_out, 1), 'tp', axis=0, tiled=True)
        up_part = lax.ppermute(part(w_up, 1), 'tp', swap)
        down_part = lax.ppermute(part(w_down, 0), 'tp', swap)

        part_emb = lookup(tok_ids.reshape(-1), emb_shard, tp_rank)
        part_emb = part_emb.reshape(n_seq, seq, d)
        part_emb, up_part, out_part = lax.optimization_barrier((part_emb, up_part, out_part))
        wo = lax.all_gather(out_part, 'dp', axis=0, tiled=False)
        wu = lax.all_gather(up_part, 'dp', axis=0, tiled=False)
        ln_pack = jnp.stack([ln_emb_w, ln_emb_b, ln1_w, ln1_b]).astype(f32)
        normed_all, resid_in = chain(part_emb, ln_pack, n_tp)
        normed_all, wu, wo, down_part = lax.optimization_barrier((normed_all, wu, wo, down_part))
        wd = lax.all_gather(down_part, 'dp', axis=0, tiled=True)
        qkv = (jnp.einsum('bsd,dhce->cbhse', normed_all, w_qkv, preferred_element_type=f32) + b_qkv.astype(f32).transpose(1, 0, 2)[:, None, :, None, :]).astype(jnp.bfloat16)
        all_slopes = jnp.array(alibi_slopes(heads_loc * n_tp), f32)
        head_slopes = lax.dynamic_slice_in_dim(all_slopes, tp_rank * heads_loc, heads_loc)
        context, b_all = attend(qkv, pad_mask, head_slopes, b_up.reshape(8, -1), n_tp)
        context, wd = lax.optimization_barrier((context, wd))
        far_bias = lax.dynamic_index_in_dim(b_all, (tp_rank + half) % n_tp, 0, keepdims=False).reshape(-1)
        bias = jnp.concatenate([b_up, far_bias]).astype(f32)
        rows = n_seq * seq // n_tp
        vecs = jnp.stack([b_out, ln2_w, ln2_b, b_down]).astype(f32)
        out = mlp(context.reshape(rows, d), resid_in.reshape(rows, d), wo, w_up, w_down, wu, wd, bias, vecs)
        return out.reshape(n_seq, seq // n_tp, d)

    replicated = P(None)
    in_specs = (P('dp', None), P('dp', None), P('tp', None), replicated, replicated, replicated, replicated, P(None, 'tp', None, None), P('tp', None, None), P('tp', None), replicated, replicated, replicated, P(None, 'tp'), P('tp'), P('tp', None), replicated)
    return jax.shard_map(local_step, mesh=mesh, in_specs=in_specs, out_specs=P('dp', 'tp', None), check_vma=False)
```

```python
import functools
import math
import jax
import jax.numpy as jnp
from jax import lax
from jax.experimental import pallas as pl
from jax.experimental.pallas import tpu as pltpu
from jax.sharding import PartitionSpec as P

LN_EPS = 1e-5
LOG2E = 1.4426950408889634
MESH = pl.DeviceIdType.MESH


def alibi_slopes(n_heads):
    closest = 2 ** int(math.floor(math.log2(n_heads)))
    base_ratio = 2.0 ** (-(2.0 ** -(math.log2(closest) - 3)))
    extra_ratio = 2.0 ** (-(2.0 ** -(math.log2(2 * closest) - 3)))
    first_part = [base_ratio ** step_k for step_k in range(1, closest + 1)]
    second_part = [extra_ratio ** step_k for step_k in range(1, 2 * (n_heads - closest), 2)]
    return first_part + second_part


def bloom_gelu(values_in):
    return values_in * 0.5 * (1.0 + jnp.tanh(0.79788456 * values_in * (1.0 + 0.044715 * values_in * values_in)))


GROUP = 64
SUB = 32
SLOTS = 4


def lookup_kernel(tile_ref, sel_ref, table_ref, out_ref, buf, sems):
    step = pl.program_id(0)
    steps = pl.num_programs(0)

    def issue(grp):
        slot = lax.rem(grp, SLOTS)
        for i in range(GROUP):
            row = pl.multiple_of(tile_ref[grp * GROUP + i] * 8, 8)
            pltpu.make_async_copy(table_ref.at[pl.ds(row, 8), :], buf.at[slot, pl.ds(i * 8, 8), :], sems.at[slot]).start()

    @pl.when(step == 0)
    def _():
        for grp in range(SLOTS - 1):
            issue(grp)

    @pl.when(step + SLOTS - 1 < steps)
    def _():
        issue(step + SLOTS - 1)

    slot = lax.rem(step, SLOTS)
    pltpu.make_async_copy(table_ref.at[pl.ds(0, GROUP * 8), :], buf.at[slot], sems.at[slot]).wait()
    for j in range(GROUP // SUB):
        cols = lax.broadcasted_iota(jnp.int32, (SUB, SUB * 8), 1)
        onehot = (cols == sel_ref[pl.ds(j * SUB, SUB), :]).astype(jnp.float32).astype(jnp.bfloat16)
        rows = jnp.dot(onehot, buf[slot, pl.ds(j * SUB * 8, SUB * 8), :], preferred_element_type=jnp.float32)
        out_ref[pl.ds(j * SUB, SUB), :] = rows.astype(jnp.bfloat16)


def lookup(ids, table, tp_rank):
    n_tok = ids.shape[0]
    vocab_loc, d = table.shape
    loc = ids - tp_rank * vocab_loc
    held = (loc >= 0) & (loc < vocab_loc)
    spread = (jnp.arange(n_tok, dtype=jnp.int32) * 5) % (vocab_loc // 8)
    tile = jnp.where(held, loc // 8, spread)
    sel = jnp.where(held, (jnp.arange(n_tok, dtype=jnp.int32) % SUB) * 8 + loc % 8, -1)[:, None]
    return pl.pallas_call(
        lookup_kernel,
        out_shape=jax.ShapeDtypeStruct((n_tok, d), jnp.bfloat16),
        grid_spec=pltpu.PrefetchScalarGridSpec(
            num_scalar_prefetch=1,
            grid=(n_tok // GROUP,),
            in_specs=[pl.BlockSpec((GROUP, 1), lambda i, t: (i, 0)), pl.BlockSpec(memory_space=pl.ANY)],
            out_specs=pl.BlockSpec((GROUP, d), lambda i, t: (i, 0)),
            scratch_shapes=[pltpu.VMEM((SLOTS, GROUP * 8, d), jnp.bfloat16), pltpu.SemaphoreType.DMA((SLOTS,))],
        ),
        compiler_params=pltpu.CompilerParams(dimension_semantics=("arbitrary",)),
        cost_estimate=pl.CostEstimate(flops=n_tok * d * 40000, bytes_accessed=n_tok * d * 18, transcendentals=0),
        name="lookup",
    )(tile, sel, table)


CHUNK = 32
LAG = 2
LN_ROWS = 16


def norm_rows(x, gain, shift):
    n = x.shape[-1]
    mean_v = jnp.sum(x, axis=-1, keepdims=True) * (1.0 / n)
    centered = x - mean_v
    var_v = jnp.sum(centered * centered, axis=-1, keepdims=True) * (1.0 / n)
    return (centered * lax.rsqrt(var_v + LN_EPS) * gain + shift).astype(jnp.bfloat16)


def chain_kernel(n_tp, part_a, part_b, ln_ref, a_ref, r0_ref, own, pre, rgt, lft, abuf, r0buf,
                 own_sem, pre_send, pre_recv, r_send, r_recv, l_send, l_recv, a_loc, a_send, a_recv, r0_loc, r0_send, r0_recv):
    seq = part_a.shape[0]
    n_chunk = seq // CHUNK
    n_z = n_tp // 2
    me = lax.axis_index("tp")
    z = me // 2
    c = lax.rem(me, 2)
    peer = me + 1 - 2 * c
    pos_per = r0_ref.shape[1]
    per_dev = pos_per // CHUNK
    last = n_z - 1

    barrier = pltpu.get_barrier_semaphore()
    pl.semaphore_signal(barrier, inc=1, device_id={"tp": peer}, device_id_type=MESH)

    @pl.when(z > 0)
    def _():
        pl.semaphore_signal(barrier, inc=1, device_id={"tp": me - 2}, device_id_type=MESH)

    @pl.when(z < last)
    def _():
        pl.semaphore_signal(barrier, inc=1, device_id={"tp": me + 2}, device_id_type=MESH)

    @pl.when((z > 0) & (z < last))
    def _():
        pl.semaphore_wait(barrier, 3)

    @pl.when((z == 0) | (z == last))
    def _():
        pl.semaphore_wait(barrier, 2)

    def rows(k):
        return pl.ds(pl.multiple_of(k * CHUNK, CHUNK), CHUNK)

    def own_copy(k, part=part_a):
        return pltpu.make_async_copy(part.at[rows(k), :], own.at[rows(k), :], own_sem.at[k])

    def pre_copy(k, part=part_a):
        return pltpu.make_async_remote_copy(part.at[rows(k), :], pre.at[rows(k), :], pre_send.at[k], pre_recv.at[k], device_id={"tp": peer}, device_id_type=MESH)

    def right_copy(src, k):
        return pltpu.make_async_remote_copy(src.at[rows(k), :], rgt.at[rows(k), :], r_send.at[k], r_recv.at[k], device_id={"tp": me + 2}, device_id_type=MESH)

    def left_copy(k):
        return pltpu.make_async_remote_copy(pre.at[rows(k), :], lft.at[rows(k), :], l_send.at[k], l_recv.at[k], device_id={"tp": me - 2}, device_id_type=MESH)

    def a_local(k):
        return pltpu.make_async_copy(abuf.at[rows(k), :], a_ref.at[c, rows(k), :], a_loc.at[k])

    def a_peer(k):
        return pltpu.make_async_remote_copy(abuf.at[rows(k), :], a_ref.at[c, rows(k), :], a_send.at[k], a_recv.at[k], device_id={"tp": peer}, device_id_type=MESH)

    def r0_local(i):
        return pltpu.make_async_copy(r0buf.at[c, rows(i), :], r0_ref.at[c, rows(i), :], r0_loc.at[i])

    def r0_peer(i):
        return pltpu.make_async_remote_copy(r0buf.at[1 - c, rows(i), :], r0_ref.at[c, rows(i), :], r0_send.at[i], r0_recv.at[i], device_id={"tp": peer}, device_id_type=MESH)

    def start(k, carry):
        @pl.when(c == 0)
        def _():
            own_copy(k, part_a).start()
            pre_copy(k, part_b).start()

        @pl.when(c == 1)
        def _():
            own_copy(k, part_b).start()
            pre_copy(k, part_a).start()

        return carry

    lax.fori_loop(0, n_chunk, start, 0)

    def step_body(s, carry):
        @pl.when(s < n_chunk)
        def _():
            own_copy(s).wait()
            pre_copy(s).wait_recv()
            own[rows(s), :] = own[rows(s), :] + pre[rows(s), :]

        kr = s - LAG * z

        @pl.when((kr >= 0) & (kr < n_chunk))
        def _():
            @pl.when(z == 0)
            def _():
                right_copy(own, kr).start()

            @pl.when(z > 0)
            def _():
                right_copy(rgt, kr).wait_recv()
                rgt[rows(kr), :] = rgt[rows(kr), :] + own[rows(kr), :]

                @pl.when(z < last)
                def _():
                    right_copy(rgt, kr).start()

        kl = s - LAG * (last - z)

        @pl.when((kl >= 0) & (kl < n_chunk))
        def _():
            @pl.when(z < last)
            def _():
                left_copy(kl).wait_recv()

                @pl.when(z > 0)
                def _():
                    pre[rows(kl), :] = lft[rows(kl), :] + own[rows(kl), :]

            @pl.when(z == last)
            def _():
                pre[rows(kl), :] = own[rows(kl), :]

            @pl.when(z > 0)
            def _():
                left_copy(kl).start()

        kt = s - LAG * jnp.maximum(z, last - z)

        @pl.when((kt >= 0) & (kt < n_chunk))
        def _():
            base = kt * CHUNK
            first = kt - z * 2 * per_dev
            near = (first >= 0) & (first < 2 * per_dev)
            side = jnp.where(near, first // per_dev, 0)
            inner = jnp.where(near, lax.rem(first, per_dev), 0)

            def norm(i, carry):
                sl = pl.ds(pl.multiple_of(base + i * LN_ROWS, LN_ROWS), LN_ROWS)

                @pl.when(z == 0)
                def _():
                    abuf[sl, :] = own[sl, :] + lft[sl, :]

                @pl.when((z > 0) & (z < last))
                def _():
                    abuf[sl, :] = rgt[sl, :] + lft[sl, :]

                @pl.when(z == last)
                def _():
                    abuf[sl, :] = rgt[sl, :]

                r0 = norm_rows(abuf[sl, :].astype(jnp.float32), ln_ref[0:1, :], ln_ref[1:2, :])
                abuf[sl, :] = norm_rows(r0.astype(jnp.float32), ln_ref[2:3, :], ln_ref[3:4, :])

                @pl.when(near)
                def _():
                    r0buf[side, pl.ds(pl.multiple_of(inner * CHUNK + i * LN_ROWS, LN_ROWS), LN_ROWS), :] = r0

                return carry

            lax.fori_loop(0, CHUNK // LN_ROWS, norm, 0)
            a_local(kt).start()
            a_peer(kt).start()

            @pl.when(near & (side == c))
            def _():
                r0_local(inner).start()

            @pl.when(near & (side != c))
            def _():
                r0_peer(inner).start()

        return carry

    lax.fori_loop(0, n_chunk + LAG * last, step_body, 0)

    def drain(k, carry):
        pre_copy(k).wait_send()
        a_local(k).wait()
        a_peer(k).wait()

        @pl.when(z < last)
        def _():
            right_copy(rgt, k).wait_send()

        @pl.when(z > 0)
        def _():
            left_copy(k).wait_send()

        return carry

    lax.fori_loop(0, n_chunk, drain, 0)

    def drain_r0(i, carry):
        r0_local(i).wait()
        r0_peer(i).wait()
        return carry

    lax.fori_loop(0, per_dev, drain_r0, 0)


def chain(part_a, part_b, ln_pack, n_tp):
    n_seq = 2
    seq, d = part_a.shape
    n_chunk = seq // CHUNK
    per_dev = seq // n_tp // CHUNK
    dma = pltpu.SemaphoreType.DMA
    big = pltpu.VMEM((seq, d), jnp.bfloat16)
    return pl.pallas_call(
        functools.partial(chain_kernel, n_tp),
        out_shape=(jax.ShapeDtypeStruct((n_seq, seq, d), jnp.bfloat16), jax.ShapeDtypeStruct((n_seq, seq // n_tp, d), jnp.bfloat16)),
        in_specs=[pl.BlockSpec(memory_space=pl.ANY), pl.BlockSpec(memory_space=pl.ANY), pl.BlockSpec(memory_space=pltpu.VMEM)],
        out_specs=(pl.BlockSpec(memory_space=pl.ANY), pl.BlockSpec(memory_space=pl.ANY)),
        scratch_shapes=[big, big, big, big, big, pltpu.VMEM((2, seq // n_tp, d), jnp.bfloat16)]
        + [dma((n_chunk,))] * 10 + [dma((per_dev,))] * 3,
        compiler_params=pltpu.CompilerParams(collective_id=0, has_side_effects=True, vmem_limit_bytes=58 * 1024 * 1024),
        cost_estimate=pl.CostEstimate(flops=10 ** 6, bytes_accessed=16 * part_a.size, transcendentals=0),
        name="chain",
    )(part_a, part_b, ln_pack)


def attend_kernel(n_tp, head_dim, qkv_ref, pad_ref, slope_ref, bup_ref, ctx_ref, ball_ref, cbuf, send_sem, recv_sem, loc_sem, b_send, b_recv, b_loc):
    n_seq, heads = qkv_ref.shape[1], qkv_ref.shape[2]
    seq = qkv_ref.shape[3]
    blk = seq // n_tp
    feat = heads * head_dim
    me = lax.axis_index("tp")

    barrier = pltpu.get_barrier_semaphore()
    for r in range(1, n_tp):
        pl.semaphore_signal(barrier, inc=1, device_id={"tp": lax.rem(me + r, n_tp)}, device_id_type=MESH)
    pl.semaphore_wait(barrier, n_tp - 1)

    def cols(t):
        return pl.ds(pl.multiple_of(t * feat, feat), feat)

    def bias_copy(r):
        return pltpu.make_async_remote_copy(bup_ref, ball_ref.at[me], b_send.at[r], b_recv.at[r], device_id={"tp": lax.rem(me + r, n_tp)}, device_id_type=MESH)

    for r in range(1, n_tp):
        bias_copy(r).start()
    own_bias = pltpu.make_async_copy(bup_ref, ball_ref.at[me], b_loc.at[0])
    own_bias.start()

    def ctx_copy(b, r):
        return pltpu.make_async_remote_copy(cbuf.at[b, r], ctx_ref.at[b, :, cols(me)], send_sem.at[b, r], recv_sem.at[b, r], device_id={"tp": lax.rem(me + r, n_tp)}, device_id_type=MESH)

    def ctx_local(b):
        return pltpu.make_async_copy(cbuf.at[b, 0], ctx_ref.at[b, :, cols(me)], loc_sem.at[b])

    def one(i, carry):
        b = lax.rem(i, n_seq)
        turn = i // n_seq
        r = n_tp // 2 + (turn + 1) // 2 * (1 - 2 * lax.rem(turn, 2))
        dest = lax.rem(me + r, n_tp)
        for j in range(n_tp):
            @pl.when(dest == j)
            def _(j=j):
                span = (j + 1) * blk
                lo = j * blk
                key_pos = lax.broadcasted_iota(jnp.int32, (1, span), 1)
                key_ok = pad_ref[b, :, 0:span] == 1
                row_in = lax.broadcasted_iota(jnp.int32, (blk, blk), 0)
                col_in = lax.broadcasted_iota(jnp.int32, (blk, blk), 1)
                diag_ok = ((col_in < row_in) & (pad_ref[b, :, lo:span] == 1)) | (col_in == row_in)
                for h in range(heads):
                    slope = slope_ref[0, h] * LOG2E
                    rel = slope * (key_pos - lo).astype(jnp.float32)
                    far = jnp.where(key_ok, rel, -1e30)
                    q = qkv_ref[0, b, h, lo:span, :]
                    scale = head_dim ** -0.5 * LOG2E
                    diag = lax.dot_general(q, qkv_ref[1, b, h, lo:span, :], (((1,), (1,)), ((), ())), preferred_element_type=jnp.float32)
                    diag = jnp.where(diag_ok, diag * scale + rel[:, lo:span], -1e30)
                    top = jnp.max(diag, axis=-1, keepdims=True)
                    if j:
                        past = lax.dot_general(q, qkv_ref[1, b, h, 0:lo, :], (((1,), (1,)), ((), ())), preferred_element_type=jnp.float32)
                        past = past * scale + far[:, 0:lo]
                        top = jnp.maximum(top, jnp.max(past, axis=-1, keepdims=True))
                        past = jnp.exp2(past - top)
                    diag = jnp.exp2(diag - top)
                    total = jnp.sum(diag, axis=-1, keepdims=True)
                    if j:
                        total = total + jnp.sum(past, axis=-1, keepdims=True)
                    inv = 1.0 / total
                    out = jnp.dot((diag * inv).astype(jnp.bfloat16), qkv_ref[2, b, h, lo:span, :], preferred_element_type=jnp.float32)
                    if j:
                        out = out + jnp.dot((past * inv).astype(jnp.bfloat16), qkv_ref[2, b, h, 0:lo, :], preferred_element_type=jnp.float32)
                    cbuf[b, r, :, h * head_dim:(h + 1) * head_dim] = out.astype(jnp.bfloat16)

        @pl.when(r > 0)
        def _():
            ctx_copy(b, r).start()

        @pl.when(r == 0)
        def _():
            ctx_local(b).start()

        return carry

    lax.fori_loop(0, n_seq * n_tp, one, 0)

    for b in range(n_seq):
        ctx_local(b).wait()
        for r in range(1, n_tp):
            ctx_copy(b, r).wait()
    own_bias.wait()
    for r in range(1, n_tp):
        bias_copy(r).wait()


def attend(qkv, pad_mask, slopes, b_up, n_tp):
    _, n_seq, heads, seq, head_dim = qkv.shape
    blk = seq // n_tp
    feat = heads * head_dim
    dma = pltpu.SemaphoreType.DMA
    vmem = pl.BlockSpec(memory_space=pltpu.VMEM)
    return pl.pallas_call(
        functools.partial(attend_kernel, n_tp, head_dim),
        out_shape=(jax.ShapeDtypeStruct((n_seq, blk, n_tp * feat), jnp.bfloat16), jax.ShapeDtypeStruct((n_tp,) + b_up.shape, jnp.bfloat16)),
        in_specs=[vmem, vmem, pl.BlockSpec(memory_space=pltpu.SMEM), vmem],
        out_specs=(pl.BlockSpec(memory_space=pl.ANY), pl.BlockSpec(memory_space=pl.ANY)),
        scratch_shapes=[pltpu.VMEM((n_seq, n_tp, blk, feat), jnp.bfloat16), dma((n_seq, n_tp)), dma((n_seq, n_tp)), dma((n_seq,)), dma((n_tp,)), dma((n_tp,)), dma((1,))],
        compiler_params=pltpu.CompilerParams(collective_id=1, has_side_effects=True, vmem_limit_bytes=56000 * 1024),
        cost_estimate=pl.CostEstimate(flops=30 * 10 ** 9, bytes_accessed=2 * qkv.size, transcendentals=seq * seq * 2),
        name="attend",
    )(qkv, pad_mask[:, None, :], slopes[None, :], b_up)


SUBROWS = 128


def mlp_kernel(n_dp, ctx_ref, r0_ref, wo_ref, wup_ref, wdn_ref, fup_ref, fdn_ref, bias_ref, vec_ref, out_ref,
               ctx, r0, r1, wo_w, xbuf, ptl, up_w, dn_w, act, from_peer, pre, from_far, obuf,
               w_sem, x_sem, px_send, px_recv, fx_send, fx_recv, fw_send, fw_recv, lp_send, lp_recv, pr_send, pr_recv, rf_send, rf_recv, o_sem):
    me = lax.axis_index("tp")
    peer = me + 1 - 2 * lax.rem(me, 2)
    far = me + 2 - 4 * lax.rem(me // 2, 2)
    mid = 2 * SUBROWS
    n_loc = ctx.shape[0] // mid
    n_sub = ctx.shape[0] // SUBROWS
    steps = 2 * n_loc + n_sub
    first_far = 2 * n_loc
    wide = up_w.shape[2]
    n_up = wup_ref.shape[1] // wide
    n_blk = up_w.shape[0]
    d_loc = wdn_ref.shape[0]
    slim = fup_ref.shape[2]

    barrier = pltpu.get_barrier_semaphore()
    pl.semaphore_signal(barrier, inc=1, device_id={"tp": peer}, device_id_type=MESH)
    pl.semaphore_signal(barrier, inc=1, device_id={"tp": far}, device_id_type=MESH)

    first = [pltpu.make_async_copy(src, dst, x_sem.at[i]) for i, (src, dst) in enumerate([(ctx_ref, ctx), (r0_ref, r0), (wo_ref, wo_w)])]
    for load in first:
        load.start()
    loads = []
    for i in range(n_up):
        loads.append(pltpu.make_async_copy(wup_ref.at[:, pl.ds(i * wide, wide)], up_w.at[i], w_sem.at[len(loads)]))
    for i in range(n_dp):
        loads.append(pltpu.make_async_copy(fup_ref.at[i], up_w.at[n_up + i * slim // wide, :, pl.ds(i * slim % wide, slim)], w_sem.at[len(loads)]))
    loads.append(pltpu.make_async_copy(wdn_ref, dn_w.at[pl.ds(0, d_loc), :], w_sem.at[len(loads)]))
    loads.append(pltpu.make_async_copy(fdn_ref, dn_w.at[pl.ds(d_loc, d_loc), :], w_sem.at[len(loads)]))
    pl.semaphore_wait(barrier, 2)

    def remote(src, dst, send, recv, to):
        return pltpu.make_async_remote_copy(src, dst, send, recv, device_id={"tp": to}, device_id_type=MESH)

    def sub(i):
        return pl.ds(pl.multiple_of(i * SUBROWS, SUBROWS), SUBROWS)

    def x_far(i):
        return remote(xbuf.at[i // 2, sub(lax.rem(i, 2)), :], xbuf.at[first_far + i, pl.ds(0, SUBROWS), :], fx_send.at[i], fx_recv.at[i], far)

    def x_peer(i):
        return remote(xbuf.at[i], xbuf.at[n_loc + i], px_send.at[i], px_recv.at[i], peer)

    def x_pass(i):
        return remote(xbuf.at[first_far + i, pl.ds(0, SUBROWS), :], xbuf.at[first_far + i, pl.ds(SUBROWS, SUBROWS), :], fw_send.at[i], fw_recv.at[i], peer)

    def back_peer(i):
        return remote(ptl.at[n_loc + i], from_peer.at[i], lp_send.at[i], lp_recv.at[i], peer)

    def back_pre(i):
        return remote(ptl.at[first_far + i, pl.ds(SUBROWS, SUBROWS), :], pre.at[i], pr_send.at[i], pr_recv.at[i], peer)

    def back_far(i):
        return remote(ptl.at[first_far + i, pl.ds(0, SUBROWS), :], from_far.at[i], rf_send.at[i], rf_recv.at[i], far)

    for load in first:
        load.wait()
    for load in loads:
        load.start()

    def project(i, carry):
        for g in range(n_dp):
            sl = pl.ds(g * wo_w.shape[2], wo_w.shape[2])
            attn = jnp.dot(ctx[sub(i), :], wo_w[g], preferred_element_type=jnp.float32)
            r1[sub(i), sl] = (r0[sub(i), sl].astype(jnp.float32) + (attn + vec_ref[0:1, sl])).astype(jnp.bfloat16)
        for r in range(0, SUBROWS, 16):
            rows = r1[pl.ds(pl.multiple_of(i * SUBROWS + r, 16), 16), :].astype(jnp.float32)
            xbuf[i // 2, pl.ds(pl.multiple_of(lax.rem(i, 2) * SUBROWS + r, 16), 16), :] = norm_rows(rows, vec_ref[1:2, :], vec_ref[2:3, :])
        x_far(i).start()

        @pl.when(lax.rem(i, 2) == 1)
        def _():
            x_peer(i // 2).start()

        return carry

    lax.fori_loop(0, n_sub, project, 0)
    for load in loads:
        load.wait()

    def body(s, carry):
        @pl.when((s >= 2) & (s < 2 + n_sub))
        def _():
            x_far(s - 2).wait_recv()
            x_pass(s - 2).start()

        @pl.when((s >= n_loc) & (s < first_far))
        def _():
            x_peer(s - n_loc).wait_recv()

        @pl.when((s >= first_far) & (s < steps))
        def _():
            x_pass(s - first_far).wait_recv()

        @pl.when(s < steps)
        def _():
            def up(n, carry):
                hid = jnp.dot(xbuf[s], up_w[n], preferred_element_type=jnp.float32) + bias_ref[n]
                act[:, pl.ds(pl.multiple_of(n * wide, wide), wide)] = bloom_gelu(hid).astype(jnp.bfloat16)
                return carry

            lax.fori_loop(0, n_blk, up, 0)

            def down(n, carry):
                sl = pl.ds(pl.multiple_of(n * wide, wide), wide)
                ptl[s, :, sl] = jnp.dot(act[...], dn_w[:, sl], preferred_element_type=jnp.float32).astype(jnp.bfloat16)
                return carry

            lax.fori_loop(0, dn_w.shape[1] // wide, down, 0)

        @pl.when((s >= n_loc) & (s < first_far))
        def _():
            back_peer(s - n_loc).start()

        @pl.when((s >= first_far) & (s < steps))
        def _():
            back_pre(s - first_far).start()

        @pl.when(s > first_far)
        def _():
            i = s - first_far - 1
            back_pre(i).wait_recv()
            for r in range(0, SUBROWS, 32):
                sl = pl.ds(r, 32)
                ptl[first_far + i, sl, :] = (ptl[first_far + i, sl, :].astype(jnp.float32) + pre[i, sl, :].astype(jnp.float32)).astype(jnp.bfloat16)
            back_far(i).start()

        return carry

    lax.fori_loop(0, steps + 1, body, 0)

    for i in range(n_loc):
        back_peer(i).wait_recv()

    def out_copy(i):
        return pltpu.make_async_copy(obuf.at[sub(i), :], out_ref.at[sub(i), :], o_sem.at[i])

    def finish(i, carry):
        back_far(i).wait_recv()
        for r in range(0, SUBROWS, 16):
            own = pl.ds(pl.multiple_of(lax.rem(i, 2) * SUBROWS + r, 16), 16)
            row = pl.ds(pl.multiple_of(i * SUBROWS + r, 16), 16)
            total = ptl[i // 2, own, :].astype(jnp.float32) + from_peer[i // 2, own, :].astype(jnp.float32) + from_far[i, pl.ds(r, 16), :].astype(jnp.float32)
            obuf[row, :] = (r1[row, :].astype(jnp.float32) + (total + vec_ref[3:4, :])).astype(jnp.bfloat16)
        out_copy(i).start()
        return carry

    lax.fori_loop(0, n_sub, finish, 0)
    for i in range(n_loc):
        x_peer(i).wait_send()
        back_peer(i).wait_send()
    for i in range(n_sub):
        x_far(i).wait_send()
        x_pass(i).wait_send()
        back_pre(i).wait_send()
        back_far(i).wait_send()
        out_copy(i).wait()


def mlp(context, r0, wo, w_up, w_down, far_up, far_down, bias, vecs):
    rows, d = context.shape
    ff = w_up.shape[1]
    wide = 512
    mid = 2 * SUBROWS
    n_loc, n_sub = rows // mid, rows // SUBROWS
    steps = 2 * n_loc + n_sub
    n_dp = far_up.shape[0]
    bf = jnp.bfloat16
    dma = pltpu.SemaphoreType.DMA
    hbm = pl.BlockSpec(memory_space=pl.ANY)
    vmem = pl.BlockSpec(memory_space=pltpu.VMEM)
    return pl.pallas_call(
        functools.partial(mlp_kernel, n_dp),
        out_shape=jax.ShapeDtypeStruct((rows, d), bf),
        in_specs=[hbm] * 7 + [vmem] * 2,
        out_specs=hbm,
        scratch_shapes=[
            pltpu.VMEM((rows, d), bf), pltpu.VMEM((rows, d), bf), pltpu.VMEM((rows, d), bf), pltpu.VMEM(wo.shape, bf), pltpu.VMEM((steps, mid, d), bf), pltpu.VMEM((steps, mid, d), bf), pltpu.VMEM((2 * ff // wide, d, wide), bf), pltpu.VMEM((2 * ff, d), bf),
            pltpu.VMEM((mid, 2 * ff), bf), pltpu.VMEM((n_loc, mid, d), bf), pltpu.VMEM((n_sub, SUBROWS, d), bf), pltpu.VMEM((n_sub, SUBROWS, d), bf), pltpu.VMEM((rows, d), bf),
            dma((32,)), dma((3,)), dma((n_loc,)), dma((n_loc,)), dma((n_sub,)), dma((n_sub,)), dma((n_sub,)), dma((n_sub,)),
            dma((n_loc,)), dma((n_loc,)), dma((n_sub,)), dma((n_sub,)), dma((n_sub,)), dma((n_sub,)), dma((n_sub,)),
        ],
        compiler_params=pltpu.CompilerParams(collective_id=2, has_side_effects=True, vmem_limit_bytes=61900 * 1024),
        cost_estimate=pl.CostEstimate(flops=10 ** 12, bytes_accessed=40 * 10 ** 6, transcendentals=0),
        name="mlp",
    )(context, r0, wo, w_up, w_down, far_up, far_down, bias.reshape(2 * ff // wide, 1, wide), vecs)


def solution(mesh):
    n_tp = mesh.shape['tp']
    n_dp = mesh.shape['dp']

    def local_step(tok_ids, pad_mask, emb_shard, ln_emb_w, ln_emb_b, ln1_w, ln1_b, w_qkv, b_qkv, w_out, b_out, ln2_w, ln2_b, w_up, b_up, w_down, b_down):
        f32 = jnp.float32
        tp_rank = lax.axis_index('tp')
        dp_rank = lax.axis_index('dp')
        n_seq, seq = tok_ids.shape
        d = emb_shard.shape[1]
        heads_loc = w_qkv.shape[1]

        def part(w, axis):
            size = w.shape[axis] // n_dp
            return lax.dynamic_slice_in_dim(w, dp_rank * size, size, axis)

        half = n_tp // 2
        swap = [(t, (t + half) % n_tp) for t in range(n_tp)]
        out_part = lax.all_gather(part(w_out, 1), 'tp', axis=0, tiled=True)
        up_part = lax.ppermute(part(w_up, 1), 'tp', swap)

        part_a = lookup(tok_ids[0], emb_shard, tp_rank)
        ids_b, down_slice, part_a = lax.optimization_barrier((tok_ids[1], part(w_down, 0), part_a))
        down_part = lax.ppermute(down_slice, 'tp', swap)
        part_b = lookup(ids_b, emb_shard, tp_rank)
        part_a, part_b, up_part, out_part = lax.optimization_barrier((part_a, part_b, up_part, out_part))
        wo = lax.all_gather(out_part, 'dp', axis=0, tiled=False)
        wu = lax.all_gather(up_part, 'dp', axis=0, tiled=False)
        ln_pack = jnp.stack([ln_emb_w, ln_emb_b, ln1_w, ln1_b]).astype(f32)
        normed_all, resid_in = chain(part_a, part_b, ln_pack, n_tp)
        normed_all, wu, wo, down_part = lax.optimization_barrier((normed_all, wu, wo, down_part))
        wd = lax.all_gather(down_part, 'dp', axis=0, tiled=True)
        qkv = (jnp.einsum('bsd,dhce->cbhse', normed_all, w_qkv, preferred_element_type=f32) + b_qkv.astype(f32).transpose(1, 0, 2)[:, None, :, None, :]).astype(jnp.bfloat16)
        all_slopes = jnp.array(alibi_slopes(heads_loc * n_tp), f32)
        head_slopes = lax.dynamic_slice_in_dim(all_slopes, tp_rank * heads_loc, heads_loc)
        context, b_all = attend(qkv, pad_mask, head_slopes, b_up.reshape(8, -1), n_tp)
        context, wd = lax.optimization_barrier((context, wd))
        far_bias = lax.dynamic_index_in_dim(b_all, (tp_rank + half) % n_tp, 0, keepdims=False).reshape(-1)
        bias = jnp.concatenate([b_up, far_bias]).astype(f32)
        rows = n_seq * seq // n_tp
        vecs = jnp.stack([b_out, ln2_w, ln2_b, b_down]).astype(f32)
        out = mlp(context.reshape(rows, d), resid_in.reshape(rows, d), wo, w_up, w_down, wu, wd, bias, vecs)
        return out.reshape(n_seq, seq // n_tp, d)

    replicated = P(None)
    in_specs = (P('dp', None), P('dp', None), P('tp', None), replicated, replicated, replicated, replicated, P(None, 'tp', None, None), P('tp', None, None), P('tp', None), replicated, replicated, replicated, P(None, 'tp'), P('tp'), P('tp', None), replicated)
    return jax.shard_map(local_step, mesh=mesh, in_specs=in_specs, out_specs=P('dp', 'tp', None), check_vma=False)
```
